32 devices in a mesh: fsdp: 8 (over y, x, core), tensor: 4 (over z).
Axes of the slice: x: 2, y: 2, z: 4, core: 2. Of those that a mesh axis runs over, the one named last changes fastest.
Arguments:
- inputs: bfloat16 [4096, 2048], P(('fsdp', 'tensor')), may hold values from -6 to 6
- cotangent: bfloat16 [4096, 2048], P(('fsdp', 'tensor')), may hold values from -6 to 6
- segments: int32 [4096], replicated, may hold values from 0 to 31, never falling along the last dimension, each value on 1 to 512 neighbouring positions
- positions: int32 [4096], P('fsdp'), may hold values from 0 to 2047
- qkv_weight: float32 [2048, 8, 768], P('fsdp', 'tensor')
- qkv_bias: float32 [8, 768], P('tensor'), may hold values from -0.6 to 0.6
- dense_weight: float32 [2048, 2048], P('fsdp', 'tensor'), may hold values from -1 to 1
- expand_weight: float32 [2048, 8192], P('fsdp', 'tensor'), may hold values from -0.125 to 0.125
- expand_bias: float32 [8192], P('tensor'), may hold values from -0.6 to 0.6
- contract_weight: float32 [2048, 8192], P('fsdp', 'tensor'), may hold values from -0.0625 to 0.0625
- norm_bias_vectors: float32 [6, 2048], replicated
- moment_qkv_weight: float32 [2048, 8, 768], P('fsdp', 'tensor'), may hold values from -24 to 24
- moment_qkv_bias: float32 [8, 768], P('tensor'), may hold values from -24 to 24
- moment_dense_weight: float32 [2048, 2048], P('fsdp', 'tensor'), may hold values from -24 to 24
- moment_expand_weight: float32 [2048, 8192], P('fsdp', 'tensor'), may hold values from -24 to 24
- moment_expand_bias: float32 [8192], P('tensor'), may hold values from -24 to 24
- moment_contract_weight: float32 [2048, 8192], P('fsdp', 'tensor'), may hold values from -24 to 24
- moment_norm_vectors: float32 [6, 2048], replicated, may hold values from -64 to 64
- second_qkv_weight: float32 [2048, 8, 768], P('fsdp', 'tensor'), may hold values from 122.88 to 491.52
- second_qkv_bias: float32 [8, 768], P('tensor'), may hold values from 122.88 to 491.52
- second_dense_weight: float32 [2048, 2048], P('fsdp', 'tensor'), may hold values from 122.88 to 491.52
- second_expand_weight: float32 [2048, 8192], P('fsdp', 'tensor'), may hold values from 122.88 to 491.52
- second_expand_bias: float32 [8192], P('tensor'), may hold values from 122.88 to 491.52
- second_contract_weight: float32 [2048, 8192], P('fsdp', 'tensor'), may hold values from 122.88 to 491.52
- second_norm_vectors: float32 [6, 2048], replicated, may hold values from 1228.8 to 4915.2
Outputs:
- output: float32 [4096, 2048], P(('fsdp', 'tensor'))
- block_input_gradient: float32 [4096, 2048], P(('fsdp', 'tensor'))
- gradient_qkv_weight: float32 [2048, 8, 768], P('fsdp', 'tensor')
- new_qkv_weight: float32 [2048, 8, 768], P('fsdp', 'tensor')
- new_moment_qkv_weight: float32 [2048, 8, 768], P('fsdp', 'tensor')
- new_second_qkv_weight: float32 [2048, 8, 768], P('fsdp', 'tensor')
- gradient_qkv_bias: float32 [8, 768], P('tensor')
- new_qkv_bias: float32 [8, 768], P('tensor')
- new_moment_qkv_bias: float32 [8, 768], P('tensor')
- new_second_qkv_bias: float32 [8, 768], P('tensor')
- gradient_dense_weight: float32 [2048, 2048], P('fsdp', 'tensor')
- new_dense_weight: float32 [2048, 2048], P('fsdp', 'tensor')
- new_moment_dense_weight: float32 [2048, 2048], P('fsdp', 'tensor')
- new_second_dense_weight: float32 [2048, 2048], P('fsdp', 'tensor')
- gradient_expand_weight: float32 [2048, 8192], P('fsdp', 'tensor')
- new_expand_weight: float32 [2048, 8192], P('fsdp', 'tensor')
- new_moment_expand_weight: float32 [2048, 8192], P('fsdp', 'tensor')
- new_second_expand_weight: float32 [2048, 8192], P('fsdp', 'tensor')
- gradient_expand_bias: float32 [8192], P('tensor')
- new_expand_bias: float32 [8192], P('tensor')
- new_moment_expand_bias: float32 [8192], P('tensor')
- new_second_expand_bias: float32 [8192], P('tensor')
- gradient_contract_weight: float32 [2048, 8192], P('fsdp', 'tensor')
- new_contract_weight: float32 [2048, 8192], P('fsdp', 'tensor')
- new_moment_contract_weight: float32 [2048, 8192], P('fsdp', 'tensor')
- new_second_contract_weight: float32 [2048, 8192], P('fsdp', 'tensor')
- gradient_norm_vectors: float32 [6, 2048], replicated
- new_norm_vectors: float32 [6, 2048], replicated
- new_moment_norm_vectors: float32 [6, 2048], replicated
- new_second_norm_vectors: float32 [6, 2048], replicated
The draws below stay inside these ranges and needn't reach their ends.
Inputs may be any that keep to these rules, and one draw needn't show every extreme that they name: `segments`: segment numbers never fall along the token stream; every document holds at most 512 tokens and one holds exactly 512.
All inputs are finite; a program needn't handle non-finite values.
Results may differ from the reference program's by a relative error of at most 0.0065.
The reference program's roundings to bfloat16 on the way count: a program that leaves them out, or rounds other values in their place, can miss the bound.
Values may be sent and summed in bfloat16 or wider, within the bound.
No kernel may reach another device: no remote copies, remote signals or barrier semaphores. Data moves between devices by JAX's collectives and lax.ppermute only.
A program may use at most 256 MiB of HBM per device.

```python
import math
import jax
import jax.numpy as jnp
import numpy as np
from jax import lax

D = 2048
HEADS = 8
HD = 256
ROT = 64
FF = 8192
CTX = 2048
STEP = 3
R = 512
TOKENS = 4096
DOCS = 32
N_FSDP = 8


def draw_qkv_weight(key, part):
    base_key = jax.random.fold_in(key, 3)
    draw_shape = (D, HEADS, 3 * HD)
    inv_root = 1.0 / jnp.sqrt(jnp.float32(D))
    return jnp.clip(jax.random.normal(base_key, draw_shape, jnp.float32), -6.0, 6.0) * inv_root


def draw_norm_bias_vectors(key, part):
    row_index = jnp.arange(6, dtype=jnp.int32)[:, None]
    is_gain = (row_index == 0) | (row_index == 2)
    shift_key = jax.random.fold_in(key, 7)
    gain_draw = 1.0 + 0.15 * jnp.clip(jax.random.normal(key, (6, D), jnp.float32), -2.5, 2.5)
    shift_draw = 0.3 * jnp.clip(jax.random.normal(shift_key, (6, D), jnp.float32), -1.6, 1.6)
    return jnp.where(is_gain, gain_draw, shift_draw)


def touch_ends(entries, rng, smallest, top_value):
    shape = entries.shape
    place = [jax.random.randint(jax.random.fold_in(rng, axis), (), 0, shape[axis]) for axis in range(len(shape))]
    entries = entries.at[tuple(place)].set(smallest)
    longest = shape.index(max(shape))
    place[longest] = (place[longest] + 1) % shape[longest]
    return entries.at[tuple(place)].set(top_value)


def strengthened(values, rng, source, target, blocks, factor):
    def block_of(dim):
        return (jnp.arange(values.shape[dim]) // (values.shape[dim] // blocks)).reshape((-1,) + (1,) * (values.ndim - 1 - dim))

    one_side = jax.random.permutation(rng, blocks)[block_of(target)]
    other_side = (block_of(target) + blocks // 2) % blocks
    return jnp.where((block_of(source) == one_side) | (block_of(source) == other_side), factor * values, values)


def levels(key, extent, cuts, least, high):
    gain, own = 1.0, jax.random.fold_in(key, 6)
    for position, parts in cuts:
        heights = jnp.exp(jax.random.uniform(jax.random.fold_in(own, position), (parts,), jnp.float32, least / len(cuts), high / len(cuts)))
        gain = gain * jnp.repeat(heights, extent[position] // parts).reshape([-1 if axis == position else 1 for axis in range(len(extent))])
    return gain


def length_profile(count, total, bound, skew):
    weights = [(1 << 20) // math.isqrt(rank ** skew) + 1 for rank in range(2, count + 1)]
    rest, counts = total - bound - (count - 1), [1] * (count - 1)
    while rest > 0:
        candidates = [i for i in range(count - 1) if counts[i] < bound]
        whole, budget = sum([weights[i] for i in candidates]), rest
        for i in candidates:
            addition = min(bound - counts[i], max(1, budget * weights[i] // whole), rest)
            counts[i] = counts[i] + addition
            rest = rest - addition
    return np.array([bound] + counts)


def ragged(key, count, total, bound, lean):
    if count == 2:
        one = jax.random.randint(key, (), max(1, total - bound), min(bound, total - 1) + 1)
        return jnp.stack([one, total - one])
    lengths = jnp.asarray(length_profile(count, total, bound, lean), jnp.int32)
    couples = (count - 1) // 2
    source_of, taker = lengths[1:1 + 2 * couples:2], lengths[2:2 + 2 * couples:2]
    margin = jnp.minimum(source_of - 1, bound - taker)
    moved = jax.random.randint(jax.random.fold_in(key, 1), (couples,), 0, 1 << 20) % (margin + 1)
    lengths = lengths.at[1:1 + 2 * couples:2].set(source_of - moved).at[2:2 + 2 * couples:2].set(taker + moved)
    return lengths[jax.random.permutation(jax.random.fold_in(key, 2), count)]


def normal_values(key, dims, deviation, reach, split=(), kind=jnp.bfloat16):
    factor_of = levels(key, dims, split, -0.22, 0.18) if split else 1.0
    values = jax.random.normal(key, dims, jnp.float32) * deviation * factor_of
    return jnp.minimum(jnp.maximum(values, -reach), reach).astype(kind)


def noise_with(own_key, extent, deviation, bound, shards, heavy, kind=jnp.bfloat16):
    array = deviation * jax.random.normal(own_key, extent, jnp.float32)
    if shards:
        array = array * levels(own_key, extent, shards, -0.22, 0.18)
    return jnp.clip(strengthened(array, jax.random.fold_in(own_key, 3), *heavy), -bound, bound).astype(kind)


def setup_inputs(seed: int = 0) -> dict:
    keys = jax.random.split(jax.random.key(seed), 26)
    inputs = normal_values(keys[0], (TOKENS, D), 1.0, 6.0, ((0, 32),))
    cotangent = noise_with(keys[1], (TOKENS, D), 1.0, 6.0, ((0, 32),), (0, 1, 32, 2.75))
    segments = jnp.searchsorted(jnp.cumsum(ragged(keys[2], DOCS, TOKENS, R, 2)), jnp.arange(TOKENS), side="right").astype(jnp.int32)
    positions = touch_ends(jax.random.randint(keys[3], (TOKENS,), 0, CTX), jax.random.fold_in(keys[3], 1), 0, CTX - 1).astype(jnp.int32)
    qkv_weight = draw_qkv_weight(jax.random.fold_in(keys[25], 71), 0)
    qkv_bias = normal_values(keys[5], (HEADS, 3 * HD), 0.1, 0.6, ((0, 4),), jnp.float32)
    dense_weight = normal_values(keys[6], (D, HEADS * HD), (HEADS * HD // 64) ** -0.5, 1.0, ((0, 8), (1, 4)), jnp.float32)
    expand_weight = normal_values(keys[7], (D, FF), D ** -0.5, 0.125, ((0, 8), (1, 4)), jnp.float32)
    expand_bias = normal_values(keys[8], (FF,), 0.1, 0.6, ((0, 4),), jnp.float32)
    contract_weight = normal_values(keys[9], (D, FF), FF ** -0.5, 0.0625, ((0, 8), (1, 4)), jnp.float32)
    norm_bias_vectors = draw_norm_bias_vectors(jax.random.fold_in(keys[25], 71), 0)
    moment_qkv_weight = normal_values(keys[11], (D, HEADS, 3 * HD), 4.0, 24.0, ((0, 8), (1, 4)), jnp.float32)
    moment_qkv_bias = normal_values(keys[12], (HEADS, 3 * HD), 4.0, 24.0, ((0, 4),), jnp.float32)
    moment_dense_weight = normal_values(keys[13], (D, HEADS * HD), 4.0, 24.0, ((0, 8), (1, 4)), jnp.float32)
    moment_expand_weight = normal_values(keys[14], (D, FF), 4.0, 24.0, ((0, 8), (1, 4)), jnp.float32)
    moment_expand_bias = normal_values(keys[15], (FF,), 4.0, 24.0, ((0, 4),), jnp.float32)
    moment_contract_weight = normal_values(keys[16], (D, FF), 4.0, 24.0, ((0, 8), (1, 4)), jnp.float32)
    moment_norm_vectors = normal_values(keys[17], (6, D), 10.0, 64.0, (), jnp.float32)
    second_qkv_weight = jnp.clip(jnp.exp(math.log(491.52) - 1.3862944 * jax.random.uniform(keys[18], (D, HEADS, 3 * HD), jnp.float32) ** levels(keys[18], (D, HEADS, 3 * HD), ((0, 8), (1, 4)), -0.2, 0.2)), 122.88, 491.52)
    second_qkv_bias = jnp.clip(jnp.exp(math.log(491.52) - 1.3862944 * jax.random.uniform(keys[19], (HEADS, 3 * HD), jnp.float32) ** levels(keys[19], (HEADS, 3 * HD), ((0, 4),), -0.2, 0.2)), 122.88, 491.52)
    second_dense_weight = jnp.clip(jnp.exp(math.log(491.52) - 1.3862944 * jax.random.uniform(keys[20], (D, HEADS * HD), jnp.float32) ** levels(keys[20], (D, HEADS * HD), ((0, 8), (1, 4)), -0.2, 0.2)), 122.88, 491.52)
    second_expand_weight = jnp.clip(jnp.exp(math.log(491.52) - 1.3862944 * jax.random.uniform(keys[21], (D, FF), jnp.float32) ** levels(keys[21], (D, FF), ((0, 8), (1, 4)), -0.2, 0.2)), 122.88, 491.52)
    second_expand_bias = jnp.clip(jnp.exp(math.log(491.52) - 1.3862944 * jax.random.uniform(keys[22], (FF,), jnp.float32) ** levels(keys[22], (FF,), ((0, 4),), -0.2, 0.2)), 122.88, 491.52)
    second_contract_weight = jnp.clip(jnp.exp(math.log(491.52) - 1.3862944 * jax.random.uniform(keys[23], (D, FF), jnp.float32) ** levels(keys[23], (D, FF), ((0, 8), (1, 4)), -0.2, 0.2)), 122.88, 491.52)
    second_norm_vectors = jnp.clip(jnp.exp(jax.random.uniform(keys[24], (6, D), jnp.float32, math.log(1228.8), math.log(4915.2))), 1228.8, 4915.2)
    return {"inputs": inputs, "cotangent": cotangent, "segments": segments, "positions": positions, "qkv_weight": qkv_weight, "qkv_bias": qkv_bias, "dense_weight": dense_weight, "expand_weight": expand_weight, "expand_bias": expand_bias, "contract_weight": contract_weight, "norm_bias_vectors": norm_bias_vectors, "moment_qkv_weight": moment_qkv_weight, "moment_qkv_bias": moment_qkv_bias, "moment_dense_weight": moment_dense_weight, "moment_expand_weight": moment_expand_weight, "moment_expand_bias": moment_expand_bias, "moment_contract_weight": moment_contract_weight, "moment_norm_vectors": moment_norm_vectors, "second_qkv_weight": second_qkv_weight, "second_qkv_bias": second_qkv_bias, "second_dense_weight": second_dense_weight, "second_expand_weight": second_expand_weight, "second_expand_bias": second_expand_bias, "second_contract_weight": second_contract_weight, "second_norm_vectors": second_norm_vectors}


norm_eps = 1e-05
masked_score = -1e+30
beta_one = 0.9
beta_two = 0.95
adam_eps = 1e-08
decay_matrix = 0.01
rate_qkv_weight = 0.005
rate_qkv_bias = 0.02
rate_dense_weight = 0.04
rate_expand_weight = 0.005
rate_expand_bias = 0.02
rate_contract_weight = 0.003
rate_norm_vectors = 0.1

def normalized_row_block(row_values):
    center = row_values - lax.optimization_barrier(jnp.mean(row_values, axis=-1, keepdims=True))
    variance = lax.optimization_barrier(jnp.mean(center * center, axis=-1, keepdims=True))
    inverse_deviation = lax.rsqrt(variance + norm_eps)
    return (center * inverse_deviation, inverse_deviation)

def norm_backward_term(upstream_gradient, gain_vector_row, centered_normalized, inverse_deviation):
    scaled_rows = upstream_gradient * gain_vector_row
    return inverse_deviation * (scaled_rows - lax.optimization_barrier(jnp.mean(scaled_rows, axis=-1, keepdims=True)) - centered_normalized * lax.optimization_barrier(jnp.mean(scaled_rows * centered_normalized, axis=-1, keepdims=True)))

def rotary_tables(token_pos):
    half_rot = ROT // 2
    frequency = 10000.0 ** (-(jnp.arange(half_rot, dtype=jnp.float32) * 2.0 / ROT))
    angles = token_pos.astype(jnp.float32)[:, None] * frequency[None, :]
    return (jnp.cos(angles)[:, None, :], jnp.sin(angles)[:, None, :])

def rotate(head_values, cosine_rotation, sine_rotation_table, direction):
    half_rot = ROT // 2
    first_half = head_values[..., :half_rot]
    second_half = head_values[..., half_rot:ROT]
    return jnp.concatenate([first_half * cosine_rotation - direction * second_half * sine_rotation_table, second_half * cosine_rotation + direction * first_half * sine_rotation_table, head_values[..., ROT:]], axis=-1)

def gelu_slope(pre_values):
    return 0.5 * (1.0 + lax.erf(pre_values * 0.7071067811865476)) + pre_values * jnp.exp(-0.5 * pre_values * pre_values) * 0.3989422804014327

def key_mask(seg_query, query_index, seg_keys, group_rows, has_prev):
    key_index = jnp.arange(seg_keys.shape[0], dtype=jnp.int32)
    causal = key_index[None, :] <= query_index[:, None]
    same_doc = seg_keys[None, :] == seg_query[:, None]
    present = (key_index[None, :] >= group_rows) | has_prev
    return causal & same_doc & present

def block_scores(query_blk, keys_all, allowed):
    scores = jnp.einsum('qhc,khc->hqk', query_blk.astype(jnp.float32), keys_all.astype(jnp.float32)) * HD ** (-0.5)
    return jnp.where(allowed[None], scores, masked_score)

def attend(query_blk, keys_all, values_all, allowed):
    scores = block_scores(query_blk, keys_all, allowed)
    row_max = lax.optimization_barrier(jnp.max(scores, axis=-1, keepdims=True))
    row_total = lax.optimization_barrier(jnp.sum(jnp.exp(scores - row_max), axis=-1, keepdims=True))
    log_total = row_max + jnp.log(row_total)
    prob_bf = jnp.exp(scores - log_total).astype(jnp.bfloat16)
    result = jnp.einsum('hqk,khc->qhc', prob_bf.astype(jnp.float32), values_all.astype(jnp.float32))
    return (result.astype(jnp.bfloat16), log_total[..., 0])

def adam_step(parameter, gradient, moment, second, step_rate, decay_weight):
    moment_new = beta_one * moment + (1.0 - beta_one) * gradient
    second_new = beta_two * second + (1.0 - beta_two) * gradient * gradient
    moment_hat = moment_new / (1.0 - beta_one ** STEP)
    second_hat = second_new / (1.0 - beta_two ** STEP)
    updated = parameter - step_rate * (moment_hat / (jnp.sqrt(second_hat) + adam_eps) + decay_weight * parameter)
    return (updated, moment_new, second_new)

def add_pair(left_sum, right_sum):
    return left_sum + right_sum

def reference(inputs, cotangent, segments, positions, qkv_weight, qkv_bias, dense_weight, expand_weight, expand_bias, contract_weight, norm_bias_vectors, moment_qkv_weight, moment_qkv_bias, moment_dense_weight, moment_expand_weight, moment_expand_bias, moment_contract_weight, moment_norm_vectors, second_qkv_weight, second_qkv_bias, second_dense_weight, second_expand_weight, second_expand_bias, second_contract_weight, second_norm_vectors):
    block_rows = min(512, R)
    blocks = R // block_rows
    qkv_flat_bf = qkv_weight.reshape(D, HEADS * 3 * HD).astype(jnp.bfloat16)
    dense_bf = dense_weight.astype(jnp.bfloat16)
    expand_bf = expand_weight.astype(jnp.bfloat16)
    contract_bf = contract_weight.astype(jnp.bfloat16)
    x_groups = inputs.reshape(N_FSDP, R, D)
    dy_groups = cotangent.reshape(N_FSDP, R, D)
    pos_groups = positions.reshape(N_FSDP, R)
    seg_groups = segments.reshape(N_FSDP, R)
    seg_before = jnp.concatenate([seg_groups[:1], seg_groups[:-1]], axis=0)
    group_ids = jnp.arange(N_FSDP, dtype=jnp.int32)
    starts = jnp.arange(blocks, dtype=jnp.int32) * block_rows
    local_index = jnp.arange(block_rows, dtype=jnp.int32)

    def prepare_inputs(input_group, position_group):
        centered_normalized, inverse_deviation = normalized_row_block(input_group.astype(jnp.float32))
        attention_normalized_input = (centered_normalized * norm_bias_vectors[0] + norm_bias_vectors[1]).astype(jnp.bfloat16)
        feedforward_normalized_input = (centered_normalized * norm_bias_vectors[2] + norm_bias_vectors[3]).astype(jnp.bfloat16)
        projected = jnp.dot(attention_normalized_input, qkv_flat_bf, preferred_element_type=jnp.float32).reshape(R, HEADS, 3 * HD) + qkv_bias[None]
        cosine_rotation, sine_rotation_table = rotary_tables(position_group)
        query_rows = rotate(projected[..., :HD], cosine_rotation, sine_rotation_table, 1.0).astype(jnp.bfloat16)
        local_segment_keys = rotate(projected[..., HD:2 * HD], cosine_rotation, sine_rotation_table, 1.0).astype(jnp.bfloat16)
        local_segment_values = projected[..., 2 * HD:].astype(jnp.bfloat16)
        expand_preactivation = jnp.dot(feedforward_normalized_input, expand_bf, preferred_element_type=jnp.float32) + expand_bias
        gelu_activated_rows = jax.nn.gelu(expand_preactivation, approximate=False).astype(jnp.bfloat16)
        return (centered_normalized, inverse_deviation, attention_normalized_input, feedforward_normalized_input, query_rows, local_segment_keys, local_segment_values, expand_preactivation, gelu_activated_rows, cosine_rotation, sine_rotation_table)

    def forward_group(carry_state, packed):
        keys_prev, values_prev = carry_state
        input_group, position_group, seg_grp, seg_prev, group_id = packed
        pieces = prepare_inputs(input_group, position_group)
        query_rows, local_segment_keys, local_segment_values, gelu_activated_rows = (pieces[4], pieces[5], pieces[6], pieces[8])
        keys_all = jnp.concatenate([keys_prev, local_segment_keys], axis=0)
        values_all = jnp.concatenate([values_prev, local_segment_values], axis=0)
        seg_keys = jnp.concatenate([seg_prev, seg_grp], axis=0)

        def one_block(block_data):
            query_blk, seg_blk, start = block_data
            allowed = key_mask(seg_blk, R + start + local_index, seg_keys, R, group_id > 0)
            return attend(query_blk, keys_all, values_all, allowed)
        attn_blocks, lse_blocks = lax.map(one_block, (query_rows.reshape(blocks, block_rows, HEADS, HD), seg_grp.reshape(blocks, block_rows), starts))
        attended = attn_blocks.reshape(R, HEADS * HD)
        branch = jnp.dot(attended, dense_bf.T, preferred_element_type=jnp.float32) + jnp.dot(gelu_activated_rows, contract_bf.T, preferred_element_type=jnp.float32)
        result = input_group.astype(jnp.float32) + branch + norm_bias_vectors[4] + norm_bias_vectors[5]
        return ((local_segment_keys, local_segment_values), (result, local_segment_keys, local_segment_values, attended, lse_blocks))
    empty_keys = jnp.zeros((R, HEADS, HD), jnp.bfloat16)
    last_keys, stacked = lax.scan(forward_group, (empty_keys, empty_keys), (x_groups, pos_groups, seg_groups, seg_before, group_ids))
    outputs, key_stack, value_stack, attended_stack, lse_stack = stacked
    key_before = jnp.concatenate([jnp.zeros_like(key_stack[:1]), key_stack[:-1]], axis=0)
    value_before = jnp.concatenate([jnp.zeros_like(value_stack[:1]), value_stack[:-1]], axis=0)

    def backward_group(carry_state, packed):
        key_next, value_next, totals = carry_state
        input_group, dy_grp, position_group, seg_grp, seg_prev, group_id, keys_prev, values_prev, attended, lse_blocks = packed
        centered_normalized, inverse_deviation, attention_normalized_input, feedforward_normalized_input, query_rows, local_segment_keys, local_segment_values, expand_preactivation, gelu_activated_rows, cosine_rotation, sine_rotation_table = prepare_inputs(input_group, position_group)
        keys_all = jnp.concatenate([keys_prev, local_segment_keys], axis=0)
        values_all = jnp.concatenate([values_prev, local_segment_values], axis=0)
        seg_keys = jnp.concatenate([seg_prev, seg_grp], axis=0)
        act_grad = jnp.dot(dy_grp, contract_bf, preferred_element_type=jnp.float32)
        pre_grad32 = act_grad * gelu_slope(expand_preactivation)
        pre_grad = pre_grad32.astype(jnp.bfloat16)
        attn_grad = jnp.dot(dy_grp, dense_bf, preferred_element_type=jnp.float32).astype(jnp.bfloat16)
        attn_heads = attn_grad.reshape(R, HEADS, HD)
        row_delta = lax.optimization_barrier(jnp.sum(attn_heads.astype(jnp.float32) * attended.reshape(R, HEADS, HD).astype(jnp.float32), axis=-1))

        def one_block(inner_carry, block_data):
            key_acc, value_acc = inner_carry
            query_blk, seg_blk, start, grad_blk, delta_blk, lse_blk = block_data
            allowed = key_mask(seg_blk, R + start + local_index, seg_keys, R, group_id > 0)
            scores = block_scores(query_blk, keys_all, allowed)
            prob_f32 = jnp.exp(scores - lse_blk[..., None])
            prob_bf = prob_f32.astype(jnp.bfloat16)
            dot_grad = jnp.einsum('qhc,khc->hqk', grad_blk.astype(jnp.float32), values_all.astype(jnp.float32))
            score_grad = (prob_f32 * (dot_grad - jnp.transpose(delta_blk)[..., None]) * HD ** (-0.5)).astype(jnp.bfloat16)
            query_grad = jnp.einsum('hqk,khc->qhc', score_grad.astype(jnp.float32), keys_all.astype(jnp.float32))
            key_acc = key_acc + jnp.einsum('hqk,qhc->khc', score_grad.astype(jnp.float32), query_blk.astype(jnp.float32))
            value_acc = value_acc + jnp.einsum('hqk,qhc->khc', prob_bf.astype(jnp.float32), grad_blk.astype(jnp.float32))
            return ((key_acc, value_acc), query_grad)
        zero_keys = jnp.zeros((2 * R, HEADS, HD), jnp.float32)
        inner_final, query_grads = lax.scan(one_block, (zero_keys, zero_keys), (query_rows.reshape(blocks, block_rows, HEADS, HD), seg_grp.reshape(blocks, block_rows), starts, attn_heads.reshape(blocks, block_rows, HEADS, HD), row_delta.reshape(blocks, block_rows, HEADS), lse_blocks))
        key_acc, value_acc = inner_final
        key_grad = key_acc[R:] + key_next
        value_grad = value_acc[R:] + value_next
        query_grad = query_grads.reshape(R, HEADS, HD)
        qkv_grad32 = jnp.concatenate([rotate(query_grad, cosine_rotation, sine_rotation_table, -1.0), rotate(key_grad, cosine_rotation, sine_rotation_table, -1.0), value_grad], axis=-1)
        qkv_grad = qkv_grad32.astype(jnp.bfloat16).reshape(R, HEADS * 3 * HD)
        attention_backward_term = jnp.dot(qkv_grad, qkv_flat_bf.T, preferred_element_type=jnp.float32)
        feedforward_backward_term = jnp.dot(pre_grad, expand_bf.T, preferred_element_type=jnp.float32)
        upstream_grad_single = dy_grp.astype(jnp.float32)
        block_input_gradient = upstream_grad_single + norm_backward_term(attention_backward_term, norm_bias_vectors[0], centered_normalized, inverse_deviation) + norm_backward_term(feedforward_backward_term, norm_bias_vectors[2], centered_normalized, inverse_deviation)
        vector_gradient_term = jnp.stack([lax.optimization_barrier(jnp.sum(attention_backward_term * centered_normalized, axis=0)), lax.optimization_barrier(jnp.sum(attention_backward_term, axis=0)), lax.optimization_barrier(jnp.sum(feedforward_backward_term * centered_normalized, axis=0)), lax.optimization_barrier(jnp.sum(feedforward_backward_term, axis=0)), lax.optimization_barrier(jnp.sum(upstream_grad_single, axis=0)), lax.optimization_barrier(jnp.sum(upstream_grad_single, axis=0))])
        new_terms = (jnp.dot(attention_normalized_input.T, qkv_grad, preferred_element_type=jnp.float32).reshape(D, HEADS, 3 * HD), lax.optimization_barrier(jnp.sum(qkv_grad32, axis=0)), jnp.dot(dy_grp.T, attended, preferred_element_type=jnp.float32), jnp.dot(feedforward_normalized_input.T, pre_grad, preferred_element_type=jnp.float32), lax.optimization_barrier(jnp.sum(pre_grad32, axis=0)), jnp.dot(dy_grp.T, gelu_activated_rows, preferred_element_type=jnp.float32), vector_gradient_term)
        totals = jax.tree.map(add_pair, totals, new_terms)
        return ((key_acc[:R], value_acc[:R], totals), block_input_gradient)
    zero_totals = (jnp.zeros((D, HEADS, 3 * HD), jnp.float32), jnp.zeros((HEADS, 3 * HD), jnp.float32), jnp.zeros((D, HEADS * HD), jnp.float32), jnp.zeros((D, FF), jnp.float32), jnp.zeros((FF,), jnp.float32), jnp.zeros((D, FF), jnp.float32), jnp.zeros((6, D), jnp.float32))
    zero_grads = jnp.zeros((R, HEADS, HD), jnp.float32)
    final_state, input_grads = lax.scan(backward_group, (zero_grads, zero_grads, zero_totals), (x_groups, dy_groups, pos_groups, seg_groups, seg_before, group_ids, key_before, value_before, attended_stack, lse_stack), reverse=True)
    grads = final_state[2]
    new_qkv_weight, new_moment_qkv_weight, new_second_qkv_weight = adam_step(qkv_weight, grads[0], moment_qkv_weight, second_qkv_weight, rate_qkv_weight, decay_matrix)
    new_qkv_bias, new_moment_qkv_bias, new_second_qkv_bias = adam_step(qkv_bias, grads[1], moment_qkv_bias, second_qkv_bias, rate_qkv_bias, 0.0)
    new_dense_weight, new_moment_dense_weight, new_second_dense_weight = adam_step(dense_weight, grads[2], moment_dense_weight, second_dense_weight, rate_dense_weight, decay_matrix)
    new_expand_weight, new_moment_expand_weight, new_second_expand_weight = adam_step(expand_weight, grads[3], moment_expand_weight, second_expand_weight, rate_expand_weight, decay_matrix)
    new_expand_bias, new_moment_expand_bias, new_second_expand_bias = adam_step(expand_bias, grads[4], moment_expand_bias, second_expand_bias, rate_expand_bias, 0.0)
    new_contract_weight, new_moment_contract_weight, new_second_contract_weight = adam_step(contract_weight, grads[5], moment_contract_weight, second_contract_weight, rate_contract_weight, decay_matrix)
    new_norm_vectors, new_moment_norm_vectors, new_second_norm_vectors = adam_step(norm_bias_vectors, grads[6], moment_norm_vectors, second_norm_vectors, rate_norm_vectors, 0.0)
    return (outputs.reshape(TOKENS, D), input_grads.reshape(TOKENS, D), grads[0], new_qkv_weight, new_moment_qkv_weight, new_second_qkv_weight, grads[1], new_qkv_bias, new_moment_qkv_bias, new_second_qkv_bias, grads[2], new_dense_weight, new_moment_dense_weight, new_second_dense_weight, grads[3], new_expand_weight, new_moment_expand_weight, new_second_expand_weight, grads[4], new_expand_bias, new_moment_expand_bias, new_second_expand_bias, grads[5], new_contract_weight, new_moment_contract_weight, new_second_contract_weight, grads[6], new_norm_vectors, new_moment_norm_vectors, new_second_norm_vectors)
```

```python
import jax
import jax.numpy as jnp
from jax import lax
from jax.sharding import PartitionSpec as P

ROT = 64
STEP = 3


norm_eps = 1e-05
masked_score = -1e30
beta_one = 0.9
beta_two = 0.95
adam_eps = 1e-08
decay_matrix = 0.01
rate_qkv_weight = 0.005
rate_qkv_bias = 0.02
rate_dense_weight = 0.04
rate_expand_weight = 0.005
rate_expand_bias = 0.02
rate_contract_weight = 0.003
rate_norm_vectors = 0.1


def shifted(value, axis, steps):
    count = lax.axis_size(axis)
    first, last = (max(0, -steps), min(count, count - steps))
    return lax.ppermute(value, axis, [(source, source + steps) for source in range(first, last)])


def normalized_row_block(row_values):
    center = row_values - jnp.mean(row_values, axis=-1, keepdims=True)
    variance = jnp.mean(center * center, axis=-1, keepdims=True)
    inverse_deviation = lax.rsqrt(variance + norm_eps)
    return (center * inverse_deviation, inverse_deviation)


def norm_backward_term(upstream_gradient, gain_vector_row, centered_normalized, inverse_deviation):
    scaled_rows = upstream_gradient * gain_vector_row
    return inverse_deviation * (
        scaled_rows
        - jnp.mean(scaled_rows, axis=-1, keepdims=True)
        - centered_normalized * jnp.mean(scaled_rows * centered_normalized, axis=-1, keepdims=True)
    )


def rotary_tables(token_pos):
    half_rot = ROT // 2
    frequency = 10000.0 ** (-(jnp.arange(half_rot, dtype=jnp.float32) * 2.0 / ROT))
    angles = token_pos.astype(jnp.float32)[:, None] * frequency[None, :]
    return (jnp.cos(angles)[:, None, :], jnp.sin(angles)[:, None, :])


def rotate(head_values, cosine_rotation, sine_rotation_table, direction):
    half_rot = ROT // 2
    first_half = head_values[..., :half_rot]
    second_half = head_values[..., half_rot:ROT]
    return jnp.concatenate(
        [
            first_half * cosine_rotation - direction * second_half * sine_rotation_table,
            second_half * cosine_rotation + direction * first_half * sine_rotation_table,
            head_values[..., ROT:],
        ],
        axis=-1,
    )


def gelu_slope(pre_values):
    return (
        0.5 * (1.0 + lax.erf(pre_values * 0.7071067811865476))
        + pre_values * jnp.exp(-0.5 * pre_values * pre_values) * 0.3989422804014327
    )


def key_mask(seg_query, query_index, seg_keys, group_rows, has_prev):
    key_index = jnp.arange(seg_keys.shape[0], dtype=jnp.int32)
    causal = key_index[None, :] <= query_index[:, None]
    same_doc = seg_keys[None, :] == seg_query[:, None]
    present = (key_index[None, :] >= group_rows) | has_prev
    return causal & same_doc & present


def block_scores(query_blk, keys_all, allowed, score_scale):
    scores = (
        jnp.einsum("qhc,khc->hqk", query_blk, keys_all, preferred_element_type=jnp.float32)
        * score_scale
    )
    return jnp.where(allowed[None], scores, masked_score)


def adam_step(parameter, gradient, moment, second, step_rate, decay_weight):
    moment_new = beta_one * moment + (1.0 - beta_one) * gradient
    second_new = beta_two * second + (1.0 - beta_two) * gradient * gradient
    moment_hat = moment_new / (1.0 - beta_one**STEP)
    second_hat = second_new / (1.0 - beta_two**STEP)
    updated = parameter - step_rate * (
        moment_hat / (jnp.sqrt(second_hat) + adam_eps) + decay_weight * parameter
    )
    return (updated, moment_new, second_new)


def contract_rows(left_rows, right_rows):
    return lax.dot_general(
        left_rows, right_rows, (((0,), (0,)), ((), ())), preferred_element_type=jnp.float32
    )


def contract_cols(left_cols, right_cols):
    return lax.dot_general(
        left_cols, right_cols, (((1,), (1,)), ((), ())), preferred_element_type=jnp.float32
    )


def per_device_generic(
    inputs,
    cotangent,
    segments,
    positions,
    qkv_weight,
    qkv_bias,
    dense_weight,
    expand_weight,
    expand_bias,
    contract_weight,
    norm_bias_vectors,
    moment_qkv_weight,
    moment_qkv_bias,
    moment_dense_weight,
    moment_expand_weight,
    moment_expand_bias,
    moment_contract_weight,
    moment_norm_vectors,
    second_qkv_weight,
    second_qkv_bias,
    second_dense_weight,
    second_expand_weight,
    second_expand_bias,
    second_contract_weight,
    second_norm_vectors,
):
    fsdp_index = lax.axis_index("fsdp")
    input_row_block, rows_dy = (
        lax.all_gather(inputs, "tensor", axis=0, tiled=True),
        lax.all_gather(cotangent, "tensor", axis=0, tiled=True),
    )
    group_rows = input_row_block.shape[0]
    shards_bf = (
        qkv_weight.astype(jnp.bfloat16),
        dense_weight.astype(jnp.bfloat16),
        expand_weight.astype(jnp.bfloat16),
        contract_weight.astype(jnp.bfloat16),
    )
    forward_set = (
        lax.all_gather(shards_bf[0], "fsdp", axis=0, tiled=True),
        lax.all_gather(shards_bf[1], "fsdp", axis=0, tiled=True),
        lax.all_gather(shards_bf[2], "fsdp", axis=0, tiled=True),
        lax.all_gather(shards_bf[3], "fsdp", axis=0, tiled=True),
    )
    full_qkv, full_dense, full_expand, full_contract = forward_set
    row_centered_normalized, inverse_row_deviation = normalized_row_block(
        input_row_block.astype(jnp.float32)
    )
    attention_normalized_input = (
        row_centered_normalized * norm_bias_vectors[0] + norm_bias_vectors[1]
    ).astype(jnp.bfloat16)
    feedforward_normalized_input = (
        row_centered_normalized * norm_bias_vectors[2] + norm_bias_vectors[3]
    ).astype(jnp.bfloat16)
    projected = (
        jnp.einsum(
            "rd,dhc->rhc", attention_normalized_input, full_qkv, preferred_element_type=jnp.float32
        )
        + qkv_bias[None]
    )
    heads_dev = projected.shape[1]
    head_dim = projected.shape[2] // 3
    score_scale = head_dim ** (-0.5)
    cosine_rotation, sine_rotation_table = rotary_tables(positions)
    query_rows = rotate(
        projected[..., :head_dim], cosine_rotation, sine_rotation_table, 1.0
    ).astype(jnp.bfloat16)
    local_segment_keys = rotate(
        projected[..., head_dim : 2 * head_dim], cosine_rotation, sine_rotation_table, 1.0
    ).astype(jnp.bfloat16)
    local_segment_values = projected[..., 2 * head_dim :].astype(jnp.bfloat16)
    keys_prev, values_prev = shifted((local_segment_keys, local_segment_values), "fsdp", 1)
    keys_all = jnp.concatenate([keys_prev, local_segment_keys], axis=0)
    values_all = jnp.concatenate([values_prev, local_segment_values], axis=0)
    seg_own = lax.dynamic_slice_in_dim(segments, fsdp_index * group_rows, group_rows)
    seg_prev = lax.dynamic_slice_in_dim(
        segments, jnp.maximum(fsdp_index - 1, 0) * group_rows, group_rows
    )
    seg_keys = jnp.concatenate([seg_prev, seg_own], axis=0)
    has_prev = fsdp_index > 0
    block_rows = min(512, group_rows)
    blocks = group_rows // block_rows
    starts = jnp.arange(blocks, dtype=jnp.int32) * block_rows
    local_index = jnp.arange(block_rows, dtype=jnp.int32)
    query_blocks = query_rows.reshape(blocks, block_rows, heads_dev, head_dim)
    seg_blocks = seg_own.reshape(blocks, block_rows)

    def forward_block(block_data):
        query_blk, seg_blk, start = block_data
        allowed = key_mask(
            seg_blk, group_rows + start + local_index, seg_keys, group_rows, has_prev
        )
        scores = block_scores(query_blk, keys_all, allowed, score_scale)
        row_max = jnp.max(scores, axis=-1, keepdims=True)
        row_total = jnp.sum(jnp.exp(scores - row_max), axis=-1, keepdims=True)
        log_total = row_max + jnp.log(row_total)
        prob_bf = jnp.exp(scores - log_total).astype(jnp.bfloat16)
        result = jnp.einsum("hqk,khc->qhc", prob_bf, values_all, preferred_element_type=jnp.float32)
        return (result.astype(jnp.bfloat16), log_total[..., 0])

    attn_blocks, lse_blocks = lax.map(forward_block, (query_blocks, seg_blocks, starts))
    attended = attn_blocks.reshape(group_rows, heads_dev * head_dim)
    expand_preactivation = (
        jnp.dot(feedforward_normalized_input, full_expand, preferred_element_type=jnp.float32)
        + expand_bias
    )
    gelu_activated_rows = jax.nn.gelu(expand_preactivation, approximate=False).astype(jnp.bfloat16)
    branch_sum = lax.psum_scatter(
        contract_cols(attended, full_dense) + contract_cols(gelu_activated_rows, full_contract),
        "tensor",
        scatter_dimension=0,
        tiled=True,
    )
    output = inputs.astype(jnp.float32) + branch_sum + norm_bias_vectors[4] + norm_bias_vectors[5]
    back_qkv, back_dense, back_expand, back_contract = forward_set
    act_grad = jnp.dot(rows_dy, back_contract, preferred_element_type=jnp.float32)
    pre_grad32 = act_grad * gelu_slope(expand_preactivation)
    pre_grad = pre_grad32.astype(jnp.bfloat16)
    attn_grad = jnp.dot(rows_dy, back_dense, preferred_element_type=jnp.float32).astype(
        jnp.bfloat16
    )
    attn_heads = attn_grad.reshape(group_rows, heads_dev, head_dim)
    row_delta = jnp.sum(
        attn_heads.astype(jnp.float32)
        * attended.reshape(group_rows, heads_dev, head_dim).astype(jnp.float32),
        axis=-1,
    )

    def backward_block(inner_carry, block_data):
        key_acc, value_acc = inner_carry
        query_blk, seg_blk, start, grad_blk, delta_blk, lse_blk = block_data
        allowed = key_mask(
            seg_blk, group_rows + start + local_index, seg_keys, group_rows, has_prev
        )
        scores = block_scores(query_blk, keys_all, allowed, score_scale)
        prob_f32 = jnp.exp(scores - lse_blk[..., None])
        prob_bf = prob_f32.astype(jnp.bfloat16)
        dot_grad = jnp.einsum(
            "qhc,khc->hqk", grad_blk, values_all, preferred_element_type=jnp.float32
        )
        score_grad = (
            prob_f32 * (dot_grad - jnp.transpose(delta_blk)[..., None]) * score_scale
        ).astype(jnp.bfloat16)
        query_grad = jnp.einsum(
            "hqk,khc->qhc", score_grad, keys_all, preferred_element_type=jnp.float32
        )
        key_acc = key_acc + jnp.einsum(
            "hqk,qhc->khc", score_grad, query_blk, preferred_element_type=jnp.float32
        )
        value_acc = value_acc + jnp.einsum(
            "hqk,qhc->khc", prob_bf, grad_blk, preferred_element_type=jnp.float32
        )
        return ((key_acc, value_acc), query_grad)

    zero_keys = jnp.zeros((2 * group_rows, heads_dev, head_dim), jnp.float32)
    inner_final, query_grads = lax.scan(
        backward_block,
        (zero_keys, zero_keys),
        (
            query_blocks,
            seg_blocks,
            starts,
            attn_heads.reshape(blocks, block_rows, heads_dev, head_dim),
            row_delta.reshape(blocks, block_rows, heads_dev),
            lse_blocks,
        ),
    )
    key_acc, value_acc = inner_final
    later_key_grad, later_value_grad = shifted(
        (key_acc[:group_rows], value_acc[:group_rows]), "fsdp", -1
    )
    key_grad = key_acc[group_rows:] + later_key_grad
    value_grad = value_acc[group_rows:] + later_value_grad
    query_grad = query_grads.reshape(group_rows, heads_dev, head_dim)
    qkv_grad32 = jnp.concatenate(
        [
            rotate(query_grad, cosine_rotation, sine_rotation_table, -1.0),
            rotate(key_grad, cosine_rotation, sine_rotation_table, -1.0),
            value_grad,
        ],
        axis=-1,
    )
    qkv_grad = qkv_grad32.astype(jnp.bfloat16)
    attn_norm_grad = jnp.einsum(
        "rhc,dhc->rd", qkv_grad, back_qkv, preferred_element_type=jnp.float32
    )
    mlp_norm_grad = contract_cols(pre_grad, back_expand)
    qkv_part = jnp.einsum(
        "rd,rhc->dhc", attention_normalized_input, qkv_grad, preferred_element_type=jnp.float32
    )
    dense_part = contract_rows(rows_dy, attended)
    expand_part = contract_rows(feedforward_normalized_input, pre_grad)
    contract_part = contract_rows(rows_dy, gelu_activated_rows)
    local_centered_normalized, inverse_local_deviation = normalized_row_block(
        inputs.astype(jnp.float32)
    )
    dy_local = cotangent.astype(jnp.float32)
    dy_column_sum = jnp.sum(dy_local, axis=0)
    attention_backward_term, feedforward_backward_term = (
        lax.psum_scatter(attn_norm_grad, "tensor", scatter_dimension=0, tiled=True),
        lax.psum_scatter(mlp_norm_grad, "tensor", scatter_dimension=0, tiled=True),
    )
    block_input_gradient = (
        dy_local
        + norm_backward_term(
            attention_backward_term,
            norm_bias_vectors[0],
            local_centered_normalized,
            inverse_local_deviation,
        )
        + norm_backward_term(
            feedforward_backward_term,
            norm_bias_vectors[2],
            local_centered_normalized,
            inverse_local_deviation,
        )
    )
    vector_part = jnp.stack(
        [
            jnp.sum(attention_backward_term * local_centered_normalized, axis=0),
            jnp.sum(attention_backward_term, axis=0),
            jnp.sum(feedforward_backward_term * local_centered_normalized, axis=0),
            jnp.sum(feedforward_backward_term, axis=0),
            dy_column_sum,
            dy_column_sum,
        ]
    )
    qkv_bias_part = jnp.sum(qkv_grad32, axis=0)
    expand_bias_part = jnp.sum(pre_grad32, axis=0)
    grad_qkv_weight, grad_dense_weight, grad_expand_weight, grad_contract_weight = (
        lax.psum_scatter(qkv_part, "fsdp", scatter_dimension=0, tiled=True),
        lax.psum_scatter(dense_part, "fsdp", scatter_dimension=0, tiled=True),
        lax.psum_scatter(expand_part, "fsdp", scatter_dimension=0, tiled=True),
        lax.psum_scatter(contract_part, "fsdp", scatter_dimension=0, tiled=True),
    )
    grad_qkv_bias, grad_expand_bias, vector_fsdp = lax.psum(
        (qkv_bias_part, expand_bias_part, vector_part), "fsdp"
    )
    grad_norm_vectors = lax.psum(vector_fsdp, "tensor")
    new_qkv_weight, new_moment_qkv_weight, new_second_qkv_weight = adam_step(
        qkv_weight,
        grad_qkv_weight,
        moment_qkv_weight,
        second_qkv_weight,
        rate_qkv_weight,
        decay_matrix,
    )
    new_qkv_bias, new_moment_qkv_bias, new_second_qkv_bias = adam_step(
        qkv_bias, grad_qkv_bias, moment_qkv_bias, second_qkv_bias, rate_qkv_bias, 0.0
    )
    new_dense_weight, new_moment_dense_weight, new_second_dense_weight = adam_step(
        dense_weight,
        grad_dense_weight,
        moment_dense_weight,
        second_dense_weight,
        rate_dense_weight,
        decay_matrix,
    )
    new_expand_weight, new_moment_expand_weight, new_second_expand_weight = adam_step(
        expand_weight,
        grad_expand_weight,
        moment_expand_weight,
        second_expand_weight,
        rate_expand_weight,
        decay_matrix,
    )
    new_expand_bias, new_moment_expand_bias, new_second_expand_bias = adam_step(
        expand_bias, grad_expand_bias, moment_expand_bias, second_expand_bias, rate_expand_bias, 0.0
    )
    new_contract_weight, new_moment_contract_weight, new_second_contract_weight = adam_step(
        contract_weight,
        grad_contract_weight,
        moment_contract_weight,
        second_contract_weight,
        rate_contract_weight,
        decay_matrix,
    )
    new_norm_vectors, new_moment_norm_vectors, new_second_norm_vectors = adam_step(
        norm_bias_vectors,
        grad_norm_vectors,
        moment_norm_vectors,
        second_norm_vectors,
        rate_norm_vectors,
        0.0,
    )
    return (
        output,
        block_input_gradient,
        grad_qkv_weight,
        new_qkv_weight,
        new_moment_qkv_weight,
        new_second_qkv_weight,
        grad_qkv_bias,
        new_qkv_bias,
        new_moment_qkv_bias,
        new_second_qkv_bias,
        grad_dense_weight,
        new_dense_weight,
        new_moment_dense_weight,
        new_second_dense_weight,
        grad_expand_weight,
        new_expand_weight,
        new_moment_expand_weight,
        new_second_expand_weight,
        grad_expand_bias,
        new_expand_bias,
        new_moment_expand_bias,
        new_second_expand_bias,
        grad_contract_weight,
        new_contract_weight,
        new_moment_contract_weight,
        new_second_contract_weight,
        grad_norm_vectors,
        new_norm_vectors,
        new_moment_norm_vectors,
        new_second_norm_vectors,
    )


def send(value, axis, pairs):
    return lax.ppermute(value, axis, pairs)


def product(left, right):
    return jnp.dot(left, right, preferred_element_type=jnp.float32)


def relative_features(value, chip):
    width = value.shape[-1] // 4
    blocks = [
        lax.dynamic_slice_in_dim(value, (chip ^ r) * width, width, axis=value.ndim - 1)
        for r in range(4)
    ]
    return jnp.concatenate(blocks, axis=-1)


def per_device_paired(
    inputs,
    cotangent,
    segments,
    positions,
    qkv_weight,
    qkv_bias,
    dense_weight,
    expand_weight,
    expand_bias,
    contract_weight,
    norm_bias_vectors,
    moment_qkv_weight,
    moment_qkv_bias,
    moment_dense_weight,
    moment_expand_weight,
    moment_expand_bias,
    moment_contract_weight,
    moment_norm_vectors,
    second_qkv_weight,
    second_qkv_bias,
    second_dense_weight,
    second_expand_weight,
    second_expand_bias,
    second_contract_weight,
    second_norm_vectors,
):
    bf16, f32 = jnp.bfloat16, jnp.float32
    fsdp_index = lax.axis_index("fsdp")
    z = lax.axis_index("tensor")
    n_z = lax.axis_size("tensor")
    core = fsdp_index % 2
    chip = fsdp_index // 2
    devices = range(lax.axis_size("fsdp"))
    to_core = [(i, i ^ 1) for i in devices]
    to_x = [(i, i ^ 2) for i in devices]
    to_y = [(i, i ^ 4) for i in devices]
    to_next = [(i, i + 2) for i in devices if i + 2 < len(devices)]
    to_prev = [(i + 2, i) for i in devices if i + 2 < len(devices)]
    first = core == 0
    head_dim = qkv_weight.shape[2] // 3
    score_scale = head_dim ** (-0.5)
    shard_rows = inputs.shape[0]
    group_rows = n_z * shard_rows
    hidden = expand_weight.shape[1] // 2
    qkv_cols = 3 * head_dim
    shard_feat = expand_weight.shape[0]
    chip_feat = 2 * shard_feat

    def half_columns(k):
        return (
            lax.dynamic_slice_in_dim(expand_weight, k * hidden, hidden, axis=1).astype(bf16),
            jnp.concatenate(
                [
                    lax.dynamic_index_in_dim(qkv_weight, k, axis=1, keepdims=False),
                    lax.dynamic_slice_in_dim(dense_weight, k * head_dim, head_dim, axis=1),
                ],
                axis=1,
            ).astype(bf16),
            lax.dynamic_slice_in_dim(contract_weight, k * hidden, hidden, axis=1).astype(bf16),
        )

    def rows_of_chip(own, other):
        return jnp.concatenate(
            [jnp.where(first, own, other), jnp.where(first, other, own)], axis=0
        )

    x_rel = relative_features(inputs, chip)
    dy_rel = relative_features(cotangent, chip)
    vectors = relative_features(norm_bias_vectors, chip)

    def gather_tokens(own):
        pieces = [own]
        for k in range(1, n_z):
            pieces.append(send(own, "tensor", [(i, (i + k) % n_z) for i in range(n_z)]))
        return jnp.concatenate(pieces, axis=0)

    mine = half_columns(core)
    theirs = half_columns(1 - core)
    gathered = []
    for own, other in zip(mine, theirs):
        block = rows_of_chip(own, send(other, "fsdp", to_core))
        from_x = send(block, "fsdp", to_x)
        from_y = send(block, "fsdp", to_y)
        diag_top = send(from_y[:shard_feat], "fsdp", to_x)
        diag_bottom = send(from_x[shard_feat:], "fsdp", to_y)
        gathered.append(jnp.concatenate([block, from_x, from_y, diag_top, diag_bottom], axis=0))
    full_expand, full_qd, full_contract = gathered
    full_qkv = full_qd[:, :qkv_cols]
    full_dense = full_qd[:, qkv_cols:]

    x_group = gather_tokens(x_rel)
    dy_group = gather_tokens(dy_rel)
    x_all = jnp.concatenate([x_group, send(x_group, "fsdp", to_core)], axis=0)
    dy_all = jnp.concatenate([dy_group, send(dy_group, "fsdp", to_core)], axis=0)

    local = jnp.arange(group_rows, dtype=jnp.int32)
    order = ((z - local // shard_rows) % n_z) * shard_rows + local % shard_rows

    def token_block(values, start):
        blocks = [
            lax.dynamic_slice_in_dim(
                values, start + ((z - k) % n_z) * shard_rows, shard_rows
            )
            for k in range(n_z)
        ]
        return jnp.concatenate(blocks)

    chip_start = chip * 2 * group_rows
    prev_start = jnp.maximum(chip_start - group_rows, 0)
    seg_first = token_block(segments, chip_start)
    seg_second = token_block(segments, chip_start + group_rows)
    seg_halo = token_block(segments, prev_start)
    position_other = send(positions, "fsdp", to_core)
    position_all = jnp.concatenate([token_block(positions, 0), token_block(position_other, 0)])

    xhat, inverse_deviation = normalized_row_block(x_all.astype(f32))
    xa = (xhat * vectors[0] + vectors[1]).astype(bf16)
    xm = (xhat * vectors[2] + vectors[3]).astype(bf16)

    expand_bias_half = lax.dynamic_slice_in_dim(expand_bias, core * hidden, hidden)
    expand_pre = product(xm, full_expand) + expand_bias_half
    activated = jax.nn.gelu(expand_pre, approximate=False).astype(bf16)

    head_bias = lax.dynamic_index_in_dim(qkv_bias, core, axis=0, keepdims=False)
    projected = (product(xa, full_qkv) + head_bias)[:, None, :]
    cosines, sines = rotary_tables(position_all)
    queries = rotate(projected[..., :head_dim], cosines, sines, 1.0)[:, 0].astype(bf16)
    keys = rotate(projected[..., head_dim : 2 * head_dim], cosines, sines, 1.0)[:, 0].astype(bf16)
    values = projected[:, 0, 2 * head_dim :].astype(bf16)
    kv = jnp.concatenate([keys, values], axis=1)
    kv_own, kv_other = kv[:group_rows], kv[group_rows:]
    kv_halo = send(jnp.where(first, kv_other, kv_own), "fsdp", to_next)
    kv_blocks = jnp.stack(
        [
            jnp.concatenate([jnp.where(first, kv_halo, kv_other), kv_own], axis=0),
            jnp.concatenate([jnp.where(first, kv_own, kv_halo), kv_other], axis=0),
        ]
    )
    keys_blocks, values_blocks = kv_blocks[..., :head_dim], kv_blocks[..., head_dim:]
    seg_own = jnp.where(first, seg_first, seg_second)
    seg_other = jnp.where(first, seg_second, seg_first)
    seg_keys = jnp.stack(
        [
            jnp.concatenate([jnp.where(first, seg_halo, seg_first), seg_own]),
            jnp.concatenate([jnp.where(first, seg_first, seg_halo), seg_other]),
        ]
    )
    seg_queries = jnp.stack([seg_own, seg_other])
    key_order = jnp.concatenate([order, order + group_rows])
    causal = key_order[None, :] <= (order + group_rows)[:, None]
    halo_block = jnp.stack([first, ~first])
    present = (
        (jnp.arange(2 * group_rows) >= group_rows)[None, :]
        | ~halo_block[:, None]
        | (chip > 0)
    )
    allowed = (
        causal[None] & (seg_queries[:, :, None] == seg_keys[:, None, :]) & present[:, None, :]
    )
    query_blocks = queries.reshape(2, group_rows, head_dim)
    scores = (
        jnp.einsum("bqc,bkc->bqk", query_blocks, keys_blocks, preferred_element_type=f32)
        * score_scale
    )
    scores = jnp.where(allowed, scores, masked_score)
    row_max = jnp.max(scores, axis=-1, keepdims=True)
    log_total = row_max + jnp.log(jnp.sum(jnp.exp(scores - row_max), axis=-1, keepdims=True))
    probs = jnp.exp(scores - log_total)
    probs_bf = probs.astype(bf16)
    attended_blocks = jnp.einsum(
        "bqk,bkc->bqc", probs_bf, values_blocks, preferred_element_type=f32
    ).astype(bf16)
    attended = attended_blocks.reshape(2 * group_rows, head_dim)

    def reduce_features(rows_left, rows_right):
        def block(r):
            parts = [
                contract_rows(left[:, r * chip_feat : (r + 1) * chip_feat], right)
                for left, right in zip(rows_left, rows_right)
            ]
            return parts[0] if len(parts) == 1 else jnp.concatenate(parts, axis=1)

        diag = block(3).astype(bf16)
        from_x = send(diag[:shard_feat], "fsdp", to_x)
        from_y = send(diag[shard_feat:], "fsdp", to_y)
        zero = jnp.zeros_like(from_x)
        for_x = (block(1) + jnp.concatenate([zero, from_y], axis=0).astype(f32)).astype(bf16)
        for_y = (block(2) + jnp.concatenate([from_x, zero], axis=0).astype(f32)).astype(bf16)
        got_x = send(for_x, "fsdp", to_x)
        got_y = send(for_y, "fsdp", to_y)
        own = block(0) + got_x.astype(f32) + got_y.astype(f32)
        kept = lax.dynamic_slice_in_dim(own, core * shard_feat, shard_feat, axis=0)
        given = lax.dynamic_slice_in_dim(own, (1 - core) * shard_feat, shard_feat, axis=0)
        taken = send(given, "fsdp", to_core)
        return jnp.where(first, kept, taken), jnp.where(first, taken, kept)

    def reduce_tokens(part):
        other = send(part[group_rows:].astype(bf16), "fsdp", to_core)
        rows = part[:group_rows] + other.astype(f32)
        total = rows[:shard_rows]
        for k in range(1, n_z):
            piece = rows[k * shard_rows : (k + 1) * shard_rows].astype(bf16)
            total = total + send(
                piece, "tensor", [(i, (i - k) % n_z) for i in range(n_z)]
            ).astype(f32)
        return total

    contract_halves = reduce_features([dy_all], [activated])

    act_grad = product(dy_all, full_contract)
    pre_grad32 = act_grad * gelu_slope(expand_pre)
    pre_grad = pre_grad32.astype(bf16)
    expand_bias_part = jnp.sum(pre_grad32, axis=0)
    expand_halves = reduce_features([xm], [pre_grad])

    attn_grad = product(dy_all, full_dense).astype(bf16)
    row_delta = jnp.sum(attn_grad.astype(f32) * attended.astype(f32), axis=-1)
    grad_blocks = attn_grad.reshape(2, group_rows, head_dim)
    dot_grad = jnp.einsum("bqc,bkc->bqk", grad_blocks, values_blocks, preferred_element_type=f32)
    score_grad = (
        probs * (dot_grad - row_delta.reshape(2, group_rows, 1)) * score_scale
    ).astype(bf16)
    query_grad = jnp.einsum(
        "bqk,bkc->bqc", score_grad, keys_blocks, preferred_element_type=f32
    ).reshape(2 * group_rows, head_dim)
    key_parts = jnp.einsum("bqk,bqc->bkc", score_grad, query_blocks, preferred_element_type=f32)
    value_parts = jnp.einsum("bqk,bqc->bkc", probs_bf, grad_blocks, preferred_element_type=f32)
    kv_parts = jnp.concatenate([key_parts, value_parts], axis=2)
    before_own, after_own = kv_parts[0, :group_rows], kv_parts[0, group_rows:]
    before_other, after_other = kv_parts[1, :group_rows], kv_parts[1, group_rows:]
    from_later = send(jnp.where(first, before_own, before_other), "fsdp", to_prev)
    kv_grad = jnp.concatenate(
        [
            after_own + jnp.where(first, before_other, from_later),
            after_other + jnp.where(first, from_later, before_own),
        ],
        axis=0,
    )
    qkv_grad32 = jnp.concatenate(
        [
            rotate(query_grad[:, None, :], cosines, sines, -1.0)[:, 0],
            rotate(kv_grad[:, None, :head_dim], cosines, sines, -1.0)[:, 0],
            kv_grad[:, head_dim:],
        ],
        axis=-1,
    )
    qkv_grad = qkv_grad32.astype(bf16)
    qkv_bias_part = jnp.sum(qkv_grad32, axis=0)
    qd_halves = reduce_features([xa, dy_all], [qkv_grad, attended])

    branch_part = contract_cols(attended, full_dense) + contract_cols(activated, full_contract)
    branch_sum = reduce_tokens(branch_part)
    output = relative_features(
        x_rel.astype(f32) + branch_sum + vectors[4] + vectors[5], chip
    )
    attn_back = contract_cols(qkv_grad, full_qkv)
    mlp_back = contract_cols(pre_grad, full_expand)
    weighted = reduce_tokens(attn_back * vectors[0] + mlp_back * vectors[2])
    xhat_own, inverse_own = xhat[:shard_rows], inverse_deviation[:shard_rows]
    input_gradient = dy_rel.astype(f32) + inverse_own * (
        weighted
        - jnp.mean(weighted, axis=-1, keepdims=True)
        - xhat_own * jnp.mean(weighted * xhat_own, axis=-1, keepdims=True)
    )
    block_input_gradient = relative_features(input_gradient, chip)

    vector_part = relative_features(
        jnp.stack(
            [
                jnp.sum(attn_back * xhat, axis=0),
                jnp.sum(attn_back, axis=0),
                jnp.sum(mlp_back * xhat, axis=0),
                jnp.sum(mlp_back, axis=0),
                jnp.sum(dy_rel.astype(f32), axis=0),
            ]
        ),
        chip,
    )
    bias_part = jnp.concatenate([qkv_bias_part, expand_bias_part])
    n_vector = vector_part.size
    small = jnp.concatenate([vector_part.reshape(-1), bias_part]).reshape(-1, 128)
    small = small + send(small, "fsdp", to_x)
    small = small + send(small, "fsdp", to_y)
    small_other = send(small, "fsdp", to_core)
    flat, flat_other = small.reshape(-1), small_other.reshape(-1)
    vector_sum = (flat[:n_vector] + flat_other[:n_vector]).reshape(-1, 128)
    for bit in (1, 2):
        vector_sum = vector_sum + send(
            vector_sum, "tensor", [(i, i ^ bit) for i in range(n_z)]
        )
    vector_sum = vector_sum.reshape(vector_part.shape)
    grad_norm_vectors = jnp.concatenate([vector_sum, vector_sum[4:]], axis=0)
    bias_first = jnp.where(first, flat[n_vector:], flat_other[n_vector:])
    bias_second = jnp.where(first, flat_other[n_vector:], flat[n_vector:])
    grad_qkv_bias = jnp.stack([bias_first[:qkv_cols], bias_second[:qkv_cols]])
    grad_expand_bias = jnp.concatenate([bias_first[qkv_cols:], bias_second[qkv_cols:]])

    grad_contract_weight = jnp.concatenate(contract_halves, axis=1)
    grad_expand_weight = jnp.concatenate(expand_halves, axis=1)
    grad_qkv_weight = jnp.stack([part[:, :qkv_cols] for part in qd_halves], axis=1)
    grad_dense_weight = jnp.concatenate([part[:, qkv_cols:] for part in qd_halves], axis=1)
    new_qkv_weight, new_moment_qkv_weight, new_second_qkv_weight = adam_step(
        qkv_weight,
        grad_qkv_weight,
        moment_qkv_weight,
        second_qkv_weight,
        rate_qkv_weight,
        decay_matrix,
    )
    new_qkv_bias, new_moment_qkv_bias, new_second_qkv_bias = adam_step(
        qkv_bias, grad_qkv_bias, moment_qkv_bias, second_qkv_bias, rate_qkv_bias, 0.0
    )
    new_dense_weight, new_moment_dense_weight, new_second_dense_weight = adam_step(
        dense_weight,
        grad_dense_weight,
        moment_dense_weight,
        second_dense_weight,
        rate_dense_weight,
        decay_matrix,
    )
    new_expand_weight, new_moment_expand_weight, new_second_expand_weight = adam_step(
        expand_weight,
        grad_expand_weight,
        moment_expand_weight,
        second_expand_weight,
        rate_expand_weight,
        decay_matrix,
    )
    new_expand_bias, new_moment_expand_bias, new_second_expand_bias = adam_step(
        expand_bias, grad_expand_bias, moment_expand_bias, second_expand_bias, rate_expand_bias, 0.0
    )
    new_contract_weight, new_moment_contract_weight, new_second_contract_weight = adam_step(
        contract_weight,
        grad_contract_weight,
        moment_contract_weight,
        second_contract_weight,
        rate_contract_weight,
        decay_matrix,
    )
    new_norm_vectors, new_moment_norm_vectors, new_second_norm_vectors = adam_step(
        norm_bias_vectors,
        grad_norm_vectors,
        moment_norm_vectors,
        second_norm_vectors,
        rate_norm_vectors,
        0.0,
    )
    return (
        output,
        block_input_gradient,
        grad_qkv_weight,
        new_qkv_weight,
        new_moment_qkv_weight,
        new_second_qkv_weight,
        grad_qkv_bias,
        new_qkv_bias,
        new_moment_qkv_bias,
        new_second_qkv_bias,
        grad_dense_weight,
        new_dense_weight,
        new_moment_dense_weight,
        new_second_dense_weight,
        grad_expand_weight,
        new_expand_weight,
        new_moment_expand_weight,
        new_second_expand_weight,
        grad_expand_bias,
        new_expand_bias,
        new_moment_expand_bias,
        new_second_expand_bias,
        grad_contract_weight,
        new_contract_weight,
        new_moment_contract_weight,
        new_second_contract_weight,
        grad_norm_vectors,
        new_norm_vectors,
        new_moment_norm_vectors,
        new_second_norm_vectors,
    )


def solution(mesh):
    paired = mesh.shape["fsdp"] == 8 and mesh.shape["tensor"] == 4
    per_device = per_device_paired if paired else per_device_generic
    return jax.shard_map(
        per_device,
        mesh=mesh,
        in_specs=(
            P(("fsdp", "tensor"), None),
            P(("fsdp", "tensor"), None),
            P(),
            P("fsdp"),
            P("fsdp", "tensor", None),
            P("tensor", None),
            P("fsdp", "tensor"),
            P("fsdp", "tensor"),
            P("tensor"),
            P("fsdp", "tensor"),
            P(),
            P("fsdp", "tensor", None),
            P("tensor", None),
            P("fsdp", "tensor"),
            P("fsdp", "tensor"),
            P("tensor"),
            P("fsdp", "tensor"),
            P(),
            P("fsdp", "tensor", None),
            P("tensor", None),
            P("fsdp", "tensor"),
            P("fsdp", "tensor"),
            P("tensor"),
            P("fsdp", "tensor"),
            P(),
        ),
        out_specs=(
            P(("fsdp", "tensor"), None),
            P(("fsdp", "tensor"), None),
            P("fsdp", "tensor", None),
            P("fsdp", "tensor", None),
            P("fsdp", "tensor", None),
            P("fsdp", "tensor", None),
            P("tensor", None),
            P("tensor", None),
            P("tensor", None),
            P("tensor", None),
            P("fsdp", "tensor"),
            P("fsdp", "tensor"),
            P("fsdp", "tensor"),
            P("fsdp", "tensor"),
            P("fsdp", "tensor"),
            P("fsdp", "tensor"),
            P("fsdp", "tensor"),
            P("fsdp", "tensor"),
            P("tensor"),
            P("tensor"),
            P("tensor"),
            P("tensor"),
            P("fsdp", "tensor"),
            P("fsdp", "tensor"),
            P("fsdp", "tensor"),
            P("fsdp", "tensor"),
            P(),
            P(),
            P(),
            P(),
        ),
        check_vma=False,
    )
```

```python
import jax
import jax.numpy as jnp
from jax import lax
from jax.experimental import pallas as pl
from jax.experimental.pallas import tpu as pltpu
from jax.sharding import PartitionSpec as P

ROT = 64
STEP = 3


norm_eps = 1e-05
masked_score = -1e30
beta_one = 0.9
beta_two = 0.95
adam_eps = 1e-08
decay_matrix = 0.01
rate_qkv_weight = 0.005
rate_qkv_bias = 0.02
rate_dense_weight = 0.04
rate_expand_weight = 0.005
rate_expand_bias = 0.02
rate_contract_weight = 0.003
rate_norm_vectors = 0.1


def shifted(value, axis, steps):
    count = lax.axis_size(axis)
    first, last = (max(0, -steps), min(count, count - steps))
    return lax.ppermute(value, axis, [(source, source + steps) for source in range(first, last)])


def normalized_row_block(row_values):
    center = row_values - jnp.mean(row_values, axis=-1, keepdims=True)
    variance = jnp.mean(center * center, axis=-1, keepdims=True)
    inverse_deviation = lax.rsqrt(variance + norm_eps)
    return (center * inverse_deviation, inverse_deviation)


def norm_backward_term(upstream_gradient, gain_vector_row, centered_normalized, inverse_deviation):
    scaled_rows = upstream_gradient * gain_vector_row
    return inverse_deviation * (
        scaled_rows
        - jnp.mean(scaled_rows, axis=-1, keepdims=True)
        - centered_normalized * jnp.mean(scaled_rows * centered_normalized, axis=-1, keepdims=True)
    )


def rotary_tables(token_pos):
    half_rot = ROT // 2
    frequency = 10000.0 ** (-(jnp.arange(half_rot, dtype=jnp.float32) * 2.0 / ROT))
    angles = token_pos.astype(jnp.float32)[:, None] * frequency[None, :]
    return (jnp.cos(angles)[:, None, :], jnp.sin(angles)[:, None, :])


def rotate(head_values, cosine_rotation, sine_rotation_table, direction):
    half_rot = ROT // 2
    first_half = head_values[..., :half_rot]
    second_half = head_values[..., half_rot:ROT]
    return jnp.concatenate(
        [
            first_half * cosine_rotation - direction * second_half * sine_rotation_table,
            second_half * cosine_rotation + direction * first_half * sine_rotation_table,
            head_values[..., ROT:],
        ],
        axis=-1,
    )


def gelu_slope(pre_values):
    return (
        0.5 * (1.0 + lax.erf(pre_values * 0.7071067811865476))
        + pre_values * jnp.exp(-0.5 * pre_values * pre_values) * 0.3989422804014327
    )


def key_mask(seg_query, query_index, seg_keys, group_rows, has_prev):
    key_index = jnp.arange(seg_keys.shape[0], dtype=jnp.int32)
    causal = key_index[None, :] <= query_index[:, None]
    same_doc = seg_keys[None, :] == seg_query[:, None]
    present = (key_index[None, :] >= group_rows) | has_prev
    return causal & same_doc & present


def block_scores(query_blk, keys_all, allowed, score_scale):
    scores = (
        jnp.einsum("qhc,khc->hqk", query_blk, keys_all, preferred_element_type=jnp.float32)
        * score_scale
    )
    return jnp.where(allowed[None], scores, masked_score)


def adam_step(parameter, gradient, moment, second, step_rate, decay_weight):
    moment_new = beta_one * moment + (1.0 - beta_one) * gradient
    second_new = beta_two * second + (1.0 - beta_two) * gradient * gradient
    moment_hat = moment_new / (1.0 - beta_one**STEP)
    second_hat = second_new / (1.0 - beta_two**STEP)
    updated = parameter - step_rate * (
        moment_hat / (jnp.sqrt(second_hat) + adam_eps) + decay_weight * parameter
    )
    return (updated, moment_new, second_new)


def contract_rows(left_rows, right_rows):
    return lax.dot_general(
        left_rows, right_rows, (((0,), (0,)), ((), ())), preferred_element_type=jnp.float32
    )


def contract_cols(left_cols, right_cols):
    return lax.dot_general(
        left_cols, right_cols, (((1,), (1,)), ((), ())), preferred_element_type=jnp.float32
    )


def per_device_generic(
    inputs,
    cotangent,
    segments,
    positions,
    qkv_weight,
    qkv_bias,
    dense_weight,
    expand_weight,
    expand_bias,
    contract_weight,
    norm_bias_vectors,
    moment_qkv_weight,
    moment_qkv_bias,
    moment_dense_weight,
    moment_expand_weight,
    moment_expand_bias,
    moment_contract_weight,
    moment_norm_vectors,
    second_qkv_weight,
    second_qkv_bias,
    second_dense_weight,
    second_expand_weight,
    second_expand_bias,
    second_contract_weight,
    second_norm_vectors,
):
    fsdp_index = lax.axis_index("fsdp")
    input_row_block, rows_dy = (
        lax.all_gather(inputs, "tensor", axis=0, tiled=True),
        lax.all_gather(cotangent, "tensor", axis=0, tiled=True),
    )
    group_rows = input_row_block.shape[0]
    shards_bf = (
        qkv_weight.astype(jnp.bfloat16),
        dense_weight.astype(jnp.bfloat16),
        expand_weight.astype(jnp.bfloat16),
        contract_weight.astype(jnp.bfloat16),
    )
    forward_set = (
        lax.all_gather(shards_bf[0], "fsdp", axis=0, tiled=True),
        lax.all_gather(shards_bf[1], "fsdp", axis=0, tiled=True),
        lax.all_gather(shards_bf[2], "fsdp", axis=0, tiled=True),
        lax.all_gather(shards_bf[3], "fsdp", axis=0, tiled=True),
    )
    full_qkv, full_dense, full_expand, full_contract = forward_set
    row_centered_normalized, inverse_row_deviation = normalized_row_block(
        input_row_block.astype(jnp.float32)
    )
    attention_normalized_input = (
        row_centered_normalized * norm_bias_vectors[0] + norm_bias_vectors[1]
    ).astype(jnp.bfloat16)
    feedforward_normalized_input = (
        row_centered_normalized * norm_bias_vectors[2] + norm_bias_vectors[3]
    ).astype(jnp.bfloat16)
    projected = (
        jnp.einsum(
            "rd,dhc->rhc", attention_normalized_input, full_qkv, preferred_element_type=jnp.float32
        )
        + qkv_bias[None]
    )
    heads_dev = projected.shape[1]
    head_dim = projected.shape[2] // 3
    score_scale = head_dim ** (-0.5)
    cosine_rotation, sine_rotation_table = rotary_tables(positions)
    query_rows = rotate(
        projected[..., :head_dim], cosine_rotation, sine_rotation_table, 1.0
    ).astype(jnp.bfloat16)
    local_segment_keys = rotate(
        projected[..., head_dim : 2 * head_dim], cosine_rotation, sine_rotation_table, 1.0
    ).astype(jnp.bfloat16)
    local_segment_values = projected[..., 2 * head_dim :].astype(jnp.bfloat16)
    keys_prev, values_prev = shifted((local_segment_keys, local_segment_values), "fsdp", 1)
    keys_all = jnp.concatenate([keys_prev, local_segment_keys], axis=0)
    values_all = jnp.concatenate([values_prev, local_segment_values], axis=0)
    seg_own = lax.dynamic_slice_in_dim(segments, fsdp_index * group_rows, group_rows)
    seg_prev = lax.dynamic_slice_in_dim(
        segments, jnp.maximum(fsdp_index - 1, 0) * group_rows, group_rows
    )
    seg_keys = jnp.concatenate([seg_prev, seg_own], axis=0)
    has_prev = fsdp_index > 0
    block_rows = min(512, group_rows)
    blocks = group_rows // block_rows
    starts = jnp.arange(blocks, dtype=jnp.int32) * block_rows
    local_index = jnp.arange(block_rows, dtype=jnp.int32)
    query_blocks = query_rows.reshape(blocks, block_rows, heads_dev, head_dim)
    seg_blocks = seg_own.reshape(blocks, block_rows)

    def forward_block(block_data):
        query_blk, seg_blk, start = block_data
        allowed = key_mask(
            seg_blk, group_rows + start + local_index, seg_keys, group_rows, has_prev
        )
        scores = block_scores(query_blk, keys_all, allowed, score_scale)
        row_max = jnp.max(scores, axis=-1, keepdims=True)
        row_total = jnp.sum(jnp.exp(scores - row_max), axis=-1, keepdims=True)
        log_total = row_max + jnp.log(row_total)
        prob_bf = jnp.exp(scores - log_total).astype(jnp.bfloat16)
        result = jnp.einsum("hqk,khc->qhc", prob_bf, values_all, preferred_element_type=jnp.float32)
        return (result.astype(jnp.bfloat16), log_total[..., 0])

    attn_blocks, lse_blocks = lax.map(forward_block, (query_blocks, seg_blocks, starts))
    attended = attn_blocks.reshape(group_rows, heads_dev * head_dim)
    expand_preactivation = (
        jnp.dot(feedforward_normalized_input, full_expand, preferred_element_type=jnp.float32)
        + expand_bias
    )
    gelu_activated_rows = jax.nn.gelu(expand_preactivation, approximate=False).astype(jnp.bfloat16)
    branch_sum = lax.psum_scatter(
        contract_cols(attended, full_dense) + contract_cols(gelu_activated_rows, full_contract),
        "tensor",
        scatter_dimension=0,
        tiled=True,
    )
    output = inputs.astype(jnp.float32) + branch_sum + norm_bias_vectors[4] + norm_bias_vectors[5]
    back_qkv, back_dense, back_expand, back_contract = forward_set
    act_grad = jnp.dot(rows_dy, back_contract, preferred_element_type=jnp.float32)
    pre_grad32 = act_grad * gelu_slope(expand_preactivation)
    pre_grad = pre_grad32.astype(jnp.bfloat16)
    attn_grad = jnp.dot(rows_dy, back_dense, preferred_element_type=jnp.float32).astype(
        jnp.bfloat16
    )
    attn_heads = attn_grad.reshape(group_rows, heads_dev, head_dim)
    row_delta = jnp.sum(
        attn_heads.astype(jnp.float32)
        * attended.reshape(group_rows, heads_dev, head_dim).astype(jnp.float32),
        axis=-1,
    )

    def backward_block(inner_carry, block_data):
        key_acc, value_acc = inner_carry
        query_blk, seg_blk, start, grad_blk, delta_blk, lse_blk = block_data
        allowed = key_mask(
            seg_blk, group_rows + start + local_index, seg_keys, group_rows, has_prev
        )
        scores = block_scores(query_blk, keys_all, allowed, score_scale)
        prob_f32 = jnp.exp(scores - lse_blk[..., None])
        prob_bf = prob_f32.astype(jnp.bfloat16)
        dot_grad = jnp.einsum(
            "qhc,khc->hqk", grad_blk, values_all, preferred_element_type=jnp.float32
        )
        score_grad = (
            prob_f32 * (dot_grad - jnp.transpose(delta_blk)[..., None]) * score_scale
        ).astype(jnp.bfloat16)
        query_grad = jnp.einsum(
            "hqk,khc->qhc", score_grad, keys_all, preferred_element_type=jnp.float32
        )
        key_acc = key_acc + jnp.einsum(
            "hqk,qhc->khc", score_grad, query_blk, preferred_element_type=jnp.float32
        )
        value_acc = value_acc + jnp.einsum(
            "hqk,qhc->khc", prob_bf, grad_blk, preferred_element_type=jnp.float32
        )
        return ((key_acc, value_acc), query_grad)

    zero_keys = jnp.zeros((2 * group_rows, heads_dev, head_dim), jnp.float32)
    inner_final, query_grads = lax.scan(
        backward_block,
        (zero_keys, zero_keys),
        (
            query_blocks,
            seg_blocks,
            starts,
            attn_heads.reshape(blocks, block_rows, heads_dev, head_dim),
            row_delta.reshape(blocks, block_rows, heads_dev),
            lse_blocks,
        ),
    )
    key_acc, value_acc = inner_final
    later_key_grad, later_value_grad = shifted(
        (key_acc[:group_rows], value_acc[:group_rows]), "fsdp", -1
    )
    key_grad = key_acc[group_rows:] + later_key_grad
    value_grad = value_acc[group_rows:] + later_value_grad
    query_grad = query_grads.reshape(group_rows, heads_dev, head_dim)
    qkv_grad32 = jnp.concatenate(
        [
            rotate(query_grad, cosine_rotation, sine_rotation_table, -1.0),
            rotate(key_grad, cosine_rotation, sine_rotation_table, -1.0),
            value_grad,
        ],
        axis=-1,
    )
    qkv_grad = qkv_grad32.astype(jnp.bfloat16)
    attn_norm_grad = jnp.einsum(
        "rhc,dhc->rd", qkv_grad, back_qkv, preferred_element_type=jnp.float32
    )
    mlp_norm_grad = contract_cols(pre_grad, back_expand)
    qkv_part = jnp.einsum(
        "rd,rhc->dhc", attention_normalized_input, qkv_grad, preferred_element_type=jnp.float32
    )
    dense_part = contract_rows(rows_dy, attended)
    expand_part = contract_rows(feedforward_normalized_input, pre_grad)
    contract_part = contract_rows(rows_dy, gelu_activated_rows)
    local_centered_normalized, inverse_local_deviation = normalized_row_block(
        inputs.astype(jnp.float32)
    )
    dy_local = cotangent.astype(jnp.float32)
    dy_column_sum = jnp.sum(dy_local, axis=0)
    attention_backward_term, feedforward_backward_term = (
        lax.psum_scatter(attn_norm_grad, "tensor", scatter_dimension=0, tiled=True),
        lax.psum_scatter(mlp_norm_grad, "tensor", scatter_dimension=0, tiled=True),
    )
    block_input_gradient = (
        dy_local
        + norm_backward_term(
            attention_backward_term,
            norm_bias_vectors[0],
            local_centered_normalized,
            inverse_local_deviation,
        )
        + norm_backward_term(
            feedforward_backward_term,
            norm_bias_vectors[2],
            local_centered_normalized,
            inverse_local_deviation,
        )
    )
    vector_part = jnp.stack(
        [
            jnp.sum(attention_backward_term * local_centered_normalized, axis=0),
            jnp.sum(attention_backward_term, axis=0),
            jnp.sum(feedforward_backward_term * local_centered_normalized, axis=0),
            jnp.sum(feedforward_backward_term, axis=0),
            dy_column_sum,
            dy_column_sum,
        ]
    )
    qkv_bias_part = jnp.sum(qkv_grad32, axis=0)
    expand_bias_part = jnp.sum(pre_grad32, axis=0)
    grad_qkv_weight, grad_dense_weight, grad_expand_weight, grad_contract_weight = (
        lax.psum_scatter(qkv_part, "fsdp", scatter_dimension=0, tiled=True),
        lax.psum_scatter(dense_part, "fsdp", scatter_dimension=0, tiled=True),
        lax.psum_scatter(expand_part, "fsdp", scatter_dimension=0, tiled=True),
        lax.psum_scatter(contract_part, "fsdp", scatter_dimension=0, tiled=True),
    )
    grad_qkv_bias, grad_expand_bias, vector_fsdp = lax.psum(
        (qkv_bias_part, expand_bias_part, vector_part), "fsdp"
    )
    grad_norm_vectors = lax.psum(vector_fsdp, "tensor")
    new_qkv_weight, new_moment_qkv_weight, new_second_qkv_weight = adam_step(
        qkv_weight,
        grad_qkv_weight,
        moment_qkv_weight,
        second_qkv_weight,
        rate_qkv_weight,
        decay_matrix,
    )
    new_qkv_bias, new_moment_qkv_bias, new_second_qkv_bias = adam_step(
        qkv_bias, grad_qkv_bias, moment_qkv_bias, second_qkv_bias, rate_qkv_bias, 0.0
    )
    new_dense_weight, new_moment_dense_weight, new_second_dense_weight = adam_step(
        dense_weight,
        grad_dense_weight,
        moment_dense_weight,
        second_dense_weight,
        rate_dense_weight,
        decay_matrix,
    )
    new_expand_weight, new_moment_expand_weight, new_second_expand_weight = adam_step(
        expand_weight,
        grad_expand_weight,
        moment_expand_weight,
        second_expand_weight,
        rate_expand_weight,
        decay_matrix,
    )
    new_expand_bias, new_moment_expand_bias, new_second_expand_bias = adam_step(
        expand_bias, grad_expand_bias, moment_expand_bias, second_expand_bias, rate_expand_bias, 0.0
    )
    new_contract_weight, new_moment_contract_weight, new_second_contract_weight = adam_step(
        contract_weight,
        grad_contract_weight,
        moment_contract_weight,
        second_contract_weight,
        rate_contract_weight,
        decay_matrix,
    )
    new_norm_vectors, new_moment_norm_vectors, new_second_norm_vectors = adam_step(
        norm_bias_vectors,
        grad_norm_vectors,
        moment_norm_vectors,
        second_norm_vectors,
        rate_norm_vectors,
        0.0,
    )
    return (
        output,
        block_input_gradient,
        grad_qkv_weight,
        new_qkv_weight,
        new_moment_qkv_weight,
        new_second_qkv_weight,
        grad_qkv_bias,
        new_qkv_bias,
        new_moment_qkv_bias,
        new_second_qkv_bias,
        grad_dense_weight,
        new_dense_weight,
        new_moment_dense_weight,
        new_second_dense_weight,
        grad_expand_weight,
        new_expand_weight,
        new_moment_expand_weight,
        new_second_expand_weight,
        grad_expand_bias,
        new_expand_bias,
        new_moment_expand_bias,
        new_second_expand_bias,
        grad_contract_weight,
        new_contract_weight,
        new_moment_contract_weight,
        new_second_contract_weight,
        grad_norm_vectors,
        new_norm_vectors,
        new_moment_norm_vectors,
        new_second_norm_vectors,
    )


def send(value, axis, pairs):
    return lax.ppermute(value, axis, pairs)


def product(left, right):
    return jnp.dot(left, right, preferred_element_type=jnp.float32)


def shape_of(shape, dtype):
    return jax.ShapeDtypeStruct(shape, dtype)


def moved(arrays, index):
    count = index.shape[0]

    def body(index_ref, *refs):
        for source, target in zip(refs[: len(arrays)], refs[len(arrays) :]):
            target[...] = source[...]

    blocks = [(value.shape[0], value.shape[1] // count) for value in arrays]
    return pl.pallas_call(
        body,
        grid_spec=pltpu.PrefetchScalarGridSpec(
            num_scalar_prefetch=1,
            grid=(count,),
            in_specs=[pl.BlockSpec(block, lambda i, index_ref: (0, index_ref[i])) for block in blocks],
            out_specs=[pl.BlockSpec(block, lambda i, index_ref: (0, i)) for block in blocks],
        ),
        out_shape=[shape_of(value.shape, value.dtype) for value in arrays],
        name="moved",
    )(index, *arrays)


def normalized_tile(tile):
    row = tile.astype(jnp.float32)
    center = row - jnp.mean(row, axis=-1, keepdims=True)
    variance = jnp.mean(center * center, axis=-1, keepdims=True)
    return center * lax.rsqrt(variance + norm_eps)


def normed_inputs(x, vectors):
    rows, width = x.shape
    tile = 256

    def body(x_ref, vector_ref, attn_ref, mlp_ref):
        xhat = normalized_tile(x_ref[...])
        attn_ref[...] = (xhat * vector_ref[0:1] + vector_ref[1:2]).astype(jnp.bfloat16)
        mlp_ref[...] = (xhat * vector_ref[2:3] + vector_ref[3:4]).astype(jnp.bfloat16)

    spec = pl.BlockSpec((tile, width), lambda i: (i, 0))
    return pl.pallas_call(
        body,
        grid=(rows // tile,),
        in_specs=[spec, pl.BlockSpec(vectors.shape, lambda i: (0, 0))],
        out_specs=[spec, spec],
        out_shape=[shape_of(x.shape, jnp.bfloat16)] * 2,
        name="normed",
    )(x, vectors)


def gathered_product(left, pieces, extras, outputs, finish, live, name):
    tile = 256
    columns = pieces[0].shape[1]
    rows = left.shape[0]
    depth = left.shape[1]
    piece_rows = pieces[3].shape[0]

    def body(left_ref, block, from_x, from_y, top, bottom, *refs):
        weight_ref = refs[len(extras)]
        parts = (
            (block, 0),
            (from_x, 0),
            (from_y, 0),
            (top, 0),
            (block, 1),
            (from_y, 1),
            (from_x, 1),
            (bottom, 0),
        )
        for i, (part, half) in enumerate(parts):
            weight_ref[i * piece_rows : (i + 1) * piece_rows, :] = part[
                half * piece_rows : (half + 1) * piece_rows, :
            ]
        step = pl.program_id(0)

        @pl.when(step < live)
        def _():
            result = product(left_ref[...], weight_ref[...])
            finish(step, result, refs[: len(extras)], refs[len(extras) + 1 :])

    def spec_of(height, moves):
        if moves:
            return pl.BlockSpec((height, tile), lambda j: (0, jnp.minimum(j, live - 1)))
        return pl.BlockSpec((height, 128), lambda j: (0, 0))

    column_spec = lambda height: pl.BlockSpec((height, tile), lambda j: (0, j))
    return pl.pallas_call(
        body,
        grid=(columns // tile,),
        in_specs=[pl.BlockSpec((rows, depth), lambda j: (0, 0))]
        + [column_spec(piece.shape[0]) for piece in pieces]
        + [spec_of(extra.shape[0], moves) for extra, moves in extras],
        out_specs=[column_spec(depth)] + [spec_of(out.shape[0], True) for out in outputs],
        out_shape=[shape_of((depth, columns), left.dtype)] + outputs,
        name=name,
    )(left, *pieces, *[extra for extra, _ in extras])


def partner_lanes(head):
    half_rot = ROT // 2
    lane = lax.broadcasted_iota(jnp.int32, head.shape, 1)
    return jnp.where(
        lane < half_rot,
        pltpu.roll(head, head.shape[1] - half_rot, 1),
        pltpu.roll(head, half_rot, 1),
    )


def qkv_product(left, pieces, bias, cosines, sines):
    rows = left.shape[0]
    columns = bias.shape[1]

    def finish(step, result, extras, outs):
        bias_ref, cosine_ref, sine_ref = extras
        value = result + bias_ref[...]
        head = value[:, :128]
        turned = head * cosine_ref[...] + partner_lanes(head) * sine_ref[...]
        outs[0][:, :128] = jnp.where(step < 2, turned, head).astype(jnp.bfloat16)
        outs[0][:, 128:] = value[:, 128:].astype(jnp.bfloat16)

    return gathered_product(
        left,
        pieces,
        [(bias, True), (cosines, False), (sines, False)],
        [shape_of((rows, columns), jnp.bfloat16)],
        finish,
        3,
        "qkv",
    )


def expand_product(left, pieces, bias):
    shape = (left.shape[0], bias.shape[1])

    def finish(step, result, extras, outs):
        pre = result + extras[0][...]
        distribution = 0.5 * (1.0 + lax.erf(pre * 0.7071067811865476))
        outs[0][...] = (pre * distribution).astype(jnp.bfloat16)
        outs[1][...] = distribution + pre * jnp.exp(-0.5 * pre * pre) * 0.3989422804014327

    return gathered_product(
        left,
        pieces,
        [(bias, True)],
        [shape_of(shape, jnp.bfloat16), shape_of(shape, jnp.float32)],
        finish,
        4,
        "expand",
    )


def contract_product(left, pieces, slope):
    def finish(step, result, extras, outs):
        gradient = result * extras[0][...]
        outs[0][...] = gradient.astype(jnp.bfloat16)
        outs[1][...] = jnp.sum(gradient, axis=0, keepdims=True)

    return gathered_product(
        left,
        pieces,
        [(slope, True)],
        [shape_of(slope.shape, jnp.bfloat16), shape_of((1, slope.shape[1]), jnp.float32)],
        finish,
        4,
        "contract",
    )


def nt(left, right):
    return lax.dot_general(
        left, right, (((1,), (1,)), ((), ())), preferred_element_type=jnp.float32
    )


def attention_call(body, halo_of, operands, extras, outputs, name):
    qkv, halo, seg_rows, token_rows, seg_columns, token_columns, seg_halo, token_halo = operands
    rows = qkv.shape[0] // 2
    head = qkv.shape[1] // 3
    block = lambda column, flip: pl.BlockSpec(
        (rows, head), lambda b, h: ((1 - b) if flip else b, column)
    )
    column_vector = pl.BlockSpec((rows, 1), lambda b, h: (b, 0))
    row_vector = lambda flip: pl.BlockSpec((1, rows), lambda b, h: (0, (1 - b) if flip else b))
    fixed = lambda value: pl.BlockSpec(value.shape, lambda b, h: (0, 0))
    by_block = lambda value: pl.BlockSpec((rows, value.shape[1]), lambda b, h: (b, 0))
    return pl.pallas_call(
        body,
        grid_spec=pltpu.PrefetchScalarGridSpec(
            num_scalar_prefetch=1,
            grid=(2,),
            in_specs=[
                block(0, False),
                block(1, True),
                block(2, True),
                block(1, False),
                block(2, False),
                fixed(halo),
                column_vector,
                column_vector,
                row_vector(True),
                row_vector(True),
                row_vector(False),
                row_vector(False),
                fixed(seg_halo),
                fixed(token_halo),
            ]
            + [by_block(extra) for extra in extras],
            out_specs=[by_block(out) for out in outputs],
        ),
        out_shape=outputs,
        name=name,
    )(
        halo_of,
        qkv,
        qkv,
        qkv,
        qkv,
        qkv,
        halo,
        seg_columns,
        token_columns,
        seg_rows,
        token_rows,
        seg_rows,
        token_rows,
        seg_halo,
        token_halo,
        *extras,
    )


def masked_scores(halo_of, refs, score_scale):
    (
        q_ref,
        k_before,
        v_before,
        k_ref,
        v_ref,
        halo,
        seg_q,
        token_q,
        seg_before,
        token_before,
        seg_k,
        token_k,
        seg_halo,
        token_halo,
    ) = refs
    use_halo = halo_of[pl.program_id(0)] == 1
    head = q_ref.shape[1]
    keys_before = jnp.where(use_halo, halo[:, :head], k_before[...])
    values_before = jnp.where(use_halo, halo[:, head:], v_before[...])
    segments_before = jnp.where(use_halo, seg_halo[...], seg_before[...])
    tokens_before = jnp.where(use_halo, token_halo[...], token_before[...])
    query = q_ref[...]

    def scores(keys, key_segments, key_tokens):
        allowed = (key_segments == seg_q[...]) & (key_tokens <= token_q[...])
        return jnp.where(allowed, nt(query, keys) * score_scale, masked_score)

    return (
        query,
        (keys_before, k_ref[...]),
        (values_before, v_ref[...]),
        (
            scores(keys_before, segments_before, tokens_before),
            scores(k_ref[...], seg_k[...], token_k[...]),
        ),
    )


def attention_forward(halo_of, operands):
    rows, columns = operands[0].shape
    head = columns // 3
    score_scale = head ** (-0.5)

    def body(halo_ref, *refs):
        _, _, values, scores = masked_scores(halo_ref, refs[:14], score_scale)
        out_ref, lse_ref = refs[14:]
        row_max = jnp.maximum(
            jnp.max(scores[0], axis=-1, keepdims=True), jnp.max(scores[1], axis=-1, keepdims=True)
        )
        powers = [jnp.exp(part - row_max) for part in scores]
        total = jnp.sum(powers[0], axis=-1, keepdims=True) + jnp.sum(
            powers[1], axis=-1, keepdims=True
        )
        inverse = 1.0 / total
        out_ref[...] = (
            product((powers[0] * inverse).astype(jnp.bfloat16), values[0])
            + product((powers[1] * inverse).astype(jnp.bfloat16), values[1])
        ).astype(jnp.bfloat16)
        lse_ref[...] = row_max + jnp.log(total)

    return attention_call(
        body,
        halo_of,
        operands,
        [],
        [shape_of((rows, head), jnp.bfloat16), shape_of((rows, 1), jnp.float32)],
        "attention",
    )


def attention_backward(halo_of, operands, lse, attended, attn_grad):
    rows, columns = operands[0].shape
    head = columns // 3
    score_scale = head ** (-0.5)

    def body(halo_ref, *refs):
        query, keys, values, scores = masked_scores(halo_ref, refs[:14], score_scale)
        lse_ref, attended_ref, grad_ref, query_out, before_out, own_out = refs[14:]
        gradient = grad_ref[...]
        row_delta = jnp.sum(
            gradient.astype(jnp.float32) * attended_ref[...].astype(jnp.float32),
            axis=-1,
            keepdims=True,
        )
        query_grad = 0.0
        for part, out in enumerate((before_out, own_out)):
            probs = jnp.exp(scores[part] - lse_ref[...])
            score_grad = (
                probs * (nt(gradient, values[part]) - row_delta) * score_scale
            ).astype(jnp.bfloat16)
            query_grad = query_grad + product(score_grad, keys[part])
            out[:, :head] = contract_rows(score_grad, query)
            out[:, head:] = contract_rows(probs.astype(jnp.bfloat16), gradient)
        query_out[...] = query_grad

    return attention_call(
        body,
        halo_of,
        operands,
        [lse, attended, attn_grad],
        [
            shape_of((rows, head), jnp.float32),
            shape_of((rows, 2 * head), jnp.float32),
            shape_of((rows, 2 * head), jnp.float32),
        ],
        "attention_back",
    )


def rotated_back(later_of, query_grad, own_part, before_part, from_later, cosines, sines):
    rows = query_grad.shape[0] // 2
    head = query_grad.shape[1]

    def body(later_ref, query_ref, own_ref, before_ref, later_grad, cosine, sine, out, bias_out):
        step = pl.program_id(0)
        extra = jnp.where(later_ref[step] == 1, later_grad[...], before_ref[...])
        pairs = own_ref[...] + extra

        def back(value):
            lanes = value[:, :128]
            lanes = lanes * cosine[...] - partner_lanes(lanes) * sine[...]
            return jnp.concatenate([lanes, value[:, 128:]], axis=1)

        @pl.when(step == 0)
        def _():
            bias_out[...] = jnp.zeros_like(bias_out)

        parts = (back(query_ref[...]), back(pairs[:, :head]), pairs[:, head:])
        for i, part in enumerate(parts):
            columns = slice(i * head, (i + 1) * head)
            out[:, columns] = part.astype(jnp.bfloat16)
            bias_out[:, columns] += jnp.sum(part, axis=0, keepdims=True)

    by_block = lambda width: pl.BlockSpec((rows, width), lambda b, h: (b, 0))
    return pl.pallas_call(
        body,
        grid_spec=pltpu.PrefetchScalarGridSpec(
            num_scalar_prefetch=1,
            grid=(2,),
            in_specs=[
                by_block(head),
                by_block(2 * head),
                pl.BlockSpec((rows, 2 * head), lambda b, h: (1 - b, 0)),
                pl.BlockSpec((rows, 2 * head), lambda b, h: (0, 0)),
                by_block(128),
                by_block(128),
            ],
            out_specs=[by_block(3 * head), pl.BlockSpec((1, 3 * head), lambda b, h: (0, 0))],
        ),
        out_shape=[
            shape_of((2 * rows, 3 * head), jnp.bfloat16),
            shape_of((1, 3 * head), jnp.float32),
        ],
        name="rotated_back",
    )(later_of, query_grad, own_part, before_part, from_later, cosines, sines)


def branch_rows(half, attended, activated, weight_qd, weight_contract, dtype):
    rows = attended.shape[0] // 2
    tile = 512
    depth = weight_qd.shape[0]

    def body(attended_ref, activated_ref, dense_ref, contract_ref, out):
        out[...] = (
            nt(attended_ref[...], dense_ref[...]) + nt(activated_ref[...], contract_ref[...])
        ).astype(dtype)

    return pl.pallas_call(
        body,
        grid=(depth // tile,),
        in_specs=[
            pl.BlockSpec((rows, attended.shape[1]), lambda j: (half, 0)),
            pl.BlockSpec((rows, activated.shape[1]), lambda j: (half, 0)),
            pl.BlockSpec((tile, attended.shape[1]), lambda j: (j, 3)),
            pl.BlockSpec((tile, activated.shape[1]), lambda j: (j, 0)),
        ],
        out_specs=pl.BlockSpec((rows, tile), lambda j: (0, j)),
        out_shape=shape_of((rows, depth), dtype),
        name="branch_%d" % half,
    )(attended, activated, weight_qd, weight_contract)


def back_rows(half, qkv_grad, pre_grad, x, weight_qd, weight_expand, vectors, dtype):
    rows = x.shape[0] // 2
    tile = 512
    depth = x.shape[1]

    def body(qkv_ref, pre_ref, x_ref, tile_ref, qd_ref, expand_ref, vector_ref, out, sums, stats):
        @pl.when(pl.program_id(0) == 0)
        def _():
            row = x_ref[...].astype(jnp.float32)
            mean = jnp.mean(row, axis=-1, keepdims=True)
            center = row - mean
            variance = jnp.mean(center * center, axis=-1, keepdims=True)
            stats[0] = jnp.broadcast_to(mean, stats.shape[1:])
            stats[1] = jnp.broadcast_to(lax.rsqrt(variance + norm_eps), stats.shape[1:])

        xhat = (tile_ref[...].astype(jnp.float32) - stats[0][:, :1]) * stats[1][:, :1]
        attn_back = nt(qkv_ref[...], qd_ref[...])
        mlp_back = nt(pre_ref[...], expand_ref[...])
        sums[0:1] = jnp.sum(attn_back * xhat, axis=0, keepdims=True)
        sums[1:2] = jnp.sum(attn_back, axis=0, keepdims=True)
        sums[2:3] = jnp.sum(mlp_back * xhat, axis=0, keepdims=True)
        sums[3:4] = jnp.sum(mlp_back, axis=0, keepdims=True)
        out[...] = (attn_back * vector_ref[0:1] + mlp_back * vector_ref[2:3]).astype(dtype)

    return pl.pallas_call(
        body,
        grid=(depth // tile,),
        in_specs=[
            pl.BlockSpec((rows, qkv_grad.shape[1]), lambda j: (half, 0)),
            pl.BlockSpec((rows, pre_grad.shape[1]), lambda j: (half, 0)),
            pl.BlockSpec((rows, depth), lambda j: (half, 0)),
            pl.BlockSpec((rows, tile), lambda j: (half, j)),
            pl.BlockSpec((tile, qkv_grad.shape[1]), lambda j: (j, 0)),
            pl.BlockSpec((tile, pre_grad.shape[1]), lambda j: (j, 0)),
            pl.BlockSpec((vectors.shape[0], tile), lambda j: (0, j)),
        ],
        out_specs=[
            pl.BlockSpec((rows, tile), lambda j: (0, j)),
            pl.BlockSpec((4, tile), lambda j: (0, j)),
        ],
        out_shape=[shape_of((rows, depth), dtype), shape_of((4, depth), jnp.float32)],
        scratch_shapes=[pltpu.VMEM((2, rows, 128), jnp.float32)],
        name="back_%d" % half,
    )(qkv_grad, pre_grad, x, x, weight_qd, weight_expand, vectors)


def tied(value, *others):
    return lax.optimization_barrier((value,) + others)[0]


def picked(values, index):
    rows = jnp.arange(values.shape[0], dtype=jnp.int32)
    chosen = index[:, None, None] == rows[None, :, None]
    return jnp.sum(jnp.where(chosen, values[None], 0), axis=1)


def per_device_paired(
    inputs,
    cotangent,
    segments,
    positions,
    qkv_weight,
    qkv_bias,
    dense_weight,
    expand_weight,
    expand_bias,
    contract_weight,
    norm_bias_vectors,
    moment_qkv_weight,
    moment_qkv_bias,
    moment_dense_weight,
    moment_expand_weight,
    moment_expand_bias,
    moment_contract_weight,
    moment_norm_vectors,
    second_qkv_weight,
    second_qkv_bias,
    second_dense_weight,
    second_expand_weight,
    second_expand_bias,
    second_contract_weight,
    second_norm_vectors,
):
    bf16, f32 = jnp.bfloat16, jnp.float32
    fsdp_index = lax.axis_index("fsdp")
    z = lax.axis_index("tensor")
    n_z = lax.axis_size("tensor")
    core = fsdp_index & 1
    chip = fsdp_index >> 1
    devices = range(lax.axis_size("fsdp"))
    to_core = [(i, i ^ 1) for i in devices]
    to_x = [(i, i ^ 2) for i in devices]
    to_y = [(i, i ^ 4) for i in devices]
    to_next = [(i, i + 2) for i in devices if i + 2 < len(devices)]
    to_prev = [(i + 2, i) for i in devices if i + 2 < len(devices)]
    first = core == 0
    head_dim = qkv_weight.shape[2] // 3
    shard_rows = inputs.shape[0]
    group_rows = n_z * shard_rows
    hidden = expand_weight.shape[1] // 2
    qkv_cols = 3 * head_dim
    shard_feat = expand_weight.shape[0]

    def column_half(weight, k, width):
        return lax.dynamic_slice_in_dim(weight, k * width, width, axis=1).astype(bf16)

    def head_columns(k):
        return jnp.concatenate(
            [
                lax.dynamic_index_in_dim(qkv_weight, k, axis=1, keepdims=False),
                lax.dynamic_slice_in_dim(dense_weight, k * head_dim, head_dim, axis=1),
            ],
            axis=1,
        ).astype(bf16)

    def rows_of_chip(own, other):
        return jnp.concatenate(
            [jnp.where(first, own, other), jnp.where(first, other, own)], axis=0
        )

    swapped = [
        send(head_columns(1 - core), "fsdp", to_core),
        send(column_half(expand_weight, 1 - core, hidden), "fsdp", to_core),
        send(column_half(contract_weight, 1 - core, hidden), "fsdp", to_core),
    ]
    own_blocks = [
        rows_of_chip(own, other)
        for own, other in zip(
            (
                head_columns(core),
                column_half(expand_weight, core, hidden),
                column_half(contract_weight, core, hidden),
            ),
            swapped,
        )
    ]

    def spread(block):
        return block, send(block, "fsdp", to_x), send(block, "fsdp", to_y)

    def relay(from_x, from_y):
        return (
            send(from_y[:shard_feat], "fsdp", to_x),
            send(from_x[shard_feat:], "fsdp", to_y),
        )

    def gather_tokens(own):
        pieces = [own]
        for k in range(1, n_z):
            pieces.append(send(own, "tensor", [(i, (i + k) % n_z) for i in range(n_z)]))
        group = jnp.concatenate(pieces, axis=0)
        return jnp.concatenate([group, send(group, "fsdp", to_core)], axis=0)

    places = jnp.arange(8, dtype=jnp.int32)
    rank = places & 3
    rank = jnp.where(places < 4, rank, 2 * (rank & 1) + (rank >> 1))
    feature_index = 2 * (chip ^ rank) + (places >> 2)
    x_rel, dy_rel, vectors = moved((inputs, cotangent, norm_bias_vectors), feature_index)
    spread_1 = spread(own_blocks[0])
    spread_2 = spread(own_blocks[1])
    relayed_1 = relay(spread_1[1], spread_1[2])
    spread_3 = spread(tied(own_blocks[2], spread_1[1], spread_1[2]))
    relayed_2 = relay(spread_2[1], spread_2[2])
    relayed_3 = relay(spread_3[1], spread_3[2])
    x_all = gather_tokens(x_rel)
    position_other = send(positions, "fsdp", to_core)

    _, segments_in, position_own, position_other = lax.optimization_barrier(
        (swapped[2], segments, positions, position_other)
    )
    local = jnp.arange(group_rows, dtype=jnp.int32)
    shard_of = (z - jnp.arange(n_z, dtype=jnp.int32)) & (n_z - 1)
    order = ((z - local // shard_rows) & (n_z - 1)) * shard_rows + local % shard_rows
    own_group = fsdp_index
    other_group = fsdp_index ^ 1
    halo_group = jnp.maximum(2 * chip - 1, 0)
    wanted = jnp.concatenate([g * n_z + shard_of for g in (own_group, other_group, halo_group)])
    seg_rows = picked(segments_in.reshape(-1, shard_rows), wanted).reshape(1, 3 * group_rows)
    seg_halo = jnp.where(chip == 0, -1, seg_rows[:, 2 * group_rows :])
    seg_rows = seg_rows[:, : 2 * group_rows]
    token_rows = jnp.concatenate(
        [order + own_group * group_rows, order + other_group * group_rows]
    ).reshape(1, 2 * group_rows)
    token_halo = (order + halo_group * group_rows).reshape(1, group_rows)
    position_rows = jnp.concatenate(
        [position_own.reshape(n_z, shard_rows), position_other.reshape(n_z, shard_rows)], axis=0
    )
    position_all = picked(
        position_rows, jnp.concatenate([shard_of, shard_of + n_z])
    ).reshape(2 * group_rows)
    lane = jnp.arange(128, dtype=jnp.int32)
    half_rot = ROT // 2
    frequency = 10000.0 ** (-((lane % half_rot).astype(f32) * 2.0 / ROT))
    angles = jnp.where(
        lane[None, :] < ROT, position_all.astype(f32)[:, None] * frequency[None, :], 0.0
    )
    cosines = jnp.cos(angles)
    sines = jnp.sin(angles) * jnp.where(lane < half_rot, -1.0, 1.0)[None, :]
    halo_of = jnp.stack([first, ~first]).astype(jnp.int32)
    later_of = 1 - halo_of

    xa, xm = normed_inputs(x_all, vectors)
    dy_all = gather_tokens(dy_rel)

    head_bias = lax.dynamic_slice_in_dim(qkv_bias, core, 1, axis=0)
    pieces_1 = lax.optimization_barrier((spread_1 + relayed_1, spread_2[1:]))[0]
    weight_qd, qkv = qkv_product(xa, pieces_1, head_bias, cosines, sines)
    kv_halo = send(
        jnp.where(first, qkv[group_rows:, head_dim:], qkv[:group_rows, head_dim:]), "fsdp", to_next
    )
    operands = (
        qkv,
        kv_halo,
        seg_rows,
        token_rows,
        seg_rows.reshape(2 * group_rows, 1),
        token_rows.reshape(2 * group_rows, 1),
        seg_halo,
        token_halo,
    )
    attended, lse = attention_forward(halo_of, operands)

    expand_bias_half = lax.dynamic_slice_in_dim(expand_bias, core * hidden, hidden).reshape(1, -1)
    pieces_2 = lax.optimization_barrier((spread_2 + relayed_2, spread_3[1:]))[0]
    weight_expand, activated, slope = expand_product(xm, pieces_2, expand_bias_half)

    def reduce_features(left, right):
        def rows(start, count):
            return contract_rows(left[:, start : start + count], right)

        got_a = send(rows(2 * shard_feat, 2 * shard_feat).astype(bf16), "fsdp", to_y)
        got_b = send(rows(6 * shard_feat, 2 * shard_feat).astype(bf16), "fsdp", to_x)
        pass_a = rows(shard_feat, shard_feat) + got_a[shard_feat:].astype(f32)
        pass_b = rows(5 * shard_feat, shard_feat) + got_b[shard_feat:].astype(f32)
        last_a = send(pass_a.astype(bf16), "fsdp", to_x)
        last_b = send(pass_b.astype(bf16), "fsdp", to_y)
        sum_a = rows(0, shard_feat) + got_a[:shard_feat].astype(f32) + last_a.astype(f32)
        sum_b = (
            rows(4 * shard_feat, shard_feat) + got_b[:shard_feat].astype(f32) + last_b.astype(f32)
        )
        taken = send(jnp.where(first, sum_b, sum_a), "fsdp", to_core)
        kept = jnp.where(first, sum_a, sum_b)
        return jnp.where(first, kept, taken), jnp.where(first, taken, kept)

    def over_tensor(rows):
        total = rows[:shard_rows]
        for k in range(1, n_z):
            piece = rows[k * shard_rows : (k + 1) * shard_rows].astype(bf16)
            total = total + send(
                piece, "tensor", [(i, (i - k) % n_z) for i in range(n_z)]
            ).astype(f32)
        return total

    dc_halves = reduce_features(dy_all, jnp.concatenate([attended, activated], axis=1))

    attn_grad = product(dy_all, weight_qd[:, qkv_cols:]).astype(bf16)
    query_grad, before_part, own_part = attention_backward(
        halo_of, operands, lse, attended, attn_grad
    )
    from_later = send(
        jnp.where(first, before_part[:group_rows], before_part[group_rows:]), "fsdp", to_prev
    )
    qkv_grad, qkv_bias_part = rotated_back(
        later_of, query_grad, own_part, before_part, from_later, cosines, sines
    )
    qkv_halves = reduce_features(xa, qkv_grad)

    weight_contract, pre_grad, expand_bias_part = contract_product(
        dy_all, spread_3 + relayed_3, slope
    )
    expand_halves = reduce_features(xm, pre_grad)

    rows_of = lambda half, dtype: branch_rows(
        half, attended, activated, weight_qd, weight_contract, dtype
    )
    branch_other = send(rows_of(1, bf16), "fsdp", to_core)
    branch_sum = over_tensor(rows_of(0, f32) + branch_other.astype(f32))
    output_rel = x_rel.astype(f32) + branch_sum + vectors[4] + vectors[5]

    backs = lambda half, dtype: back_rows(
        half, qkv_grad, pre_grad, x_all, weight_qd, weight_expand, vectors, dtype
    )
    weighted_other, sums_other = backs(1, bf16)
    weighted_other = send(weighted_other, "fsdp", to_core)
    weighted_own, sums_own = backs(0, f32)
    plain_index = jnp.sum(
        jnp.where(feature_index[None, :] == places[:, None], places[None, :], 0), axis=1
    )
    vector_part = jnp.concatenate(
        [sums_own + sums_other, jnp.sum(dy_rel.astype(f32), axis=0, keepdims=True)], axis=0
    )
    (vector_part,) = moved((vector_part,), plain_index)
    bias_part = jnp.concatenate([qkv_bias_part[0], expand_bias_part[0]])
    n_vector = vector_part.size
    small = jnp.concatenate([vector_part.reshape(-1), bias_part]).reshape(-1, 128)
    small = small + send(small, "fsdp", to_x)
    (output,) = moved((output_rel,), plain_index)
    weighted = over_tensor(tied(weighted_own + weighted_other.astype(f32), small))
    xhat_own, inverse_own = normalized_row_block(x_rel.astype(f32))
    input_gradient = dy_rel.astype(f32) + inverse_own * (
        weighted
        - jnp.mean(weighted, axis=-1, keepdims=True)
        - xhat_own * jnp.mean(weighted * xhat_own, axis=-1, keepdims=True)
    )
    (block_input_gradient,) = moved((input_gradient,), plain_index)

    small = small + send(small, "fsdp", to_y)
    small_other = send(small, "fsdp", to_core)
    flat, flat_other = small.reshape(-1), small_other.reshape(-1)
    vector_sum = (flat[:n_vector] + flat_other[:n_vector]).reshape(-1, 128)
    for bit in (1, 2):
        vector_sum = vector_sum + send(
            vector_sum, "tensor", [(i, i ^ bit) for i in range(n_z)]
        )
    vector_sum = vector_sum.reshape(vector_part.shape)
    grad_norm_vectors = jnp.concatenate([vector_sum, vector_sum[4:]], axis=0)
    bias_first = jnp.where(first, flat[n_vector:], flat_other[n_vector:])
    bias_second = jnp.where(first, flat_other[n_vector:], flat[n_vector:])
    grad_qkv_bias = jnp.stack([bias_first[:qkv_cols], bias_second[:qkv_cols]])
    grad_expand_bias = jnp.concatenate([bias_first[qkv_cols:], bias_second[qkv_cols:]])

    grad_contract_weight = jnp.concatenate([part[:, head_dim:] for part in dc_halves], axis=1)
    grad_dense_weight = jnp.concatenate([part[:, :head_dim] for part in dc_halves], axis=1)
    grad_expand_weight = jnp.concatenate(expand_halves, axis=1)
    grad_qkv_weight = jnp.stack(qkv_halves, axis=1)
    new_qkv_weight, new_moment_qkv_weight, new_second_qkv_weight = adam_step(
        qkv_weight,
        grad_qkv_weight,
        moment_qkv_weight,
        second_qkv_weight,
        rate_qkv_weight,
        decay_matrix,
    )
    new_qkv_bias, new_moment_qkv_bias, new_second_qkv_bias = adam_step(
        qkv_bias, grad_qkv_bias, moment_qkv_bias, second_qkv_bias, rate_qkv_bias, 0.0
    )
    new_dense_weight, new_moment_dense_weight, new_second_dense_weight = adam_step(
        dense_weight,
        grad_dense_weight,
        moment_dense_weight,
        second_dense_weight,
        rate_dense_weight,
        decay_matrix,
    )
    new_expand_weight, new_moment_expand_weight, new_second_expand_weight = adam_step(
        expand_weight,
        grad_expand_weight,
        moment_expand_weight,
        second_expand_weight,
        rate_expand_weight,
        decay_matrix,
    )
    new_expand_bias, new_moment_expand_bias, new_second_expand_bias = adam_step(
        expand_bias, grad_expand_bias, moment_expand_bias, second_expand_bias, rate_expand_bias, 0.0
    )
    new_contract_weight, new_moment_contract_weight, new_second_contract_weight = adam_step(
        contract_weight,
        grad_contract_weight,
        moment_contract_weight,
        second_contract_weight,
        rate_contract_weight,
        decay_matrix,
    )
    new_norm_vectors, new_moment_norm_vectors, new_second_norm_vectors = adam_step(
        norm_bias_vectors,
        grad_norm_vectors,
        moment_norm_vectors,
        second_norm_vectors,
        rate_norm_vectors,
        0.0,
    )
    return (
        output,
        block_input_gradient,
        grad_qkv_weight,
        new_qkv_weight,
        new_moment_qkv_weight,
        new_second_qkv_weight,
        grad_qkv_bias,
        new_qkv_bias,
        new_moment_qkv_bias,
        new_second_qkv_bias,
        grad_dense_weight,
        new_dense_weight,
        new_moment_dense_weight,
        new_second_dense_weight,
        grad_expand_weight,
        new_expand_weight,
        new_moment_expand_weight,
        new_second_expand_weight,
        grad_expand_bias,
        new_expand_bias,
        new_moment_expand_bias,
        new_second_expand_bias,
        grad_contract_weight,
        new_contract_weight,
        new_moment_contract_weight,
        new_second_contract_weight,
        grad_norm_vectors,
        new_norm_vectors,
        new_moment_norm_vectors,
        new_second_norm_vectors,
    )


def solution(mesh):
    paired = mesh.shape["fsdp"] == 8 and mesh.shape["tensor"] == 4
    per_device = per_device_paired if paired else per_device_generic
    return jax.shard_map(
        per_device,
        mesh=mesh,
        in_specs=(
            P(("fsdp", "tensor"), None),
            P(("fsdp", "tensor"), None),
            P(),
            P("fsdp"),
            P("fsdp", "tensor", None),
            P("tensor", None),
            P("fsdp", "tensor"),
            P("fsdp", "tensor"),
            P("tensor"),
            P("fsdp", "tensor"),
            P(),
            P("fsdp", "tensor", None),
            P("tensor", None),
            P("fsdp", "tensor"),
            P("fsdp", "tensor"),
            P("tensor"),
            P("fsdp", "tensor"),
            P(),
            P("fsdp", "tensor", None),
            P("tensor", None),
            P("fsdp", "tensor"),
            P("fsdp", "tensor"),
            P("tensor"),
            P("fsdp", "tensor"),
            P(),
        ),
        out_specs=(
            P(("fsdp", "tensor"), None),
            P(("fsdp", "tensor"), None),
            P("fsdp", "tensor", None),
            P("fsdp", "tensor", None),
            P("fsdp", "tensor", None),
            P("fsdp", "tensor", None),
            P("tensor", None),
            P("tensor", None),
            P("tensor", None),
            P("tensor", None),
            P("fsdp", "tensor"),
            P("fsdp", "tensor"),
            P("fsdp", "tensor"),
            P("fsdp", "tensor"),
            P("fsdp", "tensor"),
            P("fsdp", "tensor"),
            P("fsdp", "tensor"),
            P("fsdp", "tensor"),
            P("tensor"),
            P("tensor"),
            P("tensor"),
            P("tensor"),
            P("fsdp", "tensor"),
            P("fsdp", "tensor"),
            P("fsdp", "tensor"),
            P("fsdp", "tensor"),
            P(),
            P(),
            P(),
            P(),
        ),
        check_vma=False,
    )
```

```python
import jax
import jax.numpy as jnp
from jax import lax
from jax.experimental import pallas as pl
from jax.experimental.pallas import tpu as pltpu
from jax.sharding import PartitionSpec as P

ROT = 64
STEP = 3


norm_eps = 1e-05
masked_score = -1e30
beta_one = 0.9
beta_two = 0.95
adam_eps = 1e-08
decay_matrix = 0.01
rate_qkv_weight = 0.005
rate_qkv_bias = 0.02
rate_dense_weight = 0.04
rate_expand_weight = 0.005
rate_expand_bias = 0.02
rate_contract_weight = 0.003
rate_norm_vectors = 0.1


def shifted(value, axis, steps):
    count = lax.axis_size(axis)
    first, last = (max(0, -steps), min(count, count - steps))
    return lax.ppermute(value, axis, [(source, source + steps) for source in range(first, last)])


def normalized_row_block(row_values):
    center = row_values - jnp.mean(row_values, axis=-1, keepdims=True)
    variance = jnp.mean(center * center, axis=-1, keepdims=True)
    inverse_deviation = lax.rsqrt(variance + norm_eps)
    return (center * inverse_deviation, inverse_deviation)


def norm_backward_term(upstream_gradient, gain_vector_row, centered_normalized, inverse_deviation):
    scaled_rows = upstream_gradient * gain_vector_row
    return inverse_deviation * (
        scaled_rows
        - jnp.mean(scaled_rows, axis=-1, keepdims=True)
        - centered_normalized * jnp.mean(scaled_rows * centered_normalized, axis=-1, keepdims=True)
    )


def rotary_tables(token_pos):
    half_rot = ROT // 2
    frequency = 10000.0 ** (-(jnp.arange(half_rot, dtype=jnp.float32) * 2.0 / ROT))
    angles = token_pos.astype(jnp.float32)[:, None] * frequency[None, :]
    return (jnp.cos(angles)[:, None, :], jnp.sin(angles)[:, None, :])


def rotate(head_values, cosine_rotation, sine_rotation_table, direction):
    half_rot = ROT // 2
    first_half = head_values[..., :half_rot]
    second_half = head_values[..., half_rot:ROT]
    return jnp.concatenate(
        [
            first_half * cosine_rotation - direction * second_half * sine_rotation_table,
            second_half * cosine_rotation + direction * first_half * sine_rotation_table,
            head_values[..., ROT:],
        ],
        axis=-1,
    )


def gelu_slope(pre_values):
    return (
        0.5 * (1.0 + lax.erf(pre_values * 0.7071067811865476))
        + pre_values * jnp.exp(-0.5 * pre_values * pre_values) * 0.3989422804014327
    )


def key_mask(seg_query, query_index, seg_keys, group_rows, has_prev):
    key_index = jnp.arange(seg_keys.shape[0], dtype=jnp.int32)
    causal = key_index[None, :] <= query_index[:, None]
    same_doc = seg_keys[None, :] == seg_query[:, None]
    present = (key_index[None, :] >= group_rows) | has_prev
    return causal & same_doc & present


def block_scores(query_blk, keys_all, allowed, score_scale):
    scores = (
        jnp.einsum("qhc,khc->hqk", query_blk, keys_all, preferred_element_type=jnp.float32)
        * score_scale
    )
    return jnp.where(allowed[None], scores, masked_score)


def adam_step(parameter, gradient, moment, second, step_rate, decay_weight):
    moment_new = beta_one * moment + (1.0 - beta_one) * gradient
    second_new = beta_two * second + (1.0 - beta_two) * gradient * gradient
    moment_hat = moment_new / (1.0 - beta_one**STEP)
    second_hat = second_new / (1.0 - beta_two**STEP)
    updated = parameter - step_rate * (
        moment_hat / (jnp.sqrt(second_hat) + adam_eps) + decay_weight * parameter
    )
    return (updated, moment_new, second_new)


def contract_rows(left_rows, right_rows):
    return lax.dot_general(
        left_rows, right_rows, (((0,), (0,)), ((), ())), preferred_element_type=jnp.float32
    )


def contract_cols(left_cols, right_cols):
    return lax.dot_general(
        left_cols, right_cols, (((1,), (1,)), ((), ())), preferred_element_type=jnp.float32
    )


def per_device_generic(
    inputs,
    cotangent,
    segments,
    positions,
    qkv_weight,
    qkv_bias,
    dense_weight,
    expand_weight,
    expand_bias,
    contract_weight,
    norm_bias_vectors,
    moment_qkv_weight,
    moment_qkv_bias,
    moment_dense_weight,
    moment_expand_weight,
    moment_expand_bias,
    moment_contract_weight,
    moment_norm_vectors,
    second_qkv_weight,
    second_qkv_bias,
    second_dense_weight,
    second_expand_weight,
    second_expand_bias,
    second_contract_weight,
    second_norm_vectors,
):
    fsdp_index = lax.axis_index("fsdp")
    input_row_block, rows_dy = (
        lax.all_gather(inputs, "tensor", axis=0, tiled=True),
        lax.all_gather(cotangent, "tensor", axis=0, tiled=True),
    )
    group_rows = input_row_block.shape[0]
    shards_bf = (
        qkv_weight.astype(jnp.bfloat16),
        dense_weight.astype(jnp.bfloat16),
        expand_weight.astype(jnp.bfloat16),
        contract_weight.astype(jnp.bfloat16),
    )
    forward_set = (
        lax.all_gather(shards_bf[0], "fsdp", axis=0, tiled=True),
        lax.all_gather(shards_bf[1], "fsdp", axis=0, tiled=True),
        lax.all_gather(shards_bf[2], "fsdp", axis=0, tiled=True),
        lax.all_gather(shards_bf[3], "fsdp", axis=0, tiled=True),
    )
    full_qkv, full_dense, full_expand, full_contract = forward_set
    row_centered_normalized, inverse_row_deviation = normalized_row_block(
        input_row_block.astype(jnp.float32)
    )
    attention_normalized_input = (
        row_centered_normalized * norm_bias_vectors[0] + norm_bias_vectors[1]
    ).astype(jnp.bfloat16)
    feedforward_normalized_input = (
        row_centered_normalized * norm_bias_vectors[2] + norm_bias_vectors[3]
    ).astype(jnp.bfloat16)
    projected = (
        jnp.einsum(
            "rd,dhc->rhc", attention_normalized_input, full_qkv, preferred_element_type=jnp.float32
        )
        + qkv_bias[None]
    )
    heads_dev = projected.shape[1]
    head_dim = projected.shape[2] // 3
    score_scale = head_dim ** (-0.5)
    cosine_rotation, sine_rotation_table = rotary_tables(positions)
    query_rows = rotate(
        projected[..., :head_dim], cosine_rotation, sine_rotation_table, 1.0
    ).astype(jnp.bfloat16)
    local_segment_keys = rotate(
        projected[..., head_dim : 2 * head_dim], cosine_rotation, sine_rotation_table, 1.0
    ).astype(jnp.bfloat16)
    local_segment_values = projected[..., 2 * head_dim :].astype(jnp.bfloat16)
    keys_prev, values_prev = shifted((local_segment_keys, local_segment_values), "fsdp", 1)
    keys_all = jnp.concatenate([keys_prev, local_segment_keys], axis=0)
    values_all = jnp.concatenate([values_prev, local_segment_values], axis=0)
    seg_own = lax.dynamic_slice_in_dim(segments, fsdp_index * group_rows, group_rows)
    seg_prev = lax.dynamic_slice_in_dim(
        segments, jnp.maximum(fsdp_index - 1, 0) * group_rows, group_rows
    )
    seg_keys = jnp.concatenate([seg_prev, seg_own], axis=0)
    has_prev = fsdp_index > 0
    block_rows = min(512, group_rows)
    blocks = group_rows // block_rows
    starts = jnp.arange(blocks, dtype=jnp.int32) * block_rows
    local_index = jnp.arange(block_rows, dtype=jnp.int32)
    query_blocks = query_rows.reshape(blocks, block_rows, heads_dev, head_dim)
    seg_blocks = seg_own.reshape(blocks, block_rows)

    def forward_block(block_data):
        query_blk, seg_blk, start = block_data
        allowed = key_mask(
            seg_blk, group_rows + start + local_index, seg_keys, group_rows, has_prev
        )
        scores = block_scores(query_blk, keys_all, allowed, score_scale)
        row_max = jnp.max(scores, axis=-1, keepdims=True)
        row_total = jnp.sum(jnp.exp(scores - row_max), axis=-1, keepdims=True)
        log_total = row_max + jnp.log(row_total)
        prob_bf = jnp.exp(scores - log_total).astype(jnp.bfloat16)
        result = jnp.einsum("hqk,khc->qhc", prob_bf, values_all, preferred_element_type=jnp.float32)
        return (result.astype(jnp.bfloat16), log_total[..., 0])

    attn_blocks, lse_blocks = lax.map(forward_block, (query_blocks, seg_blocks, starts))
    attended = attn_blocks.reshape(group_rows, heads_dev * head_dim)
    expand_preactivation = (
        jnp.dot(feedforward_normalized_input, full_expand, preferred_element_type=jnp.float32)
        + expand_bias
    )
    gelu_activated_rows = jax.nn.gelu(expand_preactivation, approximate=False).astype(jnp.bfloat16)
    branch_sum = lax.psum_scatter(
        contract_cols(attended, full_dense) + contract_cols(gelu_activated_rows, full_contract),
        "tensor",
        scatter_dimension=0,
        tiled=True,
    )
    output = inputs.astype(jnp.float32) + branch_sum + norm_bias_vectors[4] + norm_bias_vectors[5]
    back_qkv, back_dense, back_expand, back_contract = forward_set
    act_grad = jnp.dot(rows_dy, back_contract, preferred_element_type=jnp.float32)
    pre_grad32 = act_grad * gelu_slope(expand_preactivation)
    pre_grad = pre_grad32.astype(jnp.bfloat16)
    attn_grad = jnp.dot(rows_dy, back_dense, preferred_element_type=jnp.float32).astype(
        jnp.bfloat16
    )
    attn_heads = attn_grad.reshape(group_rows, heads_dev, head_dim)
    row_delta = jnp.sum(
        attn_heads.astype(jnp.float32)
        * attended.reshape(group_rows, heads_dev, head_dim).astype(jnp.float32),
        axis=-1,
    )

    def backward_block(inner_carry, block_data):
        key_acc, value_acc = inner_carry
        query_blk, seg_blk, start, grad_blk, delta_blk, lse_blk = block_data
        allowed = key_mask(
            seg_blk, group_rows + start + local_index, seg_keys, group_rows, has_prev
        )
        scores = block_scores(query_blk, keys_all, allowed, score_scale)
        prob_f32 = jnp.exp(scores - lse_blk[..., None])
        prob_bf = prob_f32.astype(jnp.bfloat16)
        dot_grad = jnp.einsum(
            "qhc,khc->hqk", grad_blk, values_all, preferred_element_type=jnp.float32
        )
        score_grad = (
            prob_f32 * (dot_grad - jnp.transpose(delta_blk)[..., None]) * score_scale
        ).astype(jnp.bfloat16)
        query_grad = jnp.einsum(
            "hqk,khc->qhc", score_grad, keys_all, preferred_element_type=jnp.float32
        )
        key_acc = key_acc + jnp.einsum(
            "hqk,qhc->khc", score_grad, query_blk, preferred_element_type=jnp.float32
        )
        value_acc = value_acc + jnp.einsum(
            "hqk,qhc->khc", prob_bf, grad_blk, preferred_element_type=jnp.float32
        )
        return ((key_acc, value_acc), query_grad)

    zero_keys = jnp.zeros((2 * group_rows, heads_dev, head_dim), jnp.float32)
    inner_final, query_grads = lax.scan(
        backward_block,
        (zero_keys, zero_keys),
        (
            query_blocks,
            seg_blocks,
            starts,
            attn_heads.reshape(blocks, block_rows, heads_dev, head_dim),
            row_delta.reshape(blocks, block_rows, heads_dev),
            lse_blocks,
        ),
    )
    key_acc, value_acc = inner_final
    later_key_grad, later_value_grad = shifted(
        (key_acc[:group_rows], value_acc[:group_rows]), "fsdp", -1
    )
    key_grad = key_acc[group_rows:] + later_key_grad
    value_grad = value_acc[group_rows:] + later_value_grad
    query_grad = query_grads.reshape(group_rows, heads_dev, head_dim)
    qkv_grad32 = jnp.concatenate(
        [
            rotate(query_grad, cosine_rotation, sine_rotation_table, -1.0),
            rotate(key_grad, cosine_rotation, sine_rotation_table, -1.0),
            value_grad,
        ],
        axis=-1,
    )
    qkv_grad = qkv_grad32.astype(jnp.bfloat16)
    attn_norm_grad = jnp.einsum(
        "rhc,dhc->rd", qkv_grad, back_qkv, preferred_element_type=jnp.float32
    )
    mlp_norm_grad = contract_cols(pre_grad, back_expand)
    qkv_part = jnp.einsum(
        "rd,rhc->dhc", attention_normalized_input, qkv_grad, preferred_element_type=jnp.float32
    )
    dense_part = contract_rows(rows_dy, attended)
    expand_part = contract_rows(feedforward_normalized_input, pre_grad)
    contract_part = contract_rows(rows_dy, gelu_activated_rows)
    local_centered_normalized, inverse_local_deviation = normalized_row_block(
        inputs.astype(jnp.float32)
    )
    dy_local = cotangent.astype(jnp.float32)
    dy_column_sum = jnp.sum(dy_local, axis=0)
    attention_backward_term, feedforward_backward_term = (
        lax.psum_scatter(attn_norm_grad, "tensor", scatter_dimension=0, tiled=True),
        lax.psum_scatter(mlp_norm_grad, "tensor", scatter_dimension=0, tiled=True),
    )
    block_input_gradient = (
        dy_local
        + norm_backward_term(
            attention_backward_term,
            norm_bias_vectors[0],
            local_centered_normalized,
            inverse_local_deviation,
        )
        + norm_backward_term(
            feedforward_backward_term,
            norm_bias_vectors[2],
            local_centered_normalized,
            inverse_local_deviation,
        )
    )
    vector_part = jnp.stack(
        [
            jnp.sum(attention_backward_term * local_centered_normalized, axis=0),
            jnp.sum(attention_backward_term, axis=0),
            jnp.sum(feedforward_backward_term * local_centered_normalized, axis=0),
            jnp.sum(feedforward_backward_term, axis=0),
            dy_column_sum,
            dy_column_sum,
        ]
    )
    qkv_bias_part = jnp.sum(qkv_grad32, axis=0)
    expand_bias_part = jnp.sum(pre_grad32, axis=0)
    grad_qkv_weight, grad_dense_weight, grad_expand_weight, grad_contract_weight = (
        lax.psum_scatter(qkv_part, "fsdp", scatter_dimension=0, tiled=True),
        lax.psum_scatter(dense_part, "fsdp", scatter_dimension=0, tiled=True),
        lax.psum_scatter(expand_part, "fsdp", scatter_dimension=0, tiled=True),
        lax.psum_scatter(contract_part, "fsdp", scatter_dimension=0, tiled=True),
    )
    grad_qkv_bias, grad_expand_bias, vector_fsdp = lax.psum(
        (qkv_bias_part, expand_bias_part, vector_part), "fsdp"
    )
    grad_norm_vectors = lax.psum(vector_fsdp, "tensor")
    new_qkv_weight, new_moment_qkv_weight, new_second_qkv_weight = adam_step(
        qkv_weight,
        grad_qkv_weight,
        moment_qkv_weight,
        second_qkv_weight,
        rate_qkv_weight,
        decay_matrix,
    )
    new_qkv_bias, new_moment_qkv_bias, new_second_qkv_bias = adam_step(
        qkv_bias, grad_qkv_bias, moment_qkv_bias, second_qkv_bias, rate_qkv_bias, 0.0
    )
    new_dense_weight, new_moment_dense_weight, new_second_dense_weight = adam_step(
        dense_weight,
        grad_dense_weight,
        moment_dense_weight,
        second_dense_weight,
        rate_dense_weight,
        decay_matrix,
    )
    new_expand_weight, new_moment_expand_weight, new_second_expand_weight = adam_step(
        expand_weight,
        grad_expand_weight,
        moment_expand_weight,
        second_expand_weight,
        rate_expand_weight,
        decay_matrix,
    )
    new_expand_bias, new_moment_expand_bias, new_second_expand_bias = adam_step(
        expand_bias, grad_expand_bias, moment_expand_bias, second_expand_bias, rate_expand_bias, 0.0
    )
    new_contract_weight, new_moment_contract_weight, new_second_contract_weight = adam_step(
        contract_weight,
        grad_contract_weight,
        moment_contract_weight,
        second_contract_weight,
        rate_contract_weight,
        decay_matrix,
    )
    new_norm_vectors, new_moment_norm_vectors, new_second_norm_vectors = adam_step(
        norm_bias_vectors,
        grad_norm_vectors,
        moment_norm_vectors,
        second_norm_vectors,
        rate_norm_vectors,
        0.0,
    )
    return (
        output,
        block_input_gradient,
        grad_qkv_weight,
        new_qkv_weight,
        new_moment_qkv_weight,
        new_second_qkv_weight,
        grad_qkv_bias,
        new_qkv_bias,
        new_moment_qkv_bias,
        new_second_qkv_bias,
        grad_dense_weight,
        new_dense_weight,
        new_moment_dense_weight,
        new_second_dense_weight,
        grad_expand_weight,
        new_expand_weight,
        new_moment_expand_weight,
        new_second_expand_weight,
        grad_expand_bias,
        new_expand_bias,
        new_moment_expand_bias,
        new_second_expand_bias,
        grad_contract_weight,
        new_contract_weight,
        new_moment_contract_weight,
        new_second_contract_weight,
        grad_norm_vectors,
        new_norm_vectors,
        new_moment_norm_vectors,
        new_second_norm_vectors,
    )


def send(value, axis, pairs):
    return lax.ppermute(value, axis, pairs)


def product(left, right):
    return jnp.dot(left, right, preferred_element_type=jnp.float32)


small_cost = pl.CostEstimate(flops=1024, bytes_accessed=1024, transcendentals=0)


def shape_of(shape, dtype):
    return jax.ShapeDtypeStruct(shape, dtype)


def gathered_product(left, pieces, chip, extras, outputs, finish, live, name):
    tile = 256
    columns = pieces[0].shape[1]
    rows, depth = left.shape
    chip_rows = pieces[0].shape[0]
    half_rows = chip_rows // 2
    arrays = [pieces[0]] + [array for array, _ in pieces[1:]]
    starts = [0] + [start for _, start in pieces[1:]]

    def body(chip_ref, left_ref, block, from_x, from_y, top, bottom, *refs):
        weight_ref = refs[len(extras)]
        parts = (
            (block, 0, 0, chip_rows),
            (from_x, 1, 0, chip_rows),
            (from_y, 2, 0, chip_rows),
            (top, 3, 0, half_rows),
            (bottom, 3, half_rows, half_rows),
        )
        for (part, flip, shift, height), source in zip(parts, starts):
            start = pl.multiple_of((chip_ref[0] ^ flip) * chip_rows + shift, half_rows)
            weight_ref[pl.ds(start, height), :] = part[source : source + height, :]
        step = pl.program_id(0)

        @pl.when(step < live)
        def _():
            result = product(left_ref[...], weight_ref[...])
            finish(step, result, refs[: len(extras)], refs[len(extras) + 1 :])

    def spec_of(height, moves):
        if moves:
            return pl.BlockSpec((height, tile), lambda j, c: (0, jnp.minimum(j, live - 1)))
        return pl.BlockSpec((height, 128), lambda j, c: (0, 0))

    column_spec = lambda height: pl.BlockSpec((height, tile), lambda j, c: (0, j))
    return pl.pallas_call(
        body,
        cost_estimate=small_cost,
        grid_spec=pltpu.PrefetchScalarGridSpec(
            num_scalar_prefetch=1,
            grid=(columns // tile,),
            in_specs=[pl.BlockSpec((rows, depth), lambda j, c: (0, 0))]
            + [column_spec(array.shape[0]) for array in arrays]
            + [spec_of(extra.shape[0], moves) for extra, moves in extras],
            out_specs=[column_spec(depth)] + [spec_of(out.shape[0], True) for out in outputs],
        ),
        out_shape=[shape_of((depth, columns), left.dtype)] + outputs,
        name=name,
    )(chip.reshape(1), left, *arrays, *[extra for extra, _ in extras])


def partner_lanes(head):
    half_rot = ROT // 2
    lane = lax.broadcasted_iota(jnp.int32, head.shape, 1)
    return jnp.where(
        lane < half_rot,
        pltpu.roll(head, head.shape[1] - half_rot, 1),
        pltpu.roll(head, half_rot, 1),
    )


def qkv_product(left, pieces, chip, bias, cosines, sines):
    rows = left.shape[0]
    columns = bias.shape[1]

    def finish(step, result, extras, outs):
        bias_ref, cosine_ref, sine_ref = extras
        value = result + bias_ref[...]
        head = value[:, :128]
        turned = head * cosine_ref[...] + partner_lanes(head) * sine_ref[...]
        outs[0][:, :128] = jnp.where(step < 2, turned, head).astype(jnp.bfloat16)
        outs[0][:, 128:] = value[:, 128:].astype(jnp.bfloat16)

    return gathered_product(
        left,
        pieces,
        chip,
        [(bias, True), (cosines, False), (sines, False)],
        [shape_of((rows, columns), jnp.bfloat16)],
        finish,
        3,
        "qkv",
    )


def expand_product(left, pieces, chip, bias):
    shape = (left.shape[0], bias.shape[1])

    def finish(step, result, extras, outs):
        pre = result + extras[0][...]
        distribution = 0.5 * (1.0 + lax.erf(pre * 0.7071067811865476))
        outs[0][...] = (pre * distribution).astype(jnp.bfloat16)
        outs[1][...] = distribution + pre * jnp.exp(-0.5 * pre * pre) * 0.3989422804014327

    return gathered_product(
        left,
        pieces,
        chip,
        [(bias, True)],
        [shape_of(shape, jnp.bfloat16), shape_of(shape, jnp.float32)],
        finish,
        4,
        "expand",
    )


def contract_product(left, pieces, chip, slope):
    def finish(step, result, extras, outs):
        gradient = result * extras[0][...]
        outs[0][...] = gradient.astype(jnp.bfloat16)
        outs[1][...] = jnp.sum(gradient, axis=0, keepdims=True)

    return gathered_product(
        left,
        pieces,
        chip,
        [(slope, True)],
        [shape_of(slope.shape, jnp.bfloat16), shape_of((1, slope.shape[1]), jnp.float32)],
        finish,
        4,
        "contract",
    )


def nt(left, right):
    return lax.dot_general(
        left, right, (((1,), (1,)), ((), ())), preferred_element_type=jnp.float32
    )


def attention_call(body, halo_of, operands, extras, outputs, name):
    qkv, halo, seg_rows, token_rows, seg_columns, token_columns, seg_halo, token_halo = operands
    rows = qkv.shape[0] // 2
    head = qkv.shape[1] // 3
    block = lambda column, flip: pl.BlockSpec(
        (rows, head), lambda b, h: ((1 - b) if flip else b, column)
    )
    column_vector = pl.BlockSpec((rows, 1), lambda b, h: (b, 0))
    row_vector = lambda flip: pl.BlockSpec((1, rows), lambda b, h: (0, (1 - b) if flip else b))
    fixed = lambda value: pl.BlockSpec(value.shape, lambda b, h: (0, 0))
    by_block = lambda value: pl.BlockSpec((rows, value.shape[1]), lambda b, h: (b, 0))
    return pl.pallas_call(
        body,
        cost_estimate=small_cost,
        grid_spec=pltpu.PrefetchScalarGridSpec(
            num_scalar_prefetch=1,
            grid=(2,),
            in_specs=[
                block(0, False),
                block(1, True),
                block(2, True),
                block(1, False),
                block(2, False),
                fixed(halo),
                column_vector,
                column_vector,
                row_vector(True),
                row_vector(True),
                row_vector(False),
                row_vector(False),
                fixed(seg_halo),
                fixed(token_halo),
            ]
            + [by_block(extra) for extra in extras],
            out_specs=[by_block(out) for out in outputs],
        ),
        out_shape=outputs,
        name=name,
    )(
        halo_of,
        qkv,
        qkv,
        qkv,
        qkv,
        qkv,
        halo,
        seg_columns,
        token_columns,
        seg_rows,
        token_rows,
        seg_rows,
        token_rows,
        seg_halo,
        token_halo,
        *extras,
    )


def masked_scores(halo_of, refs, score_scale):
    (
        q_ref,
        k_before,
        v_before,
        k_ref,
        v_ref,
        halo,
        seg_q,
        token_q,
        seg_before,
        token_before,
        seg_k,
        token_k,
        seg_halo,
        token_halo,
    ) = refs
    use_halo = halo_of[pl.program_id(0)] == 1
    head = q_ref.shape[1]
    keys_before = jnp.where(use_halo, halo[:, :head], k_before[...])
    values_before = jnp.where(use_halo, halo[:, head:], v_before[...])
    segments_before = jnp.where(use_halo, seg_halo[...], seg_before[...])
    tokens_before = jnp.where(use_halo, token_halo[...], token_before[...])
    query = q_ref[...]

    def scores(keys, key_segments, key_tokens):
        allowed = (key_segments == seg_q[...]) & (key_tokens <= token_q[...])
        return jnp.where(allowed, nt(query, keys) * score_scale, masked_score)

    return (
        query,
        (keys_before, k_ref[...]),
        (values_before, v_ref[...]),
        (
            scores(keys_before, segments_before, tokens_before),
            scores(k_ref[...], seg_k[...], token_k[...]),
        ),
    )


def attention_forward(halo_of, operands):
    rows, columns = operands[0].shape
    head = columns // 3
    score_scale = head ** (-0.5)

    def body(halo_ref, *refs):
        _, _, values, scores = masked_scores(halo_ref, refs[:14], score_scale)
        out_ref, lse_ref = refs[14:]
        row_max = jnp.maximum(
            jnp.max(scores[0], axis=-1, keepdims=True), jnp.max(scores[1], axis=-1, keepdims=True)
        )
        powers = [jnp.exp(part - row_max) for part in scores]
        total = jnp.sum(powers[0], axis=-1, keepdims=True) + jnp.sum(
            powers[1], axis=-1, keepdims=True
        )
        inverse = 1.0 / total
        out_ref[...] = (
            product((powers[0] * inverse).astype(jnp.bfloat16), values[0])
            + product((powers[1] * inverse).astype(jnp.bfloat16), values[1])
        ).astype(jnp.bfloat16)
        lse_ref[...] = row_max + jnp.log(total)

    return attention_call(
        body,
        halo_of,
        operands,
        [],
        [shape_of((rows, head), jnp.bfloat16), shape_of((rows, 1), jnp.float32)],
        "attention",
    )


def attention_backward(halo_of, operands, lse, attended, attn_grad):
    rows, columns = operands[0].shape
    head = columns // 3
    score_scale = head ** (-0.5)

    def body(halo_ref, *refs):
        query, keys, values, scores = masked_scores(halo_ref, refs[:14], score_scale)
        lse_ref, attended_ref, grad_ref, query_out, before_out, own_out = refs[14:]
        gradient = grad_ref[...]
        row_delta = jnp.sum(
            gradient.astype(jnp.float32) * attended_ref[...].astype(jnp.float32),
            axis=-1,
            keepdims=True,
        )
        query_grad = 0.0
        for part, out in enumerate((before_out, own_out)):
            probs = jnp.exp(scores[part] - lse_ref[...])
            score_grad = (
                probs * (nt(gradient, values[part]) - row_delta) * score_scale
            ).astype(jnp.bfloat16)
            query_grad = query_grad + product(score_grad, keys[part])
            out[:, :head] = contract_rows(score_grad, query)
            out[:, head:] = contract_rows(probs.astype(jnp.bfloat16), gradient)
        query_out[...] = query_grad

    return attention_call(
        body,
        halo_of,
        operands,
        [lse, attended, attn_grad],
        [
            shape_of((rows, head), jnp.float32),
            shape_of((rows, 2 * head), jnp.float32),
            shape_of((rows, 2 * head), jnp.float32),
        ],
        "attention_back",
    )


def rotated_back(later_of, query_grad, own_part, before_part, from_later, cosines, sines):
    rows = query_grad.shape[0] // 2
    head = query_grad.shape[1]

    def body(later_ref, query_ref, own_ref, before_ref, later_grad, cosine, sine, out, bias_out):
        step = pl.program_id(0)
        extra = jnp.where(
            later_ref[step] == 1, later_grad[...].astype(jnp.float32), before_ref[...]
        )
        pairs = own_ref[...] + extra

        def back(value):
            lanes = value[:, :128]
            lanes = lanes * cosine[...] - partner_lanes(lanes) * sine[...]
            return jnp.concatenate([lanes, value[:, 128:]], axis=1)

        @pl.when(step == 0)
        def _():
            bias_out[...] = jnp.zeros_like(bias_out)

        parts = (back(query_ref[...]), back(pairs[:, :head]), pairs[:, head:])
        for i, part in enumerate(parts):
            columns = slice(i * head, (i + 1) * head)
            out[:, columns] = part.astype(jnp.bfloat16)
            bias_out[:, columns] += jnp.sum(part, axis=0, keepdims=True)

    by_block = lambda width: pl.BlockSpec((rows, width), lambda b, h: (b, 0))
    return pl.pallas_call(
        body,
        cost_estimate=small_cost,
        grid_spec=pltpu.PrefetchScalarGridSpec(
            num_scalar_prefetch=1,
            grid=(2,),
            in_specs=[
                by_block(head),
                by_block(2 * head),
                pl.BlockSpec((rows, 2 * head), lambda b, h: (1 - b, 0)),
                pl.BlockSpec((rows, 2 * head), lambda b, h: (0, 0)),
                by_block(128),
                by_block(128),
            ],
            out_specs=[by_block(3 * head), pl.BlockSpec((1, 3 * head), lambda b, h: (0, 0))],
        ),
        out_shape=[
            shape_of((2 * rows, 3 * head), jnp.bfloat16),
            shape_of((1, 3 * head), jnp.float32),
        ],
        name="rotated_back",
    )(later_of, query_grad, own_part, before_part, from_later, cosines, sines)


def branch_rows(half, attended, activated, weight_qd, weight_contract, dtype):
    rows = attended.shape[0] // 2
    tile = 512
    depth = weight_qd.shape[0]

    def body(attended_ref, activated_ref, dense_ref, contract_ref, out):
        out[...] = (
            nt(attended_ref[...], dense_ref[...]) + nt(activated_ref[...], contract_ref[...])
        ).astype(dtype)

    return pl.pallas_call(
        body,
        cost_estimate=small_cost,
        grid=(depth // tile,),
        in_specs=[
            pl.BlockSpec((rows, attended.shape[1]), lambda j: (half, 0)),
            pl.BlockSpec((rows, activated.shape[1]), lambda j: (half, 0)),
            pl.BlockSpec((tile, attended.shape[1]), lambda j: (j, 3)),
            pl.BlockSpec((tile, activated.shape[1]), lambda j: (j, 0)),
        ],
        out_specs=pl.BlockSpec((rows, tile), lambda j: (0, j)),
        out_shape=shape_of((rows, depth), dtype),
        name="branch_%d" % half,
    )(attended, activated, weight_qd, weight_contract)


def back_rows(half, qkv_grad, pre_grad, x, weight_qd, weight_expand, vectors, dtype):
    rows = x.shape[0] // 2
    tile = 512
    depth = x.shape[1]

    def body(qkv_ref, pre_ref, x_ref, tile_ref, qd_ref, expand_ref, vector_ref, out, sums, stats):
        @pl.when(pl.program_id(0) == 0)
        def _():
            row = x_ref[...].astype(jnp.float32)
            mean = jnp.mean(row, axis=-1, keepdims=True)
            center = row - mean
            variance = jnp.mean(center * center, axis=-1, keepdims=True)
            stats[0] = jnp.broadcast_to(mean, stats.shape[1:])
            stats[1] = jnp.broadcast_to(lax.rsqrt(variance + norm_eps), stats.shape[1:])

        xhat = (tile_ref[...].astype(jnp.float32) - stats[0][:, :1]) * stats[1][:, :1]
        attn_back = nt(qkv_ref[...], qd_ref[...])
        mlp_back = nt(pre_ref[...], expand_ref[...])
        sums[0:1] = jnp.sum(attn_back * xhat, axis=0, keepdims=True)
        sums[1:2] = jnp.sum(attn_back, axis=0, keepdims=True)
        sums[2:3] = jnp.sum(mlp_back * xhat, axis=0, keepdims=True)
        sums[3:4] = jnp.sum(mlp_back, axis=0, keepdims=True)
        out[...] = (attn_back * vector_ref[0:1] + mlp_back * vector_ref[2:3]).astype(dtype)

    return pl.pallas_call(
        body,
        cost_estimate=small_cost,
        grid=(depth // tile,),
        in_specs=[
            pl.BlockSpec((rows, qkv_grad.shape[1]), lambda j: (half, 0)),
            pl.BlockSpec((rows, pre_grad.shape[1]), lambda j: (half, 0)),
            pl.BlockSpec((rows, depth), lambda j: (half, 0)),
            pl.BlockSpec((rows, tile), lambda j: (half, j)),
            pl.BlockSpec((tile, qkv_grad.shape[1]), lambda j: (j, 0)),
            pl.BlockSpec((tile, pre_grad.shape[1]), lambda j: (j, 0)),
            pl.BlockSpec((vectors.shape[0], tile), lambda j: (0, j)),
        ],
        out_specs=[
            pl.BlockSpec((rows, tile), lambda j: (0, j)),
            pl.BlockSpec((4, tile), lambda j: (0, j)),
        ],
        out_shape=[shape_of((rows, depth), dtype), shape_of((4, depth), jnp.float32)],
        scratch_shapes=[pltpu.VMEM((2, rows, 128), jnp.float32)],
        name="back_%d" % half,
    )(qkv_grad, pre_grad, x, x, weight_qd, weight_expand, vectors)


def tied(value, *others):
    return lax.optimization_barrier((value,) + others)[0]


def picked(values, index):
    rows = jnp.arange(values.shape[0], dtype=jnp.int32)
    chosen = index[:, None, None] == rows[None, :, None]
    return jnp.sum(jnp.where(chosen, values[None], 0), axis=1)


def per_device_paired(
    inputs,
    cotangent,
    segments,
    positions,
    qkv_weight,
    qkv_bias,
    dense_weight,
    expand_weight,
    expand_bias,
    contract_weight,
    norm_bias_vectors,
    moment_qkv_weight,
    moment_qkv_bias,
    moment_dense_weight,
    moment_expand_weight,
    moment_expand_bias,
    moment_contract_weight,
    moment_norm_vectors,
    second_qkv_weight,
    second_qkv_bias,
    second_dense_weight,
    second_expand_weight,
    second_expand_bias,
    second_contract_weight,
    second_norm_vectors,
):
    bf16, f32 = jnp.bfloat16, jnp.float32
    fsdp_index = lax.axis_index("fsdp")
    z = lax.axis_index("tensor")
    n_z = lax.axis_size("tensor")
    core = fsdp_index & 1
    chip = fsdp_index >> 1
    devices = range(lax.axis_size("fsdp"))
    to_core = [(i, i ^ 1) for i in devices]
    to_x = [(i, i ^ 2) for i in devices]
    to_y = [(i, i ^ 4) for i in devices]
    to_next = [(i, i + 2) for i in devices if i + 2 < len(devices)]
    to_prev = [(i + 2, i) for i in devices if i + 2 < len(devices)]
    first = core == 0
    head_dim = qkv_weight.shape[2] // 3
    shard_rows = inputs.shape[0]
    group_rows = n_z * shard_rows
    hidden = expand_weight.shape[1] // 2
    qkv_cols = 3 * head_dim
    shard_feat = expand_weight.shape[0]
    chip_feat = 2 * shard_feat

    def column_half(weight, k, width):
        return lax.dynamic_slice_in_dim(weight, k * width, width, axis=1).astype(bf16)

    def head_columns(k):
        return jnp.concatenate(
            [
                lax.dynamic_index_in_dim(qkv_weight, k, axis=1, keepdims=False),
                lax.dynamic_slice_in_dim(dense_weight, k * head_dim, head_dim, axis=1),
            ],
            axis=1,
        ).astype(bf16)

    def rows_of_chip(own, other):
        return jnp.concatenate(
            [jnp.where(first, own, other), jnp.where(first, other, own)], axis=0
        )

    x_group = lax.all_gather(inputs, "tensor", axis=0, tiled=True)
    dy_group = lax.all_gather(cotangent, "tensor", axis=0, tiled=True)

    swap_1 = send(head_columns(1 - core), "fsdp", to_core)
    block_1 = rows_of_chip(head_columns(core), swap_1)
    expand_in, contract_in = lax.optimization_barrier((expand_weight, contract_weight, swap_1))[:2]
    swap_2 = send(column_half(expand_in, 1 - core, hidden), "fsdp", to_core)
    swap_3 = send(column_half(contract_in, 1 - core, hidden), "fsdp", to_core)
    block_2 = rows_of_chip(column_half(expand_in, core, hidden), swap_2)
    contract_own, swap_3 = lax.optimization_barrier((contract_in, swap_3, block_2))[:2]
    block_3 = rows_of_chip(column_half(contract_own, core, hidden), swap_3)

    first_x, first_y = send(block_1, "fsdp", to_x), send(block_1, "fsdp", to_y)

    def passed_on(from_x, from_y, block):
        return (
            send(jnp.concatenate([from_y[:shard_feat], block], axis=0), "fsdp", to_x),
            send(jnp.concatenate([from_x[shard_feat:], block], axis=0), "fsdp", to_y),
        )

    second_x, second_y = passed_on(first_x, first_y, block_2)
    third_x, third_y = passed_on(second_x[shard_feat:], second_y[shard_feat:], block_3)
    pieces_1 = (block_1, (first_x, 0), (first_y, 0), (second_x, 0), (second_y, 0))

    segments_in, positions_in, dy_in = lax.optimization_barrier(
        (segments, positions, cotangent, block_2)
    )[:3]
    dy_sum = lax.optimization_barrier(jnp.sum(dy_in.astype(f32), axis=0, keepdims=True))
    position_other = send(positions_in, "fsdp", to_core)
    local = jnp.arange(group_rows, dtype=jnp.int32)
    groups = jnp.stack([fsdp_index, fsdp_index ^ 1, jnp.maximum(2 * chip - 1, 0)])
    seg_rows = picked(segments_in.reshape(-1, group_rows), groups)
    seg_halo = jnp.where(chip == 0, -1, seg_rows[2:])
    seg_rows = seg_rows[:2].reshape(1, 2 * group_rows)
    token_numbers = groups[:, None] * group_rows + local[None, :]
    token_rows = token_numbers[:2].reshape(1, 2 * group_rows)
    token_halo = token_numbers[2:]
    position_all = jnp.concatenate([positions_in, position_other])
    lane = jnp.arange(128, dtype=jnp.int32)
    half_rot = ROT // 2
    frequency = 10000.0 ** (-((lane % half_rot).astype(f32) * 2.0 / ROT))
    angles = jnp.where(
        lane[None, :] < ROT, position_all.astype(f32)[:, None] * frequency[None, :], 0.0
    )
    cosines = jnp.cos(angles)
    sines = jnp.sin(angles) * jnp.where(lane < half_rot, -1.0, 1.0)[None, :]
    halo_of = jnp.stack([first, ~first]).astype(jnp.int32)
    later_of = 1 - halo_of

    x_group = tied(x_group, first_x, first_y)
    x_all = jnp.concatenate([x_group, send(x_group, "fsdp", to_core)], axis=0)
    xhat, _ = normalized_row_block(x_all.astype(f32))
    xa = (xhat * norm_bias_vectors[0] + norm_bias_vectors[1]).astype(bf16)
    xm = (xhat * norm_bias_vectors[2] + norm_bias_vectors[3]).astype(bf16)

    head_bias = lax.dynamic_slice_in_dim(qkv_bias, core, 1, axis=0)
    weight_qd, qkv = qkv_product(xa, pieces_1, chip, head_bias, cosines, sines)
    kv_halo = send(
        jnp.where(first, qkv[group_rows:, head_dim:], qkv[:group_rows, head_dim:]), "fsdp", to_next
    )
    operands = (
        qkv,
        kv_halo,
        seg_rows,
        token_rows,
        seg_rows.reshape(2 * group_rows, 1),
        token_rows.reshape(2 * group_rows, 1),
        seg_halo,
        token_halo,
    )
    attended, lse = attention_forward(halo_of, operands)

    dy_group = tied(dy_group, qkv)
    dy_all = jnp.concatenate([dy_group, send(dy_group, "fsdp", to_core)], axis=0)

    third_x, third_y = lax.optimization_barrier((third_x, third_y, qkv))[:2]
    last_x = send(third_y[shard_feat : 2 * shard_feat], "fsdp", to_x)
    last_y = send(third_x[2 * shard_feat :], "fsdp", to_y)
    pieces_2 = (
        block_2,
        (second_x, shard_feat),
        (second_y, shard_feat),
        (third_x, 0),
        (third_y, 0),
    )
    pieces_3 = (block_3, (third_x, shard_feat), (third_y, shard_feat), (last_x, 0), (last_y, 0))
    expand_bias_half = lax.dynamic_slice_in_dim(expand_bias, core * hidden, hidden).reshape(1, -1)
    weight_expand, activated, slope = expand_product(xm, pieces_2, chip, expand_bias_half)

    def block_of(left, right, r):
        columns = lax.dynamic_slice_in_dim(left, (chip ^ r) * chip_feat, chip_feat, axis=1)
        return contract_rows(columns, right)

    def diagonal(left, right):
        return block_of(left, right, 3).astype(bf16)

    def sent_diagonal(block):
        return (
            send(block[:shard_feat], "fsdp", to_x),
            send(block[shard_feat:], "fsdp", to_y),
        )

    def neighbours(left, right, got):
        zero = jnp.zeros_like(got[0])
        for_x = block_of(left, right, 1) + jnp.concatenate([zero, got[1]], axis=0).astype(f32)
        for_y = block_of(left, right, 2) + jnp.concatenate([got[0], zero], axis=0).astype(f32)
        return for_x.astype(bf16), for_y.astype(bf16)

    def sent_neighbours(blocks):
        return send(blocks[0], "fsdp", to_x), send(blocks[1], "fsdp", to_y)

    def own_gradient(left, right, got):
        total = block_of(left, right, 0) + got[0].astype(f32) + got[1].astype(f32)
        kept = lax.dynamic_slice_in_dim(total, core * shard_feat, shard_feat, axis=0)
        given = lax.dynamic_slice_in_dim(total, (1 - core) * shard_feat, shard_feat, axis=0)
        taken = send(given, "fsdp", to_core)
        return jnp.where(first, kept, taken), jnp.where(first, taken, kept)

    dc_right = tied(jnp.concatenate([attended, activated], axis=1), last_x, last_y)
    dc_diagonal = diagonal(dy_all, dc_right)
    dc_got = sent_diagonal(dc_diagonal)
    attn_dy = tied(dy_all, dc_diagonal)
    attn_grad = product(attn_dy, weight_qd[:, qkv_cols:]).astype(bf16)
    query_grad, before_part, own_part = attention_backward(
        halo_of, operands, lse, attended, attn_grad
    )
    from_later = send(
        jnp.where(first, before_part[:group_rows], before_part[group_rows:]).astype(bf16),
        "fsdp",
        to_prev,
    )

    weight_contract, pre_grad, expand_bias_part = contract_product(
        dy_all, pieces_3, chip, tied(slope, before_part)
    )
    dc_next = neighbours(tied(dy_all, pre_grad), dc_right, dc_got)
    dc_from = sent_neighbours(dc_next)
    qkv_grad, qkv_bias_part = rotated_back(
        later_of, tied(query_grad, dc_next), own_part, before_part, from_later, cosines, sines
    )
    qkv_diagonal = diagonal(xa, qkv_grad)
    qkv_got = sent_diagonal(qkv_diagonal)
    expand_diagonal = diagonal(tied(xm, qkv_diagonal), pre_grad)
    expand_got = sent_diagonal(expand_diagonal)

    branch_weight = tied(weight_contract, expand_diagonal)
    rows_of = lambda half, dtype: branch_rows(
        half, attended, activated, weight_qd, branch_weight, dtype
    )
    branch_other = send(rows_of(1, bf16), "fsdp", to_core)
    branch_rows_own = (rows_of(0, f32) + branch_other.astype(f32)).astype(bf16)
    backs = lambda half, back_x, dtype: back_rows(
        half, qkv_grad, pre_grad, back_x, weight_qd, weight_expand, norm_bias_vectors, dtype
    )
    qkv_next = neighbours(tied(xa, branch_rows_own, dc_from), qkv_grad, qkv_got)
    qkv_from = sent_neighbours(qkv_next)
    expand_next = neighbours(tied(xm, qkv_next), pre_grad, expand_got)
    expand_from = sent_neighbours(expand_next)
    weighted_other, sums_other = backs(1, tied(x_all, expand_next), bf16)
    weighted_other = send(weighted_other, "fsdp", to_core)
    weighted_own, sums_own = backs(0, tied(x_all, sums_other, qkv_from), f32)
    branch_sum = lax.psum_scatter(branch_rows_own, "tensor", scatter_dimension=0, tiled=True)
    vector_part = jnp.concatenate(
        [sums_own + sums_other, dy_sum], axis=0
    )
    bias_part = jnp.concatenate([qkv_bias_part, expand_bias_part], axis=1)
    n_vector = vector_part.size
    small = jnp.concatenate([vector_part.reshape(-1), bias_part.reshape(-1)]).reshape(-1, 128)
    small = small + send(small, "fsdp", to_x)
    small = small + send(small, "fsdp", to_y)
    small_other = send(small, "fsdp", to_core)
    flat, flat_other = small.reshape(-1), small_other.reshape(-1)
    vector_sum = (flat[:n_vector] + flat_other[:n_vector]).reshape(-1, 128)
    for bit in (1, 2):
        vector_sum = vector_sum + send(
            vector_sum, "tensor", [(i, i ^ bit) for i in range(n_z)]
        )
    vector_sum = vector_sum.reshape(vector_part.shape)
    grad_norm_vectors = jnp.concatenate([vector_sum, vector_sum[4:]], axis=0)
    bias_first = jnp.where(first, flat[n_vector:], flat_other[n_vector:])
    bias_second = jnp.where(first, flat_other[n_vector:], flat[n_vector:])
    grad_qkv_bias = jnp.stack([bias_first[:qkv_cols], bias_second[:qkv_cols]])
    grad_expand_bias = jnp.concatenate([bias_first[qkv_cols:], bias_second[qkv_cols:]])
    weighted_rows = (weighted_own + weighted_other.astype(f32)).astype(bf16)
    weighted_rows = tied(weighted_rows, branch_sum, expand_from)
    weighted = lax.psum_scatter(
        weighted_rows, "tensor", scatter_dimension=0, tiled=True
    ).astype(f32)
    output = (
        inputs.astype(f32) + branch_sum.astype(f32) + norm_bias_vectors[4] + norm_bias_vectors[5]
    )
    xhat_own, inverse_own = normalized_row_block(inputs.astype(f32))
    block_input_gradient = cotangent.astype(f32) + inverse_own * (
        weighted
        - jnp.mean(weighted, axis=-1, keepdims=True)
        - xhat_own * jnp.mean(weighted * xhat_own, axis=-1, keepdims=True)
    )

    dc_halves = own_gradient(dy_all, dc_right, dc_from)
    qkv_halves = own_gradient(xa, qkv_grad, qkv_from)
    expand_halves = own_gradient(xm, pre_grad, expand_from)
    grad_contract_weight = jnp.concatenate([part[:, head_dim:] for part in dc_halves], axis=1)
    grad_dense_weight = jnp.concatenate([part[:, :head_dim] for part in dc_halves], axis=1)
    grad_expand_weight = jnp.concatenate(expand_halves, axis=1)
    grad_qkv_weight = jnp.stack(qkv_halves, axis=1)
    new_qkv_weight, new_moment_qkv_weight, new_second_qkv_weight = adam_step(
        qkv_weight,
        grad_qkv_weight,
        moment_qkv_weight,
        second_qkv_weight,
        rate_qkv_weight,
        decay_matrix,
    )
    new_qkv_bias, new_moment_qkv_bias, new_second_qkv_bias = adam_step(
        qkv_bias, grad_qkv_bias, moment_qkv_bias, second_qkv_bias, rate_qkv_bias, 0.0
    )
    new_dense_weight, new_moment_dense_weight, new_second_dense_weight = adam_step(
        dense_weight,
        grad_dense_weight,
        moment_dense_weight,
        second_dense_weight,
        rate_dense_weight,
        decay_matrix,
    )
    new_expand_weight, new_moment_expand_weight, new_second_expand_weight = adam_step(
        expand_weight,
        grad_expand_weight,
        moment_expand_weight,
        second_expand_weight,
        rate_expand_weight,
        decay_matrix,
    )
    new_expand_bias, new_moment_expand_bias, new_second_expand_bias = adam_step(
        expand_bias, grad_expand_bias, moment_expand_bias, second_expand_bias, rate_expand_bias, 0.0
    )
    new_contract_weight, new_moment_contract_weight, new_second_contract_weight = adam_step(
        contract_weight,
        grad_contract_weight,
        moment_contract_weight,
        second_contract_weight,
        rate_contract_weight,
        decay_matrix,
    )
    new_norm_vectors, new_moment_norm_vectors, new_second_norm_vectors = adam_step(
        norm_bias_vectors,
        grad_norm_vectors,
        moment_norm_vectors,
        second_norm_vectors,
        rate_norm_vectors,
        0.0,
    )
    return (
        output,
        block_input_gradient,
        grad_qkv_weight,
        new_qkv_weight,
        new_moment_qkv_weight,
        new_second_qkv_weight,
        grad_qkv_bias,
        new_qkv_bias,
        new_moment_qkv_bias,
        new_second_qkv_bias,
        grad_dense_weight,
        new_dense_weight,
        new_moment_dense_weight,
        new_second_dense_weight,
        grad_expand_weight,
        new_expand_weight,
        new_moment_expand_weight,
        new_second_expand_weight,
        grad_expand_bias,
        new_expand_bias,
        new_moment_expand_bias,
        new_second_expand_bias,
        grad_contract_weight,
        new_contract_weight,
        new_moment_contract_weight,
        new_second_contract_weight,
        grad_norm_vectors,
        new_norm_vectors,
        new_moment_norm_vectors,
        new_second_norm_vectors,
    )


def solution(mesh):
    paired = mesh.shape["fsdp"] == 8 and mesh.shape["tensor"] == 4
    per_device = per_device_paired if paired else per_device_generic
    return jax.shard_map(
        per_device,
        mesh=mesh,
        in_specs=(
            P(("fsdp", "tensor"), None),
            P(("fsdp", "tensor"), None),
            P(),
            P("fsdp"),
            P("fsdp", "tensor", None),
            P("tensor", None),
            P("fsdp", "tensor"),
            P("fsdp", "tensor"),
            P("tensor"),
            P("fsdp", "tensor"),
            P(),
            P("fsdp", "tensor", None),
            P("tensor", None),
            P("fsdp", "tensor"),
            P("fsdp", "tensor"),
            P("tensor"),
            P("fsdp", "tensor"),
            P(),
            P("fsdp", "tensor", None),
            P("tensor", None),
            P("fsdp", "tensor"),
            P("fsdp", "tensor"),
            P("tensor"),
            P("fsdp", "tensor"),
            P(),
        ),
        out_specs=(
            P(("fsdp", "tensor"), None),
            P(("fsdp", "tensor"), None),
            P("fsdp", "tensor", None),
            P("fsdp", "tensor", None),
            P("fsdp", "tensor", None),
            P("fsdp", "tensor", None),
            P("tensor", None),
            P("tensor", None),
            P("tensor", None),
            P("tensor", None),
            P("fsdp", "tensor"),
            P("fsdp", "tensor"),
            P("fsdp", "tensor"),
            P("fsdp", "tensor"),
            P("fsdp", "tensor"),
            P("fsdp", "tensor"),
            P("fsdp", "tensor"),
            P("fsdp", "tensor"),
            P("tensor"),
            P("tensor"),
            P("tensor"),
            P("tensor"),
            P("fsdp", "tensor"),
            P("fsdp", "tensor"),
            P("fsdp", "tensor"),
            P("fsdp", "tensor"),
            P(),
            P(),
            P(),
            P(),
        ),
        check_vma=False,
    )
```

```python
import jax
import jax.numpy as jnp
from jax import lax
from jax.experimental import pallas as pl
from jax.experimental.pallas import tpu as pltpu
from jax.sharding import PartitionSpec as P

ROT = 64
STEP = 3


norm_eps = 1e-05
masked_score = -1e30
beta_one = 0.9
beta_two = 0.95
adam_eps = 1e-08
decay_matrix = 0.01
rate_qkv_weight = 0.005
rate_qkv_bias = 0.02
rate_dense_weight = 0.04
rate_expand_weight = 0.005
rate_expand_bias = 0.02
rate_contract_weight = 0.003
rate_norm_vectors = 0.1


def shifted(value, axis, steps):
    count = lax.axis_size(axis)
    first, last = (max(0, -steps), min(count, count - steps))
    return lax.ppermute(value, axis, [(source, source + steps) for source in range(first, last)])


def normalized_row_block(row_values):
    center = row_values - jnp.mean(row_values, axis=-1, keepdims=True)
    variance = jnp.mean(center * center, axis=-1, keepdims=True)
    inverse_deviation = lax.rsqrt(variance + norm_eps)
    return (center * inverse_deviation, inverse_deviation)


def norm_backward_term(upstream_gradient, gain_vector_row, centered_normalized, inverse_deviation):
    scaled_rows = upstream_gradient * gain_vector_row
    return inverse_deviation * (
        scaled_rows
        - jnp.mean(scaled_rows, axis=-1, keepdims=True)
        - centered_normalized * jnp.mean(scaled_rows * centered_normalized, axis=-1, keepdims=True)
    )


def rotary_tables(token_pos):
    half_rot = ROT // 2
    frequency = 10000.0 ** (-(jnp.arange(half_rot, dtype=jnp.float32) * 2.0 / ROT))
    angles = token_pos.astype(jnp.float32)[:, None] * frequency[None, :]
    return (jnp.cos(angles)[:, None, :], jnp.sin(angles)[:, None, :])


def rotate(head_values, cosine_rotation, sine_rotation_table, direction):
    half_rot = ROT // 2
    first_half = head_values[..., :half_rot]
    second_half = head_values[..., half_rot:ROT]
    return jnp.concatenate(
        [
            first_half * cosine_rotation - direction * second_half * sine_rotation_table,
            second_half * cosine_rotation + direction * first_half * sine_rotation_table,
            head_values[..., ROT:],
        ],
        axis=-1,
    )


def gelu_slope(pre_values):
    return (
        0.5 * (1.0 + lax.erf(pre_values * 0.7071067811865476))
        + pre_values * jnp.exp(-0.5 * pre_values * pre_values) * 0.3989422804014327
    )


def key_mask(seg_query, query_index, seg_keys, group_rows, has_prev):
    key_index = jnp.arange(seg_keys.shape[0], dtype=jnp.int32)
    causal = key_index[None, :] <= query_index[:, None]
    same_doc = seg_keys[None, :] == seg_query[:, None]
    present = (key_index[None, :] >= group_rows) | has_prev
    return causal & same_doc & present


def block_scores(query_blk, keys_all, allowed, score_scale):
    scores = (
        jnp.einsum("qhc,khc->hqk", query_blk, keys_all, preferred_element_type=jnp.float32)
        * score_scale
    )
    return jnp.where(allowed[None], scores, masked_score)


def adam_step(parameter, gradient, moment, second, step_rate, decay_weight):
    moment_new = beta_one * moment + (1.0 - beta_one) * gradient
    second_new = beta_two * second + (1.0 - beta_two) * gradient * gradient
    moment_hat = moment_new / (1.0 - beta_one**STEP)
    second_hat = second_new / (1.0 - beta_two**STEP)
    updated = parameter - step_rate * (
        moment_hat / (jnp.sqrt(second_hat) + adam_eps) + decay_weight * parameter
    )
    return (updated, moment_new, second_new)


def contract_rows(left_rows, right_rows):
    return lax.dot_general(
        left_rows, right_rows, (((0,), (0,)), ((), ())), preferred_element_type=jnp.float32
    )


def contract_cols(left_cols, right_cols):
    return lax.dot_general(
        left_cols, right_cols, (((1,), (1,)), ((), ())), preferred_element_type=jnp.float32
    )


def per_device_generic(
    inputs,
    cotangent,
    segments,
    positions,
    qkv_weight,
    qkv_bias,
    dense_weight,
    expand_weight,
    expand_bias,
    contract_weight,
    norm_bias_vectors,
    moment_qkv_weight,
    moment_qkv_bias,
    moment_dense_weight,
    moment_expand_weight,
    moment_expand_bias,
    moment_contract_weight,
    moment_norm_vectors,
    second_qkv_weight,
    second_qkv_bias,
    second_dense_weight,
    second_expand_weight,
    second_expand_bias,
    second_contract_weight,
    second_norm_vectors,
):
    fsdp_index = lax.axis_index("fsdp")
    input_row_block, rows_dy = (
        lax.all_gather(inputs, "tensor", axis=0, tiled=True),
        lax.all_gather(cotangent, "tensor", axis=0, tiled=True),
    )
    group_rows = input_row_block.shape[0]
    shards_bf = (
        qkv_weight.astype(jnp.bfloat16),
        dense_weight.astype(jnp.bfloat16),
        expand_weight.astype(jnp.bfloat16),
        contract_weight.astype(jnp.bfloat16),
    )
    forward_set = (
        lax.all_gather(shards_bf[0], "fsdp", axis=0, tiled=True),
        lax.all_gather(shards_bf[1], "fsdp", axis=0, tiled=True),
        lax.all_gather(shards_bf[2], "fsdp", axis=0, tiled=True),
        lax.all_gather(shards_bf[3], "fsdp", axis=0, tiled=True),
    )
    full_qkv, full_dense, full_expand, full_contract = forward_set
    row_centered_normalized, inverse_row_deviation = normalized_row_block(
        input_row_block.astype(jnp.float32)
    )
    attention_normalized_input = (
        row_centered_normalized * norm_bias_vectors[0] + norm_bias_vectors[1]
    ).astype(jnp.bfloat16)
    feedforward_normalized_input = (
        row_centered_normalized * norm_bias_vectors[2] + norm_bias_vectors[3]
    ).astype(jnp.bfloat16)
    projected = (
        jnp.einsum(
            "rd,dhc->rhc", attention_normalized_input, full_qkv, preferred_element_type=jnp.float32
        )
        + qkv_bias[None]
    )
    heads_dev = projected.shape[1]
    head_dim = projected.shape[2] // 3
    score_scale = head_dim ** (-0.5)
    cosine_rotation, sine_rotation_table = rotary_tables(positions)
    query_rows = rotate(
        projected[..., :head_dim], cosine_rotation, sine_rotation_table, 1.0
    ).astype(jnp.bfloat16)
    local_segment_keys = rotate(
        projected[..., head_dim : 2 * head_dim], cosine_rotation, sine_rotation_table, 1.0
    ).astype(jnp.bfloat16)
    local_segment_values = projected[..., 2 * head_dim :].astype(jnp.bfloat16)
    keys_prev, values_prev = shifted((local_segment_keys, local_segment_values), "fsdp", 1)
    keys_all = jnp.concatenate([keys_prev, local_segment_keys], axis=0)
    values_all = jnp.concatenate([values_prev, local_segment_values], axis=0)
    seg_own = lax.dynamic_slice_in_dim(segments, fsdp_index * group_rows, group_rows)
    seg_prev = lax.dynamic_slice_in_dim(
        segments, jnp.maximum(fsdp_index - 1, 0) * group_rows, group_rows
    )
    seg_keys = jnp.concatenate([seg_prev, seg_own], axis=0)
    has_prev = fsdp_index > 0
    block_rows = min(512, group_rows)
    blocks = group_rows // block_rows
    starts = jnp.arange(blocks, dtype=jnp.int32) * block_rows
    local_index = jnp.arange(block_rows, dtype=jnp.int32)
    query_blocks = query_rows.reshape(blocks, block_rows, heads_dev, head_dim)
    seg_blocks = seg_own.reshape(blocks, block_rows)

    def forward_block(block_data):
        query_blk, seg_blk, start = block_data
        allowed = key_mask(
            seg_blk, group_rows + start + local_index, seg_keys, group_rows, has_prev
        )
        scores = block_scores(query_blk, keys_all, allowed, score_scale)
        row_max = jnp.max(scores, axis=-1, keepdims=True)
        row_total = jnp.sum(jnp.exp(scores - row_max), axis=-1, keepdims=True)
        log_total = row_max + jnp.log(row_total)
        prob_bf = jnp.exp(scores - log_total).astype(jnp.bfloat16)
        result = jnp.einsum("hqk,khc->qhc", prob_bf, values_all, preferred_element_type=jnp.float32)
        return (result.astype(jnp.bfloat16), log_total[..., 0])

    attn_blocks, lse_blocks = lax.map(forward_block, (query_blocks, seg_blocks, starts))
    attended = attn_blocks.reshape(group_rows, heads_dev * head_dim)
    expand_preactivation = (
        jnp.dot(feedforward_normalized_input, full_expand, preferred_element_type=jnp.float32)
        + expand_bias
    )
    gelu_activated_rows = jax.nn.gelu(expand_preactivation, approximate=False).astype(jnp.bfloat16)
    branch_sum = lax.psum_scatter(
        contract_cols(attended, full_dense) + contract_cols(gelu_activated_rows, full_contract),
        "tensor",
        scatter_dimension=0,
        tiled=True,
    )
    output = inputs.astype(jnp.float32) + branch_sum + norm_bias_vectors[4] + norm_bias_vectors[5]
    back_qkv, back_dense, back_expand, back_contract = forward_set
    act_grad = jnp.dot(rows_dy, back_contract, preferred_element_type=jnp.float32)
    pre_grad32 = act_grad * gelu_slope(expand_preactivation)
    pre_grad = pre_grad32.astype(jnp.bfloat16)
    attn_grad = jnp.dot(rows_dy, back_dense, preferred_element_type=jnp.float32).astype(
        jnp.bfloat16
    )
    attn_heads = attn_grad.reshape(group_rows, heads_dev, head_dim)
    row_delta = jnp.sum(
        attn_heads.astype(jnp.float32)
        * attended.reshape(group_rows, heads_dev, head_dim).astype(jnp.float32),
        axis=-1,
    )

    def backward_block(inner_carry, block_data):
        key_acc, value_acc = inner_carry
        query_blk, seg_blk, start, grad_blk, delta_blk, lse_blk = block_data
        allowed = key_mask(
            seg_blk, group_rows + start + local_index, seg_keys, group_rows, has_prev
        )
        scores = block_scores(query_blk, keys_all, allowed, score_scale)
        prob_f32 = jnp.exp(scores - lse_blk[..., None])
        prob_bf = prob_f32.astype(jnp.bfloat16)
        dot_grad = jnp.einsum(
            "qhc,khc->hqk", grad_blk, values_all, preferred_element_type=jnp.float32
        )
        score_grad = (
            prob_f32 * (dot_grad - jnp.transpose(delta_blk)[..., None]) * score_scale
        ).astype(jnp.bfloat16)
        query_grad = jnp.einsum(
            "hqk,khc->qhc", score_grad, keys_all, preferred_element_type=jnp.float32
        )
        key_acc = key_acc + jnp.einsum(
            "hqk,qhc->khc", score_grad, query_blk, preferred_element_type=jnp.float32
        )
        value_acc = value_acc + jnp.einsum(
            "hqk,qhc->khc", prob_bf, grad_blk, preferred_element_type=jnp.float32
        )
        return ((key_acc, value_acc), query_grad)

    zero_keys = jnp.zeros((2 * group_rows, heads_dev, head_dim), jnp.float32)
    inner_final, query_grads = lax.scan(
        backward_block,
        (zero_keys, zero_keys),
        (
            query_blocks,
            seg_blocks,
            starts,
            attn_heads.reshape(blocks, block_rows, heads_dev, head_dim),
            row_delta.reshape(blocks, block_rows, heads_dev),
            lse_blocks,
        ),
    )
    key_acc, value_acc = inner_final
    later_key_grad, later_value_grad = shifted(
        (key_acc[:group_rows], value_acc[:group_rows]), "fsdp", -1
    )
    key_grad = key_acc[group_rows:] + later_key_grad
    value_grad = value_acc[group_rows:] + later_value_grad
    query_grad = query_grads.reshape(group_rows, heads_dev, head_dim)
    qkv_grad32 = jnp.concatenate(
        [
            rotate(query_grad, cosine_rotation, sine_rotation_table, -1.0),
            rotate(key_grad, cosine_rotation, sine_rotation_table, -1.0),
            value_grad,
        ],
        axis=-1,
    )
    qkv_grad = qkv_grad32.astype(jnp.bfloat16)
    attn_norm_grad = jnp.einsum(
        "rhc,dhc->rd", qkv_grad, back_qkv, preferred_element_type=jnp.float32
    )
    mlp_norm_grad = contract_cols(pre_grad, back_expand)
    qkv_part = jnp.einsum(
        "rd,rhc->dhc", attention_normalized_input, qkv_grad, preferred_element_type=jnp.float32
    )
    dense_part = contract_rows(rows_dy, attended)
    expand_part = contract_rows(feedforward_normalized_input, pre_grad)
    contract_part = contract_rows(rows_dy, gelu_activated_rows)
    local_centered_normalized, inverse_local_deviation = normalized_row_block(
        inputs.astype(jnp.float32)
    )
    dy_local = cotangent.astype(jnp.float32)
    dy_column_sum = jnp.sum(dy_local, axis=0)
    attention_backward_term, feedforward_backward_term = (
        lax.psum_scatter(attn_norm_grad, "tensor", scatter_dimension=0, tiled=True),
        lax.psum_scatter(mlp_norm_grad, "tensor", scatter_dimension=0, tiled=True),
    )
    block_input_gradient = (
        dy_local
        + norm_backward_term(
            attention_backward_term,
            norm_bias_vectors[0],
            local_centered_normalized,
            inverse_local_deviation,
        )
        + norm_backward_term(
            feedforward_backward_term,
            norm_bias_vectors[2],
            local_centered_normalized,
            inverse_local_deviation,
        )
    )
    vector_part = jnp.stack(
        [
            jnp.sum(attention_backward_term * local_centered_normalized, axis=0),
            jnp.sum(attention_backward_term, axis=0),
            jnp.sum(feedforward_backward_term * local_centered_normalized, axis=0),
            jnp.sum(feedforward_backward_term, axis=0),
            dy_column_sum,
            dy_column_sum,
        ]
    )
    qkv_bias_part = jnp.sum(qkv_grad32, axis=0)
    expand_bias_part = jnp.sum(pre_grad32, axis=0)
    grad_qkv_weight, grad_dense_weight, grad_expand_weight, grad_contract_weight = (
        lax.psum_scatter(qkv_part, "fsdp", scatter_dimension=0, tiled=True),
        lax.psum_scatter(dense_part, "fsdp", scatter_dimension=0, tiled=True),
        lax.psum_scatter(expand_part, "fsdp", scatter_dimension=0, tiled=True),
        lax.psum_scatter(contract_part, "fsdp", scatter_dimension=0, tiled=True),
    )
    grad_qkv_bias, grad_expand_bias, vector_fsdp = lax.psum(
        (qkv_bias_part, expand_bias_part, vector_part), "fsdp"
    )
    grad_norm_vectors = lax.psum(vector_fsdp, "tensor")
    new_qkv_weight, new_moment_qkv_weight, new_second_qkv_weight = adam_step(
        qkv_weight,
        grad_qkv_weight,
        moment_qkv_weight,
        second_qkv_weight,
        rate_qkv_weight,
        decay_matrix,
    )
    new_qkv_bias, new_moment_qkv_bias, new_second_qkv_bias = adam_step(
        qkv_bias, grad_qkv_bias, moment_qkv_bias, second_qkv_bias, rate_qkv_bias, 0.0
    )
    new_dense_weight, new_moment_dense_weight, new_second_dense_weight = adam_step(
        dense_weight,
        grad_dense_weight,
        moment_dense_weight,
        second_dense_weight,
        rate_dense_weight,
        decay_matrix,
    )
    new_expand_weight, new_moment_expand_weight, new_second_expand_weight = adam_step(
        expand_weight,
        grad_expand_weight,
        moment_expand_weight,
        second_expand_weight,
        rate_expand_weight,
        decay_matrix,
    )
    new_expand_bias, new_moment_expand_bias, new_second_expand_bias = adam_step(
        expand_bias, grad_expand_bias, moment_expand_bias, second_expand_bias, rate_expand_bias, 0.0
    )
    new_contract_weight, new_moment_contract_weight, new_second_contract_weight = adam_step(
        contract_weight,
        grad_contract_weight,
        moment_contract_weight,
        second_contract_weight,
        rate_contract_weight,
        decay_matrix,
    )
    new_norm_vectors, new_moment_norm_vectors, new_second_norm_vectors = adam_step(
        norm_bias_vectors,
        grad_norm_vectors,
        moment_norm_vectors,
        second_norm_vectors,
        rate_norm_vectors,
        0.0,
    )
    return (
        output,
        block_input_gradient,
        grad_qkv_weight,
        new_qkv_weight,
        new_moment_qkv_weight,
        new_second_qkv_weight,
        grad_qkv_bias,
        new_qkv_bias,
        new_moment_qkv_bias,
        new_second_qkv_bias,
        grad_dense_weight,
        new_dense_weight,
        new_moment_dense_weight,
        new_second_dense_weight,
        grad_expand_weight,
        new_expand_weight,
        new_moment_expand_weight,
        new_second_expand_weight,
        grad_expand_bias,
        new_expand_bias,
        new_moment_expand_bias,
        new_second_expand_bias,
        grad_contract_weight,
        new_contract_weight,
        new_moment_contract_weight,
        new_second_contract_weight,
        grad_norm_vectors,
        new_norm_vectors,
        new_moment_norm_vectors,
        new_second_norm_vectors,
    )


def send(value, axis, pairs):
    return lax.ppermute(value, axis, pairs)


def product(left, right):
    return jnp.dot(left, right, preferred_element_type=jnp.float32)


small_cost = pl.CostEstimate(flops=1024, bytes_accessed=1024, transcendentals=0)


def shape_of(shape, dtype):
    return jax.ShapeDtypeStruct(shape, dtype)


def gathered_product(left, pieces, chip, extras, outputs, finish, live, name):
    tile = 256
    columns = pieces[0].shape[1]
    rows, depth = left.shape
    chip_rows = pieces[0].shape[0]
    half_rows = chip_rows // 2
    arrays = [pieces[0]] + [array for array, _ in pieces[1:]]
    starts = [0] + [start for _, start in pieces[1:]]

    def body(chip_ref, left_ref, block, from_x, from_y, top, bottom, *refs):
        weight_ref = refs[len(extras)]
        parts = (
            (block, 0, 0, chip_rows),
            (from_x, 1, 0, chip_rows),
            (from_y, 2, 0, chip_rows),
            (top, 3, 0, half_rows),
            (bottom, 3, half_rows, half_rows),
        )
        for (part, flip, shift, height), source in zip(parts, starts):
            start = pl.multiple_of((chip_ref[0] ^ flip) * chip_rows + shift, half_rows)
            weight_ref[pl.ds(start, height), :] = part[source : source + height, :]
        step = pl.program_id(0)

        @pl.when(step < live)
        def _():
            result = product(left_ref[...], weight_ref[...])
            finish(step, result, refs[: len(extras)], refs[len(extras) + 1 :])

    def spec_of(height, moves):
        if moves:
            return pl.BlockSpec((height, tile), lambda j, c: (0, jnp.minimum(j, live - 1)))
        return pl.BlockSpec((height, 128), lambda j, c: (0, 0))

    column_spec = lambda height: pl.BlockSpec((height, tile), lambda j, c: (0, j))
    return pl.pallas_call(
        body,
        cost_estimate=small_cost,
        grid_spec=pltpu.PrefetchScalarGridSpec(
            num_scalar_prefetch=1,
            grid=(columns // tile,),
            in_specs=[pl.BlockSpec((rows, depth), lambda j, c: (0, 0))]
            + [column_spec(array.shape[0]) for array in arrays]
            + [spec_of(extra.shape[0], moves) for extra, moves in extras],
            out_specs=[column_spec(depth)] + [spec_of(out.shape[0], True) for out in outputs],
        ),
        out_shape=[shape_of((depth, columns), left.dtype)] + outputs,
        name=name,
    )(chip.reshape(1), left, *arrays, *[extra for extra, _ in extras])


def partner_lanes(head):
    half_rot = ROT // 2
    lane = lax.broadcasted_iota(jnp.int32, head.shape, 1)
    return jnp.where(
        lane < half_rot,
        pltpu.roll(head, head.shape[1] - half_rot, 1),
        pltpu.roll(head, half_rot, 1),
    )


def qkv_product(left, pieces, chip, bias, cosines, sines):
    rows = left.shape[0]
    columns = bias.shape[1]

    def finish(step, result, extras, outs):
        bias_ref, cosine_ref, sine_ref = extras
        value = result + bias_ref[...]
        head = value[:, :128]
        turned = head * cosine_ref[...] + partner_lanes(head) * sine_ref[...]
        outs[0][:, :128] = jnp.where(step < 2, turned, head).astype(jnp.bfloat16)
        outs[0][:, 128:] = value[:, 128:].astype(jnp.bfloat16)

    return gathered_product(
        left,
        pieces,
        chip,
        [(bias, True), (cosines, False), (sines, False)],
        [shape_of((rows, columns), jnp.bfloat16)],
        finish,
        3,
        "qkv",
    )


def expand_product(left, pieces, chip, bias):
    shape = (left.shape[0], bias.shape[1])

    def finish(step, result, extras, outs):
        pre = result + extras[0][...]
        distribution = 0.5 * (1.0 + lax.erf(pre * 0.7071067811865476))
        outs[0][...] = (pre * distribution).astype(jnp.bfloat16)
        outs[1][...] = distribution + pre * jnp.exp(-0.5 * pre * pre) * 0.3989422804014327

    return gathered_product(
        left,
        pieces,
        chip,
        [(bias, True)],
        [shape_of(shape, jnp.bfloat16), shape_of(shape, jnp.float32)],
        finish,
        4,
        "expand",
    )


def contract_product(left, pieces, chip, slope):
    def finish(step, result, extras, outs):
        gradient = result * extras[0][...]
        outs[0][...] = gradient.astype(jnp.bfloat16)
        outs[1][...] = jnp.sum(gradient, axis=0, keepdims=True)

    return gathered_product(
        left,
        pieces,
        chip,
        [(slope, True)],
        [shape_of(slope.shape, jnp.bfloat16), shape_of((1, slope.shape[1]), jnp.float32)],
        finish,
        4,
        "contract",
    )


def nt(left, right):
    return lax.dot_general(
        left, right, (((1,), (1,)), ((), ())), preferred_element_type=jnp.float32
    )


def attention_call(body, halo_of, operands, extras, outputs, name):
    qkv, halo, seg_rows, token_rows, seg_columns, token_columns, seg_halo, token_halo = operands
    rows = qkv.shape[0] // 2
    head = qkv.shape[1] // 3
    block = lambda column, flip: pl.BlockSpec(
        (rows, head), lambda b, h: ((1 - b) if flip else b, column)
    )
    column_vector = pl.BlockSpec((rows, 1), lambda b, h: (b, 0))
    row_vector = lambda flip: pl.BlockSpec((1, rows), lambda b, h: (0, (1 - b) if flip else b))
    fixed = lambda value: pl.BlockSpec(value.shape, lambda b, h: (0, 0))
    by_block = lambda value: pl.BlockSpec((rows, value.shape[1]), lambda b, h: (b, 0))
    return pl.pallas_call(
        body,
        cost_estimate=small_cost,
        grid_spec=pltpu.PrefetchScalarGridSpec(
            num_scalar_prefetch=1,
            grid=(2,),
            in_specs=[
                block(0, False),
                block(1, True),
                block(2, True),
                block(1, False),
                block(2, False),
                fixed(halo),
                column_vector,
                column_vector,
                row_vector(True),
                row_vector(True),
                row_vector(False),
                row_vector(False),
                fixed(seg_halo),
                fixed(token_halo),
            ]
            + [by_block(extra) for extra in extras],
            out_specs=[by_block(out) for out in outputs],
        ),
        out_shape=outputs,
        name=name,
    )(
        halo_of,
        qkv,
        qkv,
        qkv,
        qkv,
        qkv,
        halo,
        seg_columns,
        token_columns,
        seg_rows,
        token_rows,
        seg_rows,
        token_rows,
        seg_halo,
        token_halo,
        *extras,
    )


def masked_scores(halo_of, refs, score_scale):
    (
        q_ref,
        k_before,
        v_before,
        k_ref,
        v_ref,
        halo,
        seg_q,
        token_q,
        seg_before,
        token_before,
        seg_k,
        token_k,
        seg_halo,
        token_halo,
    ) = refs
    use_halo = halo_of[pl.program_id(0)] == 1
    head = q_ref.shape[1]
    keys_before = jnp.where(use_halo, halo[:, :head], k_before[...])
    values_before = jnp.where(use_halo, halo[:, head:], v_before[...])
    segments_before = jnp.where(use_halo, seg_halo[...], seg_before[...])
    tokens_before = jnp.where(use_halo, token_halo[...], token_before[...])
    query = q_ref[...]

    def scores(keys, key_segments, key_tokens):
        allowed = (key_segments == seg_q[...]) & (key_tokens <= token_q[...])
        return jnp.where(allowed, nt(query, keys) * score_scale, masked_score)

    return (
        query,
        (keys_before, k_ref[...]),
        (values_before, v_ref[...]),
        (
            scores(keys_before, segments_before, tokens_before),
            scores(k_ref[...], seg_k[...], token_k[...]),
        ),
    )


def attention_forward(halo_of, operands):
    rows, columns = operands[0].shape
    head = columns // 3
    score_scale = head ** (-0.5)

    def body(halo_ref, *refs):
        _, _, values, scores = masked_scores(halo_ref, refs[:14], score_scale)
        out_ref, lse_ref = refs[14:]
        row_max = jnp.maximum(
            jnp.max(scores[0], axis=-1, keepdims=True), jnp.max(scores[1], axis=-1, keepdims=True)
        )
        powers = [jnp.exp(part - row_max) for part in scores]
        total = jnp.sum(powers[0], axis=-1, keepdims=True) + jnp.sum(
            powers[1], axis=-1, keepdims=True
        )
        inverse = 1.0 / total
        out_ref[...] = (
            product((powers[0] * inverse).astype(jnp.bfloat16), values[0])
            + product((powers[1] * inverse).astype(jnp.bfloat16), values[1])
        ).astype(jnp.bfloat16)
        lse_ref[...] = row_max + jnp.log(total)

    return attention_call(
        body,
        halo_of,
        operands,
        [],
        [shape_of((rows, head), jnp.bfloat16), shape_of((rows, 1), jnp.float32)],
        "attention",
    )


def attention_backward(halo_of, operands, lse, attended, attn_grad):
    rows, columns = operands[0].shape
    head = columns // 3
    score_scale = head ** (-0.5)

    def body(halo_ref, *refs):
        query, keys, values, scores = masked_scores(halo_ref, refs[:14], score_scale)
        lse_ref, attended_ref, grad_ref, query_out, before_out, own_out = refs[14:]
        gradient = grad_ref[...]
        row_delta = jnp.sum(
            gradient.astype(jnp.float32) * attended_ref[...].astype(jnp.float32),
            axis=-1,
            keepdims=True,
        )
        query_grad = 0.0
        for part, out in enumerate((before_out, own_out)):
            probs = jnp.exp(scores[part] - lse_ref[...])
            score_grad = (
                probs * (nt(gradient, values[part]) - row_delta) * score_scale
            ).astype(jnp.bfloat16)
            query_grad = query_grad + product(score_grad, keys[part])
            out[:, :head] = contract_rows(score_grad, query)
            out[:, head:] = contract_rows(probs.astype(jnp.bfloat16), gradient)
        query_out[...] = query_grad

    return attention_call(
        body,
        halo_of,
        operands,
        [lse, attended, attn_grad],
        [
            shape_of((rows, head), jnp.float32),
            shape_of((rows, 2 * head), jnp.float32),
            shape_of((rows, 2 * head), jnp.float32),
        ],
        "attention_back",
    )


def rotated_back(later_of, query_grad, own_part, before_part, from_later, cosines, sines):
    rows = query_grad.shape[0] // 2
    head = query_grad.shape[1]

    def body(later_ref, query_ref, own_ref, before_ref, later_grad, cosine, sine, out, bias_out):
        step = pl.program_id(0)
        extra = jnp.where(
            later_ref[step] == 1, later_grad[...].astype(jnp.float32), before_ref[...]
        )
        pairs = own_ref[...] + extra

        def back(value):
            lanes = value[:, :128]
            lanes = lanes * cosine[...] - partner_lanes(lanes) * sine[...]
            return jnp.concatenate([lanes, value[:, 128:]], axis=1)

        @pl.when(step == 0)
        def _():
            bias_out[...] = jnp.zeros_like(bias_out)

        parts = (back(query_ref[...]), back(pairs[:, :head]), pairs[:, head:])
        for i, part in enumerate(parts):
            columns = slice(i * head, (i + 1) * head)
            out[:, columns] = part.astype(jnp.bfloat16)
            bias_out[:, columns] += jnp.sum(part, axis=0, keepdims=True)

    by_block = lambda width: pl.BlockSpec((rows, width), lambda b, h: (b, 0))
    return pl.pallas_call(
        body,
        cost_estimate=small_cost,
        grid_spec=pltpu.PrefetchScalarGridSpec(
            num_scalar_prefetch=1,
            grid=(2,),
            in_specs=[
                by_block(head),
                by_block(2 * head),
                pl.BlockSpec((rows, 2 * head), lambda b, h: (1 - b, 0)),
                pl.BlockSpec((rows, 2 * head), lambda b, h: (0, 0)),
                by_block(128),
                by_block(128),
            ],
            out_specs=[by_block(3 * head), pl.BlockSpec((1, 3 * head), lambda b, h: (0, 0))],
        ),
        out_shape=[
            shape_of((2 * rows, 3 * head), jnp.bfloat16),
            shape_of((1, 3 * head), jnp.float32),
        ],
        name="rotated_back",
    )(later_of, query_grad, own_part, before_part, from_later, cosines, sines)


def branch_rows(half, attended, activated, weight_qd, weight_contract, dtype):
    rows = attended.shape[0] // 2
    tile = 512
    depth = weight_qd.shape[0]

    def body(attended_ref, activated_ref, dense_ref, contract_ref, out):
        out[...] = (
            nt(attended_ref[...], dense_ref[...]) + nt(activated_ref[...], contract_ref[...])
        ).astype(dtype)

    return pl.pallas_call(
        body,
        cost_estimate=small_cost,
        grid=(depth // tile,),
        in_specs=[
            pl.BlockSpec((rows, attended.shape[1]), lambda j: (half, 0)),
            pl.BlockSpec((rows, activated.shape[1]), lambda j: (half, 0)),
            pl.BlockSpec((tile, attended.shape[1]), lambda j: (j, 3)),
            pl.BlockSpec((tile, activated.shape[1]), lambda j: (j, 0)),
        ],
        out_specs=pl.BlockSpec((rows, tile), lambda j: (0, j)),
        out_shape=shape_of((rows, depth), dtype),
        name="branch_%d" % half,
    )(attended, activated, weight_qd, weight_contract)


def back_rows(half, qkv_grad, pre_grad, x, weight_qd, weight_expand, vectors, dtype):
    rows = x.shape[0] // 2
    tile = 512
    depth = x.shape[1]

    def body(qkv_ref, pre_ref, x_ref, tile_ref, qd_ref, expand_ref, vector_ref, out, sums, stats):
        @pl.when(pl.program_id(0) == 0)
        def _():
            row = x_ref[...].astype(jnp.float32)
            mean = jnp.mean(row, axis=-1, keepdims=True)
            center = row - mean
            variance = jnp.mean(center * center, axis=-1, keepdims=True)
            stats[0] = jnp.broadcast_to(mean, stats.shape[1:])
            stats[1] = jnp.broadcast_to(lax.rsqrt(variance + norm_eps), stats.shape[1:])

        xhat = (tile_ref[...].astype(jnp.float32) - stats[0][:, :1]) * stats[1][:, :1]
        attn_back = nt(qkv_ref[...], qd_ref[...])
        mlp_back = nt(pre_ref[...], expand_ref[...])
        sums[0:1] = jnp.sum(attn_back * xhat, axis=0, keepdims=True)
        sums[1:2] = jnp.sum(attn_back, axis=0, keepdims=True)
        sums[2:3] = jnp.sum(mlp_back * xhat, axis=0, keepdims=True)
        sums[3:4] = jnp.sum(mlp_back, axis=0, keepdims=True)
        out[...] = (attn_back * vector_ref[0:1] + mlp_back * vector_ref[2:3]).astype(dtype)

    return pl.pallas_call(
        body,
        cost_estimate=small_cost,
        grid=(depth // tile,),
        in_specs=[
            pl.BlockSpec((rows, qkv_grad.shape[1]), lambda j: (half, 0)),
            pl.BlockSpec((rows, pre_grad.shape[1]), lambda j: (half, 0)),
            pl.BlockSpec((rows, depth), lambda j: (half, 0)),
            pl.BlockSpec((rows, tile), lambda j: (half, j)),
            pl.BlockSpec((tile, qkv_grad.shape[1]), lambda j: (j, 0)),
            pl.BlockSpec((tile, pre_grad.shape[1]), lambda j: (j, 0)),
            pl.BlockSpec((vectors.shape[0], tile), lambda j: (0, j)),
        ],
        out_specs=[
            pl.BlockSpec((rows, tile), lambda j: (0, j)),
            pl.BlockSpec((4, tile), lambda j: (0, j)),
        ],
        out_shape=[shape_of((rows, depth), dtype), shape_of((4, depth), jnp.float32)],
        scratch_shapes=[pltpu.VMEM((2, rows, 128), jnp.float32)],
        name="back_%d" % half,
    )(qkv_grad, pre_grad, x, x, weight_qd, weight_expand, vectors)


def tied(value, *others):
    return lax.optimization_barrier((value,) + others)[0]


def picked(values, index):
    rows = jnp.arange(values.shape[0], dtype=jnp.int32)
    chosen = index[:, None, None] == rows[None, :, None]
    return jnp.sum(jnp.where(chosen, values[None], 0), axis=1)


def per_device_paired(
    inputs,
    cotangent,
    segments,
    positions,
    qkv_weight,
    qkv_bias,
    dense_weight,
    expand_weight,
    expand_bias,
    contract_weight,
    norm_bias_vectors,
    moment_qkv_weight,
    moment_qkv_bias,
    moment_dense_weight,
    moment_expand_weight,
    moment_expand_bias,
    moment_contract_weight,
    moment_norm_vectors,
    second_qkv_weight,
    second_qkv_bias,
    second_dense_weight,
    second_expand_weight,
    second_expand_bias,
    second_contract_weight,
    second_norm_vectors,
):
    bf16, f32 = jnp.bfloat16, jnp.float32
    fsdp_index = lax.axis_index("fsdp")
    z = lax.axis_index("tensor")
    n_z = lax.axis_size("tensor")
    core = fsdp_index & 1
    chip = fsdp_index >> 1
    devices = range(lax.axis_size("fsdp"))
    to_core = [(i, i ^ 1) for i in devices]
    to_x = [(i, i ^ 2) for i in devices]
    to_y = [(i, i ^ 4) for i in devices]
    to_next = [(i, i + 2) for i in devices if i + 2 < len(devices)]
    to_prev = [(i + 2, i) for i in devices if i + 2 < len(devices)]
    first = core == 0
    head_dim = qkv_weight.shape[2] // 3
    shard_rows = inputs.shape[0]
    group_rows = n_z * shard_rows
    hidden = expand_weight.shape[1] // 2
    qkv_cols = 3 * head_dim
    shard_feat = expand_weight.shape[0]
    chip_feat = 2 * shard_feat

    def column_half(weight, k, width):
        return lax.dynamic_slice_in_dim(weight, k * width, width, axis=1).astype(bf16)

    def head_columns(k):
        return jnp.concatenate(
            [
                lax.dynamic_index_in_dim(qkv_weight, k, axis=1, keepdims=False),
                lax.dynamic_slice_in_dim(dense_weight, k * head_dim, head_dim, axis=1),
            ],
            axis=1,
        ).astype(bf16)

    def rows_of_chip(own, other):
        return jnp.concatenate(
            [jnp.where(first, own, other), jnp.where(first, other, own)], axis=0
        )

    x_group = lax.all_gather(inputs, "tensor", axis=0, tiled=True)
    dy_group = lax.all_gather(cotangent, "tensor", axis=0, tiled=True)

    swap_1 = send(head_columns(1 - core), "fsdp", to_core)
    block_1 = rows_of_chip(head_columns(core), swap_1)
    expand_in, contract_in = lax.optimization_barrier((expand_weight, contract_weight, swap_1))[:2]
    swap_2 = send(column_half(expand_in, 1 - core, hidden), "fsdp", to_core)
    swap_3 = send(column_half(contract_in, 1 - core, hidden), "fsdp", to_core)
    block_2 = rows_of_chip(column_half(expand_in, core, hidden), swap_2)
    contract_own, swap_3 = lax.optimization_barrier((contract_in, swap_3, block_2))[:2]
    block_3 = rows_of_chip(column_half(contract_own, core, hidden), swap_3)

    first_x, first_y = send(block_1, "fsdp", to_x), send(block_1, "fsdp", to_y)

    def passed_on(from_x, from_y, block):
        return (
            send(jnp.concatenate([from_y[:shard_feat], block], axis=0), "fsdp", to_x),
            send(jnp.concatenate([from_x[shard_feat:], block], axis=0), "fsdp", to_y),
        )

    second_x, second_y = passed_on(first_x, first_y, block_2)
    third_x, third_y = passed_on(second_x[shard_feat:], second_y[shard_feat:], block_3)
    pieces_1 = (block_1, (first_x, 0), (first_y, 0), (second_x, 0), (second_y, 0))

    segments_in, positions_in, dy_in = lax.optimization_barrier(
        (segments, positions, cotangent, block_2)
    )[:3]
    dy_sum = lax.optimization_barrier(jnp.sum(dy_in.astype(f32), axis=0, keepdims=True))
    position_other = send(positions_in, "fsdp", to_core)
    local = jnp.arange(group_rows, dtype=jnp.int32)
    groups = jnp.stack([fsdp_index, fsdp_index ^ 1, jnp.maximum(2 * chip - 1, 0)])
    seg_rows = picked(segments_in.reshape(-1, group_rows), groups)
    seg_halo = jnp.where(chip == 0, -1, seg_rows[2:])
    seg_rows = seg_rows[:2].reshape(1, 2 * group_rows)
    token_numbers = groups[:, None] * group_rows + local[None, :]
    token_rows = token_numbers[:2].reshape(1, 2 * group_rows)
    token_halo = token_numbers[2:]
    position_all = jnp.concatenate([positions_in, position_other])
    lane = jnp.arange(128, dtype=jnp.int32)
    half_rot = ROT // 2
    frequency = 10000.0 ** (-((lane % half_rot).astype(f32) * 2.0 / ROT))
    angles = jnp.where(
        lane[None, :] < ROT, position_all.astype(f32)[:, None] * frequency[None, :], 0.0
    )
    cosines = jnp.cos(angles)
    sines = jnp.sin(angles) * jnp.where(lane < half_rot, -1.0, 1.0)[None, :]
    halo_of = jnp.stack([first, ~first]).astype(jnp.int32)
    later_of = 1 - halo_of

    x_group = tied(x_group, first_x, first_y)
    x_all = jnp.concatenate([x_group, send(x_group, "fsdp", to_core)], axis=0)
    xhat, _ = normalized_row_block(x_all.astype(f32))
    xa = (xhat * norm_bias_vectors[0] + norm_bias_vectors[1]).astype(bf16)
    xm = (xhat * norm_bias_vectors[2] + norm_bias_vectors[3]).astype(bf16)

    head_bias = lax.dynamic_slice_in_dim(qkv_bias, core, 1, axis=0)
    weight_qd, qkv = qkv_product(xa, pieces_1, chip, head_bias, cosines, sines)
    kv_halo = send(
        jnp.where(first, qkv[group_rows:, head_dim:], qkv[:group_rows, head_dim:]), "fsdp", to_next
    )
    operands = (
        qkv,
        kv_halo,
        seg_rows,
        token_rows,
        seg_rows.reshape(2 * group_rows, 1),
        token_rows.reshape(2 * group_rows, 1),
        seg_halo,
        token_halo,
    )
    attended, lse = attention_forward(halo_of, operands)

    dy_group = tied(dy_group, qkv)
    dy_all = jnp.concatenate([dy_group, send(dy_group, "fsdp", to_core)], axis=0)

    third_x, third_y = lax.optimization_barrier((third_x, third_y, qkv))[:2]
    last_x = send(third_y[shard_feat : 2 * shard_feat], "fsdp", to_x)
    last_y = send(third_x[2 * shard_feat :], "fsdp", to_y)
    pieces_2 = (
        block_2,
        (second_x, shard_feat),
        (second_y, shard_feat),
        (third_x, 0),
        (third_y, 0),
    )
    pieces_3 = (block_3, (third_x, shard_feat), (third_y, shard_feat), (last_x, 0), (last_y, 0))
    expand_bias_half = lax.dynamic_slice_in_dim(expand_bias, core * hidden, hidden).reshape(1, -1)
    weight_expand, activated, slope = expand_product(xm, pieces_2, chip, expand_bias_half)

    def block_of(left, right, r):
        columns = lax.dynamic_slice_in_dim(left, (chip ^ r) * chip_feat, chip_feat, axis=1)
        return contract_rows(columns, right)

    def diagonal(left, right):
        return block_of(left, right, 3).astype(bf16)

    def sent_diagonal(block):
        return (
            send(block[:shard_feat], "fsdp", to_x),
            send(block[shard_feat:], "fsdp", to_y),
        )

    def neighbours(left, right, got):
        zero = jnp.zeros_like(got[0])
        for_x = block_of(left, right, 1) + jnp.concatenate([zero, got[1]], axis=0).astype(f32)
        for_y = block_of(left, right, 2) + jnp.concatenate([got[0], zero], axis=0).astype(f32)
        return for_x.astype(bf16), for_y.astype(bf16)

    def sent_neighbours(blocks):
        return send(blocks[0], "fsdp", to_x), send(blocks[1], "fsdp", to_y)

    def own_gradient(left, right, got):
        total = block_of(left, right, 0) + got[0].astype(f32) + got[1].astype(f32)
        kept = lax.dynamic_slice_in_dim(total, core * shard_feat, shard_feat, axis=0)
        given = lax.dynamic_slice_in_dim(total, (1 - core) * shard_feat, shard_feat, axis=0)
        taken = send(given, "fsdp", to_core)
        return jnp.where(first, kept, taken), jnp.where(first, taken, kept)

    dc_right = tied(jnp.concatenate([attended, activated], axis=1), last_x, last_y)
    dc_diagonal = diagonal(dy_all, dc_right)
    dc_got = sent_diagonal(dc_diagonal)
    attn_dy = tied(dy_all, dc_diagonal)
    attn_grad = product(attn_dy, weight_qd[:, qkv_cols:]).astype(bf16)
    query_grad, before_part, own_part = attention_backward(
        halo_of, operands, lse, attended, attn_grad
    )
    from_later = send(
        jnp.where(first, before_part[:group_rows], before_part[group_rows:]).astype(bf16),
        "fsdp",
        to_prev,
    )

    weight_contract, pre_grad, expand_bias_part = contract_product(
        dy_all, pieces_3, chip, tied(slope, before_part)
    )
    dc_next = neighbours(tied(dy_all, pre_grad), dc_right, dc_got)
    dc_from = sent_neighbours(dc_next)
    qkv_grad, qkv_bias_part = rotated_back(
        later_of, tied(query_grad, dc_next), own_part, before_part, from_later, cosines, sines
    )
    qkv_diagonal = diagonal(xa, qkv_grad)
    qkv_got = sent_diagonal(qkv_diagonal)
    expand_diagonal = diagonal(tied(xm, qkv_diagonal), pre_grad)
    expand_got = sent_diagonal(expand_diagonal)

    branch_weight = tied(weight_contract, expand_diagonal)
    rows_of = lambda half, dtype: branch_rows(
        half, attended, activated, weight_qd, branch_weight, dtype
    )
    branch_other = send(rows_of(1, bf16), "fsdp", to_core)
    branch_rows_own = (rows_of(0, f32) + branch_other.astype(f32)).astype(bf16)
    backs = lambda half, back_x, dtype: back_rows(
        half, qkv_grad, pre_grad, back_x, weight_qd, weight_expand, norm_bias_vectors, dtype
    )
    qkv_next = neighbours(tied(xa, branch_rows_own, dc_from), qkv_grad, qkv_got)
    qkv_from = sent_neighbours(qkv_next)
    expand_next = neighbours(tied(xm, qkv_next), pre_grad, expand_got)
    expand_from = sent_neighbours(expand_next)
    weighted_other, sums_other = backs(1, tied(x_all, expand_next), bf16)
    weighted_other = send(weighted_other, "fsdp", to_core)
    weighted_own, sums_own = backs(0, tied(x_all, sums_other, qkv_from), f32)
    branch_sum = lax.psum_scatter(branch_rows_own, "tensor", scatter_dimension=0, tiled=True)
    vector_part = jnp.concatenate(
        [sums_own + sums_other, dy_sum], axis=0
    )
    bias_part = jnp.concatenate([qkv_bias_part, expand_bias_part], axis=1)
    n_vector = vector_part.size
    small = jnp.concatenate([vector_part.reshape(-1), bias_part.reshape(-1)]).reshape(-1, 128)
    small = small + send(small, "fsdp", to_x)
    small = small + send(small, "fsdp", to_y)
    small_other = send(small, "fsdp", to_core)
    flat, flat_other = small.reshape(-1), small_other.reshape(-1)
    vector_sum = (flat[:n_vector] + flat_other[:n_vector]).reshape(-1, 128)
    for bit in (1, 2):
        vector_sum = vector_sum + send(
            vector_sum, "tensor", [(i, i ^ bit) for i in range(n_z)]
        )
    vector_sum = vector_sum.reshape(vector_part.shape)
    grad_norm_vectors = jnp.concatenate([vector_sum, vector_sum[4:]], axis=0)
    bias_first = jnp.where(first, flat[n_vector:], flat_other[n_vector:])
    bias_second = jnp.where(first, flat_other[n_vector:], flat[n_vector:])
    grad_qkv_bias = jnp.stack([bias_first[:qkv_cols], bias_second[:qkv_cols]])
    grad_expand_bias = jnp.concatenate([bias_first[qkv_cols:], bias_second[qkv_cols:]])
    weighted_rows = (weighted_own + weighted_other.astype(f32)).astype(bf16)
    weighted_rows = tied(weighted_rows, branch_sum)
    weighted = lax.psum_scatter(
        weighted_rows, "tensor", scatter_dimension=0, tiled=True
    ).astype(f32)
    output = (
        inputs.astype(f32) + branch_sum.astype(f32) + norm_bias_vectors[4] + norm_bias_vectors[5]
    )
    xhat_own, inverse_own = normalized_row_block(inputs.astype(f32))
    block_input_gradient = cotangent.astype(f32) + inverse_own * (
        weighted
        - jnp.mean(weighted, axis=-1, keepdims=True)
        - xhat_own * jnp.mean(weighted * xhat_own, axis=-1, keepdims=True)
    )

    dc_halves = own_gradient(dy_all, dc_right, dc_from)
    qkv_halves = own_gradient(xa, qkv_grad, qkv_from)
    expand_halves = own_gradient(xm, pre_grad, expand_from)
    dc_halves, qkv_halves = lax.optimization_barrier((dc_halves, qkv_halves, weighted_rows))[:2]
    grad_contract_weight = jnp.concatenate([part[:, head_dim:] for part in dc_halves], axis=1)
    grad_dense_weight = jnp.concatenate([part[:, :head_dim] for part in dc_halves], axis=1)
    grad_expand_weight = jnp.concatenate(expand_halves, axis=1)
    grad_qkv_weight = jnp.stack(qkv_halves, axis=1)
    new_qkv_weight, new_moment_qkv_weight, new_second_qkv_weight = adam_step(
        qkv_weight,
        grad_qkv_weight,
        moment_qkv_weight,
        second_qkv_weight,
        rate_qkv_weight,
        decay_matrix,
    )
    new_qkv_bias, new_moment_qkv_bias, new_second_qkv_bias = adam_step(
        qkv_bias, grad_qkv_bias, moment_qkv_bias, second_qkv_bias, rate_qkv_bias, 0.0
    )
    new_dense_weight, new_moment_dense_weight, new_second_dense_weight = adam_step(
        dense_weight,
        grad_dense_weight,
        moment_dense_weight,
        second_dense_weight,
        rate_dense_weight,
        decay_matrix,
    )
    new_expand_weight, new_moment_expand_weight, new_second_expand_weight = adam_step(
        expand_weight,
        grad_expand_weight,
        moment_expand_weight,
        second_expand_weight,
        rate_expand_weight,
        decay_matrix,
    )
    new_expand_bias, new_moment_expand_bias, new_second_expand_bias = adam_step(
        expand_bias, grad_expand_bias, moment_expand_bias, second_expand_bias, rate_expand_bias, 0.0
    )
    new_contract_weight, new_moment_contract_weight, new_second_contract_weight = adam_step(
        contract_weight,
        grad_contract_weight,
        moment_contract_weight,
        second_contract_weight,
        rate_contract_weight,
        decay_matrix,
    )
    new_norm_vectors, new_moment_norm_vectors, new_second_norm_vectors = adam_step(
        norm_bias_vectors,
        grad_norm_vectors,
        moment_norm_vectors,
        second_norm_vectors,
        rate_norm_vectors,
        0.0,
    )
    return (
        output,
        block_input_gradient,
        grad_qkv_weight,
        new_qkv_weight,
        new_moment_qkv_weight,
        new_second_qkv_weight,
        grad_qkv_bias,
        new_qkv_bias,
        new_moment_qkv_bias,
        new_second_qkv_bias,
        grad_dense_weight,
        new_dense_weight,
        new_moment_dense_weight,
        new_second_dense_weight,
        grad_expand_weight,
        new_expand_weight,
        new_moment_expand_weight,
        new_second_expand_weight,
        grad_expand_bias,
        new_expand_bias,
        new_moment_expand_bias,
        new_second_expand_bias,
        grad_contract_weight,
        new_contract_weight,
        new_moment_contract_weight,
        new_second_contract_weight,
        grad_norm_vectors,
        new_norm_vectors,
        new_moment_norm_vectors,
        new_second_norm_vectors,
    )


def solution(mesh):
    paired = mesh.shape["fsdp"] == 8 and mesh.shape["tensor"] == 4
    per_device = per_device_paired if paired else per_device_generic
    return jax.shard_map(
        per_device,
        mesh=mesh,
        in_specs=(
            P(("fsdp", "tensor"), None),
            P(("fsdp", "tensor"), None),
            P(),
            P("fsdp"),
            P("fsdp", "tensor", None),
            P("tensor", None),
            P("fsdp", "tensor"),
            P("fsdp", "tensor"),
            P("tensor"),
            P("fsdp", "tensor"),
            P(),
            P("fsdp", "tensor", None),
            P("tensor", None),
            P("fsdp", "tensor"),
            P("fsdp", "tensor"),
            P("tensor"),
            P("fsdp", "tensor"),
            P(),
            P("fsdp", "tensor", None),
            P("tensor", None),
            P("fsdp", "tensor"),
            P("fsdp", "tensor"),
            P("tensor"),
            P("fsdp", "tensor"),
            P(),
        ),
        out_specs=(
            P(("fsdp", "tensor"), None),
            P(("fsdp", "tensor"), None),
            P("fsdp", "tensor", None),
            P("fsdp", "tensor", None),
            P("fsdp", "tensor", None),
            P("fsdp", "tensor", None),
            P("tensor", None),
            P("tensor", None),
            P("tensor", None),
            P("tensor", None),
            P("fsdp", "tensor"),
            P("fsdp", "tensor"),
            P("fsdp", "tensor"),
            P("fsdp", "tensor"),
            P("fsdp", "tensor"),
            P("fsdp", "tensor"),
            P("fsdp", "tensor"),
            P("fsdp", "tensor"),
            P("tensor"),
            P("tensor"),
            P("tensor"),
            P("tensor"),
            P("fsdp", "tensor"),
            P("fsdp", "tensor"),
            P("fsdp", "tensor"),
            P("fsdp", "tensor"),
            P(),
            P(),
            P(),
            P(),
        ),
        check_vma=False,
    )
```

```python
import jax
import jax.numpy as jnp
from jax import lax
from jax.experimental import pallas as pl
from jax.experimental.pallas import tpu as pltpu
from jax.sharding import PartitionSpec as P

ROT = 64
STEP = 3


norm_eps = 1e-05
masked_score = -1e30
beta_one = 0.9
beta_two = 0.95
adam_eps = 1e-08
decay_matrix = 0.01
rate_qkv_weight = 0.005
rate_qkv_bias = 0.02
rate_dense_weight = 0.04
rate_expand_weight = 0.005
rate_expand_bias = 0.02
rate_contract_weight = 0.003
rate_norm_vectors = 0.1


def shifted(value, axis, steps):
    count = lax.axis_size(axis)
    first, last = (max(0, -steps), min(count, count - steps))
    return lax.ppermute(value, axis, [(source, source + steps) for source in range(first, last)])


def normalized_row_block(row_values):
    center = row_values - jnp.mean(row_values, axis=-1, keepdims=True)
    variance = jnp.mean(center * center, axis=-1, keepdims=True)
    inverse_deviation = lax.rsqrt(variance + norm_eps)
    return (center * inverse_deviation, inverse_deviation)


def norm_backward_term(upstream_gradient, gain_vector_row, centered_normalized, inverse_deviation):
    scaled_rows = upstream_gradient * gain_vector_row
    return inverse_deviation * (
        scaled_rows
        - jnp.mean(scaled_rows, axis=-1, keepdims=True)
        - centered_normalized * jnp.mean(scaled_rows * centered_normalized, axis=-1, keepdims=True)
    )


def rotary_tables(token_pos):
    half_rot = ROT // 2
    frequency = 10000.0 ** (-(jnp.arange(half_rot, dtype=jnp.float32) * 2.0 / ROT))
    angles = token_pos.astype(jnp.float32)[:, None] * frequency[None, :]
    return (jnp.cos(angles)[:, None, :], jnp.sin(angles)[:, None, :])


def rotate(head_values, cosine_rotation, sine_rotation_table, direction):
    half_rot = ROT // 2
    first_half = head_values[..., :half_rot]
    second_half = head_values[..., half_rot:ROT]
    return jnp.concatenate(
        [
            first_half * cosine_rotation - direction * second_half * sine_rotation_table,
            second_half * cosine_rotation + direction * first_half * sine_rotation_table,
            head_values[..., ROT:],
        ],
        axis=-1,
    )


def gelu_slope(pre_values):
    return (
        0.5 * (1.0 + lax.erf(pre_values * 0.7071067811865476))
        + pre_values * jnp.exp(-0.5 * pre_values * pre_values) * 0.3989422804014327
    )


def key_mask(seg_query, query_index, seg_keys, group_rows, has_prev):
    key_index = jnp.arange(seg_keys.shape[0], dtype=jnp.int32)
    causal = key_index[None, :] <= query_index[:, None]
    same_doc = seg_keys[None, :] == seg_query[:, None]
    present = (key_index[None, :] >= group_rows) | has_prev
    return causal & same_doc & present


def block_scores(query_blk, keys_all, allowed, score_scale):
    scores = (
        jnp.einsum("qhc,khc->hqk", query_blk, keys_all, preferred_element_type=jnp.float32)
        * score_scale
    )
    return jnp.where(allowed[None], scores, masked_score)


def adam_step(parameter, gradient, moment, second, step_rate, decay_weight):
    moment_new = beta_one * moment + (1.0 - beta_one) * gradient
    second_new = beta_two * second + (1.0 - beta_two) * gradient * gradient
    moment_hat = moment_new / (1.0 - beta_one**STEP)
    second_hat = second_new / (1.0 - beta_two**STEP)
    updated = parameter - step_rate * (
        moment_hat / (jnp.sqrt(second_hat) + adam_eps) + decay_weight * parameter
    )
    return (updated, moment_new, second_new)


def contract_rows(left_rows, right_rows):
    return lax.dot_general(
        left_rows, right_rows, (((0,), (0,)), ((), ())), preferred_element_type=jnp.float32
    )


def contract_cols(left_cols, right_cols):
    return lax.dot_general(
        left_cols, right_cols, (((1,), (1,)), ((), ())), preferred_element_type=jnp.float32
    )


def per_device_generic(
    inputs,
    cotangent,
    segments,
    positions,
    qkv_weight,
    qkv_bias,
    dense_weight,
    expand_weight,
    expand_bias,
    contract_weight,
    norm_bias_vectors,
    moment_qkv_weight,
    moment_qkv_bias,
    moment_dense_weight,
    moment_expand_weight,
    moment_expand_bias,
    moment_contract_weight,
    moment_norm_vectors,
    second_qkv_weight,
    second_qkv_bias,
    second_dense_weight,
    second_expand_weight,
    second_expand_bias,
    second_contract_weight,
    second_norm_vectors,
):
    fsdp_index = lax.axis_index("fsdp")
    input_row_block, rows_dy = (
        lax.all_gather(inputs, "tensor", axis=0, tiled=True),
        lax.all_gather(cotangent, "tensor", axis=0, tiled=True),
    )
    group_rows = input_row_block.shape[0]
    shards_bf = (
        qkv_weight.astype(jnp.bfloat16),
        dense_weight.astype(jnp.bfloat16),
        expand_weight.astype(jnp.bfloat16),
        contract_weight.astype(jnp.bfloat16),
    )
    forward_set = (
        lax.all_gather(shards_bf[0], "fsdp", axis=0, tiled=True),
        lax.all_gather(shards_bf[1], "fsdp", axis=0, tiled=True),
        lax.all_gather(shards_bf[2], "fsdp", axis=0, tiled=True),
        lax.all_gather(shards_bf[3], "fsdp", axis=0, tiled=True),
    )
    full_qkv, full_dense, full_expand, full_contract = forward_set
    row_centered_normalized, inverse_row_deviation = normalized_row_block(
        input_row_block.astype(jnp.float32)
    )
    attention_normalized_input = (
        row_centered_normalized * norm_bias_vectors[0] + norm_bias_vectors[1]
    ).astype(jnp.bfloat16)
    feedforward_normalized_input = (
        row_centered_normalized * norm_bias_vectors[2] + norm_bias_vectors[3]
    ).astype(jnp.bfloat16)
    projected = (
        jnp.einsum(
            "rd,dhc->rhc", attention_normalized_input, full_qkv, preferred_element_type=jnp.float32
        )
        + qkv_bias[None]
    )
    heads_dev = projected.shape[1]
    head_dim = projected.shape[2] // 3
    score_scale = head_dim ** (-0.5)
    cosine_rotation, sine_rotation_table = rotary_tables(positions)
    query_rows = rotate(
        projected[..., :head_dim], cosine_rotation, sine_rotation_table, 1.0
    ).astype(jnp.bfloat16)
    local_segment_keys = rotate(
        projected[..., head_dim : 2 * head_dim], cosine_rotation, sine_rotation_table, 1.0
    ).astype(jnp.bfloat16)
    local_segment_values = projected[..., 2 * head_dim :].astype(jnp.bfloat16)
    keys_prev, values_prev = shifted((local_segment_keys, local_segment_values), "fsdp", 1)
    keys_all = jnp.concatenate([keys_prev, local_segment_keys], axis=0)
    values_all = jnp.concatenate([values_prev, local_segment_values], axis=0)
    seg_own = lax.dynamic_slice_in_dim(segments, fsdp_index * group_rows, group_rows)
    seg_prev = lax.dynamic_slice_in_dim(
        segments, jnp.maximum(fsdp_index - 1, 0) * group_rows, group_rows
    )
    seg_keys = jnp.concatenate([seg_prev, seg_own], axis=0)
    has_prev = fsdp_index > 0
    block_rows = min(512, group_rows)
    blocks = group_rows // block_rows
    starts = jnp.arange(blocks, dtype=jnp.int32) * block_rows
    local_index = jnp.arange(block_rows, dtype=jnp.int32)
    query_blocks = query_rows.reshape(blocks, block_rows, heads_dev, head_dim)
    seg_blocks = seg_own.reshape(blocks, block_rows)

    def forward_block(block_data):
        query_blk, seg_blk, start = block_data
        allowed = key_mask(
            seg_blk, group_rows + start + local_index, seg_keys, group_rows, has_prev
        )
        scores = block_scores(query_blk, keys_all, allowed, score_scale)
        row_max = jnp.max(scores, axis=-1, keepdims=True)
        row_total = jnp.sum(jnp.exp(scores - row_max), axis=-1, keepdims=True)
        log_total = row_max + jnp.log(row_total)
        prob_bf = jnp.exp(scores - log_total).astype(jnp.bfloat16)
        result = jnp.einsum("hqk,khc->qhc", prob_bf, values_all, preferred_element_type=jnp.float32)
        return (result.astype(jnp.bfloat16), log_total[..., 0])

    attn_blocks, lse_blocks = lax.map(forward_block, (query_blocks, seg_blocks, starts))
    attended = attn_blocks.reshape(group_rows, heads_dev * head_dim)
    expand_preactivation = (
        jnp.dot(feedforward_normalized_input, full_expand, preferred_element_type=jnp.float32)
        + expand_bias
    )
    gelu_activated_rows = jax.nn.gelu(expand_preactivation, approximate=False).astype(jnp.bfloat16)
    branch_sum = lax.psum_scatter(
        contract_cols(attended, full_dense) + contract_cols(gelu_activated_rows, full_contract),
        "tensor",
        scatter_dimension=0,
        tiled=True,
    )
    output = inputs.astype(jnp.float32) + branch_sum + norm_bias_vectors[4] + norm_bias_vectors[5]
    back_qkv, back_dense, back_expand, back_contract = forward_set
    act_grad = jnp.dot(rows_dy, back_contract, preferred_element_type=jnp.float32)
    pre_grad32 = act_grad * gelu_slope(expand_preactivation)
    pre_grad = pre_grad32.astype(jnp.bfloat16)
    attn_grad = jnp.dot(rows_dy, back_dense, preferred_element_type=jnp.float32).astype(
        jnp.bfloat16
    )
    attn_heads = attn_grad.reshape(group_rows, heads_dev, head_dim)
    row_delta = jnp.sum(
        attn_heads.astype(jnp.float32)
        * attended.reshape(group_rows, heads_dev, head_dim).astype(jnp.float32),
        axis=-1,
    )

    def backward_block(inner_carry, block_data):
        key_acc, value_acc = inner_carry
        query_blk, seg_blk, start, grad_blk, delta_blk, lse_blk = block_data
        allowed = key_mask(
            seg_blk, group_rows + start + local_index, seg_keys, group_rows, has_prev
        )
        scores = block_scores(query_blk, keys_all, allowed, score_scale)
        prob_f32 = jnp.exp(scores - lse_blk[..., None])
        prob_bf = prob_f32.astype(jnp.bfloat16)
        dot_grad = jnp.einsum(
            "qhc,khc->hqk", grad_blk, values_all, preferred_element_type=jnp.float32
        )
        score_grad = (
            prob_f32 * (dot_grad - jnp.transpose(delta_blk)[..., None]) * score_scale
        ).astype(jnp.bfloat16)
        query_grad = jnp.einsum(
            "hqk,khc->qhc", score_grad, keys_all, preferred_element_type=jnp.float32
        )
        key_acc = key_acc + jnp.einsum(
            "hqk,qhc->khc", score_grad, query_blk, preferred_element_type=jnp.float32
        )
        value_acc = value_acc + jnp.einsum(
            "hqk,qhc->khc", prob_bf, grad_blk, preferred_element_type=jnp.float32
        )
        return ((key_acc, value_acc), query_grad)

    zero_keys = jnp.zeros((2 * group_rows, heads_dev, head_dim), jnp.float32)
    inner_final, query_grads = lax.scan(
        backward_block,
        (zero_keys, zero_keys),
        (
            query_blocks,
            seg_blocks,
            starts,
            attn_heads.reshape(blocks, block_rows, heads_dev, head_dim),
            row_delta.reshape(blocks, block_rows, heads_dev),
            lse_blocks,
        ),
    )
    key_acc, value_acc = inner_final
    later_key_grad, later_value_grad = shifted(
        (key_acc[:group_rows], value_acc[:group_rows]), "fsdp", -1
    )
    key_grad = key_acc[group_rows:] + later_key_grad
    value_grad = value_acc[group_rows:] + later_value_grad
    query_grad = query_grads.reshape(group_rows, heads_dev, head_dim)
    qkv_grad32 = jnp.concatenate(
        [
            rotate(query_grad, cosine_rotation, sine_rotation_table, -1.0),
            rotate(key_grad, cosine_rotation, sine_rotation_table, -1.0),
            value_grad,
        ],
        axis=-1,
    )
    qkv_grad = qkv_grad32.astype(jnp.bfloat16)
    attn_norm_grad = jnp.einsum(
        "rhc,dhc->rd", qkv_grad, back_qkv, preferred_element_type=jnp.float32
    )
    mlp_norm_grad = contract_cols(pre_grad, back_expand)
    qkv_part = jnp.einsum(
        "rd,rhc->dhc", attention_normalized_input, qkv_grad, preferred_element_type=jnp.float32
    )
    dense_part = contract_rows(rows_dy, attended)
    expand_part = contract_rows(feedforward_normalized_input, pre_grad)
    contract_part = contract_rows(rows_dy, gelu_activated_rows)
    local_centered_normalized, inverse_local_deviation = normalized_row_block(
        inputs.astype(jnp.float32)
    )
    dy_local = cotangent.astype(jnp.float32)
    dy_column_sum = jnp.sum(dy_local, axis=0)
    attention_backward_term, feedforward_backward_term = (
        lax.psum_scatter(attn_norm_grad, "tensor", scatter_dimension=0, tiled=True),
        lax.psum_scatter(mlp_norm_grad, "tensor", scatter_dimension=0, tiled=True),
    )
    block_input_gradient = (
        dy_local
        + norm_backward_term(
            attention_backward_term,
            norm_bias_vectors[0],
            local_centered_normalized,
            inverse_local_deviation,
        )
        + norm_backward_term(
            feedforward_backward_term,
            norm_bias_vectors[2],
            local_centered_normalized,
            inverse_local_deviation,
        )
    )
    vector_part = jnp.stack(
        [
            jnp.sum(attention_backward_term * local_centered_normalized, axis=0),
            jnp.sum(attention_backward_term, axis=0),
            jnp.sum(feedforward_backward_term * local_centered_normalized, axis=0),
            jnp.sum(feedforward_backward_term, axis=0),
            dy_column_sum,
            dy_column_sum,
        ]
    )
    qkv_bias_part = jnp.sum(qkv_grad32, axis=0)
    expand_bias_part = jnp.sum(pre_grad32, axis=0)
    grad_qkv_weight, grad_dense_weight, grad_expand_weight, grad_contract_weight = (
        lax.psum_scatter(qkv_part, "fsdp", scatter_dimension=0, tiled=True),
        lax.psum_scatter(dense_part, "fsdp", scatter_dimension=0, tiled=True),
        lax.psum_scatter(expand_part, "fsdp", scatter_dimension=0, tiled=True),
        lax.psum_scatter(contract_part, "fsdp", scatter_dimension=0, tiled=True),
    )
    grad_qkv_bias, grad_expand_bias, vector_fsdp = lax.psum(
        (qkv_bias_part, expand_bias_part, vector_part), "fsdp"
    )
    grad_norm_vectors = lax.psum(vector_fsdp, "tensor")
    new_qkv_weight, new_moment_qkv_weight, new_second_qkv_weight = adam_step(
        qkv_weight,
        grad_qkv_weight,
        moment_qkv_weight,
        second_qkv_weight,
        rate_qkv_weight,
        decay_matrix,
    )
    new_qkv_bias, new_moment_qkv_bias, new_second_qkv_bias = adam_step(
        qkv_bias, grad_qkv_bias, moment_qkv_bias, second_qkv_bias, rate_qkv_bias, 0.0
    )
    new_dense_weight, new_moment_dense_weight, new_second_dense_weight = adam_step(
        dense_weight,
        grad_dense_weight,
        moment_dense_weight,
        second_dense_weight,
        rate_dense_weight,
        decay_matrix,
    )
    new_expand_weight, new_moment_expand_weight, new_second_expand_weight = adam_step(
        expand_weight,
        grad_expand_weight,
        moment_expand_weight,
        second_expand_weight,
        rate_expand_weight,
        decay_matrix,
    )
    new_expand_bias, new_moment_expand_bias, new_second_expand_bias = adam_step(
        expand_bias, grad_expand_bias, moment_expand_bias, second_expand_bias, rate_expand_bias, 0.0
    )
    new_contract_weight, new_moment_contract_weight, new_second_contract_weight = adam_step(
        contract_weight,
        grad_contract_weight,
        moment_contract_weight,
        second_contract_weight,
        rate_contract_weight,
        decay_matrix,
    )
    new_norm_vectors, new_moment_norm_vectors, new_second_norm_vectors = adam_step(
        norm_bias_vectors,
        grad_norm_vectors,
        moment_norm_vectors,
        second_norm_vectors,
        rate_norm_vectors,
        0.0,
    )
    return (
        output,
        block_input_gradient,
        grad_qkv_weight,
        new_qkv_weight,
        new_moment_qkv_weight,
        new_second_qkv_weight,
        grad_qkv_bias,
        new_qkv_bias,
        new_moment_qkv_bias,
        new_second_qkv_bias,
        grad_dense_weight,
        new_dense_weight,
        new_moment_dense_weight,
        new_second_dense_weight,
        grad_expand_weight,
        new_expand_weight,
        new_moment_expand_weight,
        new_second_expand_weight,
        grad_expand_bias,
        new_expand_bias,
        new_moment_expand_bias,
        new_second_expand_bias,
        grad_contract_weight,
        new_contract_weight,
        new_moment_contract_weight,
        new_second_contract_weight,
        grad_norm_vectors,
        new_norm_vectors,
        new_moment_norm_vectors,
        new_second_norm_vectors,
    )


def send(value, axis, pairs):
    return lax.ppermute(value, axis, pairs)


def product(left, right):
    return jnp.dot(left, right, preferred_element_type=jnp.float32)


small_cost = pl.CostEstimate(flops=1024, bytes_accessed=1024, transcendentals=0)


def shape_of(shape, dtype):
    return jax.ShapeDtypeStruct(shape, dtype)


def gathered_product(left, pieces, chip, extras, outputs, finish, live, name):
    tile = 256
    columns = pieces[0].shape[1]
    rows, depth = left.shape
    chip_rows = pieces[0].shape[0]
    half_rows = chip_rows // 2
    arrays = [pieces[0]] + [array for array, _ in pieces[1:]]
    starts = [0] + [start for _, start in pieces[1:]]

    def body(chip_ref, left_ref, block, from_x, from_y, top, bottom, *refs):
        weight_ref = refs[len(extras)]
        parts = (
            (block, 0, 0, chip_rows),
            (from_x, 1, 0, chip_rows),
            (from_y, 2, 0, chip_rows),
            (top, 3, 0, half_rows),
            (bottom, 3, half_rows, half_rows),
        )
        for (part, flip, shift, height), source in zip(parts, starts):
            start = pl.multiple_of((chip_ref[0] ^ flip) * chip_rows + shift, half_rows)
            weight_ref[pl.ds(start, height), :] = part[source : source + height, :]
        step = pl.program_id(0)

        @pl.when(step < live)
        def _():
            result = product(left_ref[...], weight_ref[...])
            finish(step, result, refs[: len(extras)], refs[len(extras) + 1 :])

    def spec_of(height, moves):
        if moves:
            return pl.BlockSpec((height, tile), lambda j, c: (0, jnp.minimum(j, live - 1)))
        return pl.BlockSpec((height, 128), lambda j, c: (0, 0))

    column_spec = lambda height: pl.BlockSpec((height, tile), lambda j, c: (0, j))
    return pl.pallas_call(
        body,
        cost_estimate=small_cost,
        grid_spec=pltpu.PrefetchScalarGridSpec(
            num_scalar_prefetch=1,
            grid=(columns // tile,),
            in_specs=[pl.BlockSpec((rows, depth), lambda j, c: (0, 0))]
            + [column_spec(array.shape[0]) for array in arrays]
            + [spec_of(extra.shape[0], moves) for extra, moves in extras],
            out_specs=[column_spec(depth)] + [spec_of(out.shape[0], True) for out in outputs],
        ),
        out_shape=[shape_of((depth, columns), left.dtype)] + outputs,
        name=name,
    )(chip.reshape(1), left, *arrays, *[extra for extra, _ in extras])


def partner_lanes(head):
    half_rot = ROT // 2
    lane = lax.broadcasted_iota(jnp.int32, head.shape, 1)
    return jnp.where(
        lane < half_rot,
        pltpu.roll(head, head.shape[1] - half_rot, 1),
        pltpu.roll(head, half_rot, 1),
    )


def qkv_product(left, pieces, chip, bias, cosines, sines):
    rows = left.shape[0]
    columns = bias.shape[1]

    def finish(step, result, extras, outs):
        bias_ref, cosine_ref, sine_ref = extras
        value = result + bias_ref[...]
        head = value[:, :128]
        turned = head * cosine_ref[...] + partner_lanes(head) * sine_ref[...]
        outs[0][:, :128] = jnp.where(step < 2, turned, head).astype(jnp.bfloat16)
        outs[0][:, 128:] = value[:, 128:].astype(jnp.bfloat16)

    return gathered_product(
        left,
        pieces,
        chip,
        [(bias, True), (cosines, False), (sines, False)],
        [shape_of((rows, columns), jnp.bfloat16)],
        finish,
        3,
        "qkv",
    )


def expand_product(left, pieces, chip, bias):
    shape = (left.shape[0], bias.shape[1])

    def finish(step, result, extras, outs):
        pre = result + extras[0][...]
        distribution = 0.5 * (1.0 + lax.erf(pre * 0.7071067811865476))
        outs[0][...] = (pre * distribution).astype(jnp.bfloat16)
        outs[1][...] = distribution + pre * jnp.exp(-0.5 * pre * pre) * 0.3989422804014327

    return gathered_product(
        left,
        pieces,
        chip,
        [(bias, True)],
        [shape_of(shape, jnp.bfloat16), shape_of(shape, jnp.float32)],
        finish,
        4,
        "expand",
    )


def contract_product(left, pieces, chip, slope):
    def finish(step, result, extras, outs):
        gradient = result * extras[0][...]
        outs[0][...] = gradient.astype(jnp.bfloat16)
        outs[1][...] = jnp.sum(gradient, axis=0, keepdims=True)

    return gathered_product(
        left,
        pieces,
        chip,
        [(slope, True)],
        [shape_of(slope.shape, jnp.bfloat16), shape_of((1, slope.shape[1]), jnp.float32)],
        finish,
        4,
        "contract",
    )


def nt(left, right):
    return lax.dot_general(
        left, right, (((1,), (1,)), ((), ())), preferred_element_type=jnp.float32
    )


def attention_call(body, halo_of, operands, extras, outputs, name):
    qkv, halo, seg_rows, token_rows, seg_columns, token_columns, seg_halo, token_halo = operands
    rows = qkv.shape[0] // 2
    head = qkv.shape[1] // 3
    block = lambda column, flip: pl.BlockSpec(
        (rows, head), lambda b, h: ((1 - b) if flip else b, column)
    )
    column_vector = pl.BlockSpec((rows, 1), lambda b, h: (b, 0))
    row_vector = lambda flip: pl.BlockSpec((1, rows), lambda b, h: (0, (1 - b) if flip else b))
    fixed = lambda value: pl.BlockSpec(value.shape, lambda b, h: (0, 0))
    by_block = lambda value: pl.BlockSpec((rows, value.shape[1]), lambda b, h: (b, 0))
    return pl.pallas_call(
        body,
        cost_estimate=small_cost,
        grid_spec=pltpu.PrefetchScalarGridSpec(
            num_scalar_prefetch=1,
            grid=(2,),
            in_specs=[
                block(0, False),
                block(1, True),
                block(2, True),
                block(1, False),
                block(2, False),
                fixed(halo),
                column_vector,
                column_vector,
                row_vector(True),
                row_vector(True),
                row_vector(False),
                row_vector(False),
                fixed(seg_halo),
                fixed(token_halo),
            ]
            + [by_block(extra) for extra in extras],
            out_specs=[by_block(out) for out in outputs],
        ),
        out_shape=outputs,
        name=name,
    )(
        halo_of,
        qkv,
        qkv,
        qkv,
        qkv,
        qkv,
        halo,
        seg_columns,
        token_columns,
        seg_rows,
        token_rows,
        seg_rows,
        token_rows,
        seg_halo,
        token_halo,
        *extras,
    )


def masked_scores(halo_of, refs, score_scale):
    (
        q_ref,
        k_before,
        v_before,
        k_ref,
        v_ref,
        halo,
        seg_q,
        token_q,
        seg_before,
        token_before,
        seg_k,
        token_k,
        seg_halo,
        token_halo,
    ) = refs
    use_halo = halo_of[pl.program_id(0)] == 1
    head = q_ref.shape[1]
    keys_before = jnp.where(use_halo, halo[:, :head], k_before[...])
    values_before = jnp.where(use_halo, halo[:, head:], v_before[...])
    segments_before = jnp.where(use_halo, seg_halo[...], seg_before[...])
    tokens_before = jnp.where(use_halo, token_halo[...], token_before[...])
    query = q_ref[...]

    def scores(keys, key_segments, key_tokens):
        allowed = (key_segments == seg_q[...]) & (key_tokens <= token_q[...])
        return jnp.where(allowed, nt(query, keys) * score_scale, masked_score)

    return (
        query,
        (keys_before, k_ref[...]),
        (values_before, v_ref[...]),
        (
            scores(keys_before, segments_before, tokens_before),
            scores(k_ref[...], seg_k[...], token_k[...]),
        ),
    )


def attention_forward(halo_of, operands):
    rows, columns = operands[0].shape
    head = columns // 3
    score_scale = head ** (-0.5)

    def body(halo_ref, *refs):
        _, _, values, scores = masked_scores(halo_ref, refs[:14], score_scale)
        out_ref, lse_ref = refs[14:]
        row_max = jnp.maximum(
            jnp.max(scores[0], axis=-1, keepdims=True), jnp.max(scores[1], axis=-1, keepdims=True)
        )
        powers = [jnp.exp(part - row_max) for part in scores]
        total = jnp.sum(powers[0], axis=-1, keepdims=True) + jnp.sum(
            powers[1], axis=-1, keepdims=True
        )
        inverse = 1.0 / total
        out_ref[...] = (
            product((powers[0] * inverse).astype(jnp.bfloat16), values[0])
            + product((powers[1] * inverse).astype(jnp.bfloat16), values[1])
        ).astype(jnp.bfloat16)
        lse_ref[...] = row_max + jnp.log(total)

    return attention_call(
        body,
        halo_of,
        operands,
        [],
        [shape_of((rows, head), jnp.bfloat16), shape_of((rows, 1), jnp.float32)],
        "attention",
    )


def attention_backward(halo_of, operands, lse, attended, attn_grad):
    rows, columns = operands[0].shape
    head = columns // 3
    score_scale = head ** (-0.5)

    def body(halo_ref, *refs):
        query, keys, values, scores = masked_scores(halo_ref, refs[:14], score_scale)
        lse_ref, attended_ref, grad_ref, query_out, before_out, own_out = refs[14:]
        gradient = grad_ref[...]
        row_delta = jnp.sum(
            gradient.astype(jnp.float32) * attended_ref[...].astype(jnp.float32),
            axis=-1,
            keepdims=True,
        )
        query_grad = 0.0
        for part, out in enumerate((before_out, own_out)):
            probs = jnp.exp(scores[part] - lse_ref[...])
            score_grad = (
                probs * (nt(gradient, values[part]) - row_delta) * score_scale
            ).astype(jnp.bfloat16)
            query_grad = query_grad + product(score_grad, keys[part])
            out[:, :head] = contract_rows(score_grad, query)
            out[:, head:] = contract_rows(probs.astype(jnp.bfloat16), gradient)
        query_out[...] = query_grad

    return attention_call(
        body,
        halo_of,
        operands,
        [lse, attended, attn_grad],
        [
            shape_of((rows, head), jnp.float32),
            shape_of((rows, 2 * head), jnp.float32),
            shape_of((rows, 2 * head), jnp.float32),
        ],
        "attention_back",
    )


def rotated_back(later_of, query_grad, own_part, before_part, from_later, cosines, sines):
    rows = query_grad.shape[0] // 2
    head = query_grad.shape[1]

    def body(later_ref, query_ref, own_ref, before_ref, later_grad, cosine, sine, out, bias_out):
        step = pl.program_id(0)
        extra = jnp.where(
            later_ref[step] == 1, later_grad[...].astype(jnp.float32), before_ref[...]
        )
        pairs = own_ref[...] + extra

        def back(value):
            lanes = value[:, :128]
            lanes = lanes * cosine[...] - partner_lanes(lanes) * sine[...]
            return jnp.concatenate([lanes, value[:, 128:]], axis=1)

        @pl.when(step == 0)
        def _():
            bias_out[...] = jnp.zeros_like(bias_out)

        parts = (back(query_ref[...]), back(pairs[:, :head]), pairs[:, head:])
        for i, part in enumerate(parts):
            columns = slice(i * head, (i + 1) * head)
            out[:, columns] = part.astype(jnp.bfloat16)
            bias_out[:, columns] += jnp.sum(part, axis=0, keepdims=True)

    by_block = lambda width: pl.BlockSpec((rows, width), lambda b, h: (b, 0))
    return pl.pallas_call(
        body,
        cost_estimate=small_cost,
        grid_spec=pltpu.PrefetchScalarGridSpec(
            num_scalar_prefetch=1,
            grid=(2,),
            in_specs=[
                by_block(head),
                by_block(2 * head),
                pl.BlockSpec((rows, 2 * head), lambda b, h: (1 - b, 0)),
                pl.BlockSpec((rows, 2 * head), lambda b, h: (0, 0)),
                by_block(128),
                by_block(128),
            ],
            out_specs=[by_block(3 * head), pl.BlockSpec((1, 3 * head), lambda b, h: (0, 0))],
        ),
        out_shape=[
            shape_of((2 * rows, 3 * head), jnp.bfloat16),
            shape_of((1, 3 * head), jnp.float32),
        ],
        name="rotated_back",
    )(later_of, query_grad, own_part, before_part, from_later, cosines, sines)


def branch_rows(half, attended, activated, weight_qd, weight_contract, dtype):
    rows = attended.shape[0] // 2
    tile = 1024
    depth = weight_qd.shape[0]

    def body(attended_ref, activated_ref, dense_ref, contract_ref, out):
        out[...] = (
            nt(attended_ref[...], dense_ref[...]) + nt(activated_ref[...], contract_ref[...])
        ).astype(dtype)

    return pl.pallas_call(
        body,
        cost_estimate=small_cost,
        grid=(depth // tile,),
        in_specs=[
            pl.BlockSpec((rows, attended.shape[1]), lambda j: (half, 0)),
            pl.BlockSpec((rows, activated.shape[1]), lambda j: (half, 0)),
            pl.BlockSpec((tile, attended.shape[1]), lambda j: (j, 3)),
            pl.BlockSpec((tile, activated.shape[1]), lambda j: (j, 0)),
        ],
        out_specs=pl.BlockSpec((rows, tile), lambda j: (0, j)),
        out_shape=shape_of((rows, depth), dtype),
        name="branch_%d" % half,
    )(attended, activated, weight_qd, weight_contract)


def back_rows(half, qkv_grad, pre_grad, x, weight_qd, weight_expand, vectors, dtype):
    rows = x.shape[0] // 2
    tile = 512
    depth = x.shape[1]

    def body(qkv_ref, pre_ref, x_ref, tile_ref, qd_ref, expand_ref, vector_ref, out, sums, stats):
        @pl.when(pl.program_id(0) == 0)
        def _():
            row = x_ref[...].astype(jnp.float32)
            mean = jnp.mean(row, axis=-1, keepdims=True)
            center = row - mean
            variance = jnp.mean(center * center, axis=-1, keepdims=True)
            stats[0] = jnp.broadcast_to(mean, stats.shape[1:])
            stats[1] = jnp.broadcast_to(lax.rsqrt(variance + norm_eps), stats.shape[1:])

        xhat = (tile_ref[...].astype(jnp.float32) - stats[0][:, :1]) * stats[1][:, :1]
        attn_back = nt(qkv_ref[...], qd_ref[...])
        mlp_back = nt(pre_ref[...], expand_ref[...])
        sums[0:1] = jnp.sum(attn_back * xhat, axis=0, keepdims=True)
        sums[1:2] = jnp.sum(attn_back, axis=0, keepdims=True)
        sums[2:3] = jnp.sum(mlp_back * xhat, axis=0, keepdims=True)
        sums[3:4] = jnp.sum(mlp_back, axis=0, keepdims=True)
        out[...] = (attn_back * vector_ref[0:1] + mlp_back * vector_ref[2:3]).astype(dtype)

    return pl.pallas_call(
        body,
        cost_estimate=small_cost,
        grid=(depth // tile,),
        in_specs=[
            pl.BlockSpec((rows, qkv_grad.shape[1]), lambda j: (half, 0)),
            pl.BlockSpec((rows, pre_grad.shape[1]), lambda j: (half, 0)),
            pl.BlockSpec((rows, depth), lambda j: (half, 0)),
            pl.BlockSpec((rows, tile), lambda j: (half, j)),
            pl.BlockSpec((tile, qkv_grad.shape[1]), lambda j: (j, 0)),
            pl.BlockSpec((tile, pre_grad.shape[1]), lambda j: (j, 0)),
            pl.BlockSpec((vectors.shape[0], tile), lambda j: (0, j)),
        ],
        out_specs=[
            pl.BlockSpec((rows, tile), lambda j: (0, j)),
            pl.BlockSpec((4, tile), lambda j: (0, j)),
        ],
        out_shape=[shape_of((rows, depth), dtype), shape_of((4, depth), jnp.float32)],
        scratch_shapes=[pltpu.VMEM((2, rows, 128), jnp.float32)],
        name="back_%d" % half,
    )(qkv_grad, pre_grad, x, x, weight_qd, weight_expand, vectors)


def tied(value, *others):
    return lax.optimization_barrier((value,) + others)[0]


def picked(values, index):
    rows = jnp.arange(values.shape[0], dtype=jnp.int32)
    chosen = index[:, None, None] == rows[None, :, None]
    return jnp.sum(jnp.where(chosen, values[None], 0), axis=1)


def per_device_paired(
    inputs,
    cotangent,
    segments,
    positions,
    qkv_weight,
    qkv_bias,
    dense_weight,
    expand_weight,
    expand_bias,
    contract_weight,
    norm_bias_vectors,
    moment_qkv_weight,
    moment_qkv_bias,
    moment_dense_weight,
    moment_expand_weight,
    moment_expand_bias,
    moment_contract_weight,
    moment_norm_vectors,
    second_qkv_weight,
    second_qkv_bias,
    second_dense_weight,
    second_expand_weight,
    second_expand_bias,
    second_contract_weight,
    second_norm_vectors,
):
    bf16, f32 = jnp.bfloat16, jnp.float32
    fsdp_index = lax.axis_index("fsdp")
    z = lax.axis_index("tensor")
    n_z = lax.axis_size("tensor")
    core = fsdp_index & 1
    chip = fsdp_index >> 1
    devices = range(lax.axis_size("fsdp"))
    to_core = [(i, i ^ 1) for i in devices]
    to_x = [(i, i ^ 2) for i in devices]
    to_y = [(i, i ^ 4) for i in devices]
    to_next = [(i, i + 2) for i in devices if i + 2 < len(devices)]
    to_prev = [(i + 2, i) for i in devices if i + 2 < len(devices)]
    first = core == 0
    head_dim = qkv_weight.shape[2] // 3
    shard_rows = inputs.shape[0]
    group_rows = n_z * shard_rows
    hidden = expand_weight.shape[1] // 2
    qkv_cols = 3 * head_dim
    shard_feat = expand_weight.shape[0]
    chip_feat = 2 * shard_feat

    def column_half(weight, k, width):
        return lax.dynamic_slice_in_dim(weight, k * width, width, axis=1).astype(bf16)

    def head_columns(k):
        return jnp.concatenate(
            [
                lax.dynamic_index_in_dim(qkv_weight, k, axis=1, keepdims=False),
                lax.dynamic_slice_in_dim(dense_weight, k * head_dim, head_dim, axis=1),
            ],
            axis=1,
        ).astype(bf16)

    def rows_of_chip(own, other):
        return jnp.concatenate(
            [jnp.where(first, own, other), jnp.where(first, other, own)], axis=0
        )

    x_group = lax.all_gather(inputs, "tensor", axis=0, tiled=True)
    dy_group = lax.all_gather(cotangent, "tensor", axis=0, tiled=True)

    swap_1 = send(head_columns(1 - core), "fsdp", to_core)
    block_1 = rows_of_chip(head_columns(core), swap_1)
    expand_in, contract_in = lax.optimization_barrier((expand_weight, contract_weight, swap_1))[:2]
    swap_2 = send(column_half(expand_in, 1 - core, hidden), "fsdp", to_core)
    swap_3 = send(column_half(contract_in, 1 - core, hidden), "fsdp", to_core)
    block_2 = rows_of_chip(column_half(expand_in, core, hidden), swap_2)
    contract_own, swap_3 = lax.optimization_barrier((contract_in, swap_3, block_2))[:2]
    block_3 = rows_of_chip(column_half(contract_own, core, hidden), swap_3)

    first_x, first_y = send(block_1, "fsdp", to_x), send(block_1, "fsdp", to_y)

    def passed_on(from_x, from_y, block):
        return (
            send(jnp.concatenate([from_y[:shard_feat], block], axis=0), "fsdp", to_x),
            send(jnp.concatenate([from_x[shard_feat:], block], axis=0), "fsdp", to_y),
        )

    second_x, second_y = passed_on(first_x, first_y, block_2)
    third_x, third_y = passed_on(second_x[shard_feat:], second_y[shard_feat:], block_3)
    pieces_1 = (block_1, (first_x, 0), (first_y, 0), (second_x, 0), (second_y, 0))

    segments_in, positions_in, dy_in = lax.optimization_barrier(
        (segments, positions, cotangent, block_2)
    )[:3]
    dy_sum = lax.optimization_barrier(jnp.sum(dy_in.astype(f32), axis=0, keepdims=True))
    position_other = send(positions_in, "fsdp", to_core)
    local = jnp.arange(group_rows, dtype=jnp.int32)
    groups = jnp.stack([fsdp_index, fsdp_index ^ 1, jnp.maximum(2 * chip - 1, 0)])
    seg_rows = picked(segments_in.reshape(-1, group_rows), groups)
    seg_halo = jnp.where(chip == 0, -1, seg_rows[2:])
    seg_rows = seg_rows[:2].reshape(1, 2 * group_rows)
    token_numbers = groups[:, None] * group_rows + local[None, :]
    token_rows = token_numbers[:2].reshape(1, 2 * group_rows)
    token_halo = token_numbers[2:]
    position_all = jnp.concatenate([positions_in, position_other])
    lane = jnp.arange(128, dtype=jnp.int32)
    half_rot = ROT // 2
    frequency = 10000.0 ** (-((lane % half_rot).astype(f32) * 2.0 / ROT))
    angles = jnp.where(
        lane[None, :] < ROT, position_all.astype(f32)[:, None] * frequency[None, :], 0.0
    )
    cosines = jnp.cos(angles)
    sines = jnp.sin(angles) * jnp.where(lane < half_rot, -1.0, 1.0)[None, :]
    halo_of = jnp.stack([first, ~first]).astype(jnp.int32)
    later_of = 1 - halo_of

    x_group = tied(x_group, first_x, first_y)
    x_all = jnp.concatenate([x_group, send(x_group, "fsdp", to_core)], axis=0)
    xhat, _ = normalized_row_block(x_all.astype(f32))
    xa = (xhat * norm_bias_vectors[0] + norm_bias_vectors[1]).astype(bf16)
    xm = (xhat * norm_bias_vectors[2] + norm_bias_vectors[3]).astype(bf16)

    head_bias = lax.dynamic_slice_in_dim(qkv_bias, core, 1, axis=0)
    weight_qd, qkv = qkv_product(xa, pieces_1, chip, head_bias, cosines, sines)
    kv_halo = send(
        jnp.where(first, qkv[group_rows:, head_dim:], qkv[:group_rows, head_dim:]), "fsdp", to_next
    )
    operands = (
        qkv,
        kv_halo,
        seg_rows,
        token_rows,
        seg_rows.reshape(2 * group_rows, 1),
        token_rows.reshape(2 * group_rows, 1),
        seg_halo,
        token_halo,
    )
    attended, lse = attention_forward(halo_of, operands)

    dy_group = tied(dy_group, qkv)
    dy_all = jnp.concatenate([dy_group, send(dy_group, "fsdp", to_core)], axis=0)

    third_x, third_y = lax.optimization_barrier((third_x, third_y, qkv))[:2]
    last_x = send(third_y[shard_feat : 2 * shard_feat], "fsdp", to_x)
    last_y = send(third_x[2 * shard_feat :], "fsdp", to_y)
    pieces_2 = (
        block_2,
        (second_x, shard_feat),
        (second_y, shard_feat),
        (third_x, 0),
        (third_y, 0),
    )
    pieces_3 = (block_3, (third_x, shard_feat), (third_y, shard_feat), (last_x, 0), (last_y, 0))
    expand_bias_half = lax.dynamic_slice_in_dim(expand_bias, core * hidden, hidden).reshape(1, -1)
    weight_expand, activated, slope = expand_product(xm, pieces_2, chip, expand_bias_half)

    def block_of(left, right, r):
        columns = lax.dynamic_slice_in_dim(left, (chip ^ r) * chip_feat, chip_feat, axis=1)
        return contract_rows(columns, right)

    def diagonal(left, right):
        return block_of(left, right, 3).astype(bf16)

    def sent_diagonal(block):
        return (
            send(block[:shard_feat], "fsdp", to_x),
            send(block[shard_feat:], "fsdp", to_y),
        )

    def neighbours(left, right, got):
        zero = jnp.zeros_like(got[0])
        for_x = block_of(left, right, 1) + jnp.concatenate([zero, got[1]], axis=0).astype(f32)
        for_y = block_of(left, right, 2) + jnp.concatenate([got[0], zero], axis=0).astype(f32)
        return for_x.astype(bf16), for_y.astype(bf16)

    def sent_neighbours(blocks):
        return send(blocks[0], "fsdp", to_x), send(blocks[1], "fsdp", to_y)

    def own_gradient(left, right, got):
        total = block_of(left, right, 0) + got[0].astype(f32) + got[1].astype(f32)
        kept = lax.dynamic_slice_in_dim(total, core * shard_feat, shard_feat, axis=0)
        given = lax.dynamic_slice_in_dim(total, (1 - core) * shard_feat, shard_feat, axis=0)
        taken = send(given, "fsdp", to_core)
        return jnp.where(first, kept, taken), jnp.where(first, taken, kept)

    dc_right = tied(jnp.concatenate([attended, activated], axis=1), last_x, last_y)
    dc_diagonal = diagonal(dy_all, dc_right)
    dc_got = sent_diagonal(dc_diagonal)
    attn_dy = tied(dy_all, dc_diagonal)
    attn_grad = product(attn_dy, weight_qd[:, qkv_cols:]).astype(bf16)
    query_grad, before_part, own_part = attention_backward(
        halo_of, operands, lse, attended, attn_grad
    )
    from_later = send(
        jnp.where(first, before_part[:group_rows], before_part[group_rows:]).astype(bf16),
        "fsdp",
        to_prev,
    )

    weight_contract, pre_grad, expand_bias_part = contract_product(
        dy_all, pieces_3, chip, tied(slope, before_part, dc_got)
    )
    dc_next = neighbours(tied(dy_all, pre_grad), dc_right, dc_got)
    dc_from = sent_neighbours(dc_next)
    qkv_grad, qkv_bias_part = rotated_back(
        later_of, tied(query_grad, dc_next), own_part, before_part, from_later, cosines, sines
    )
    qkv_diagonal = diagonal(xa, qkv_grad)
    qkv_got = sent_diagonal(qkv_diagonal)
    expand_diagonal = diagonal(tied(xm, qkv_diagonal), pre_grad)
    expand_got = sent_diagonal(expand_diagonal)

    branch_weight = tied(weight_contract, expand_diagonal)
    rows_of = lambda half, dtype: branch_rows(
        half, attended, activated, weight_qd, branch_weight, dtype
    )
    branch_other = send(rows_of(1, bf16), "fsdp", to_core)
    branch_rows_own = (rows_of(0, f32) + branch_other.astype(f32)).astype(bf16)
    backs = lambda half, back_x, dtype: back_rows(
        half, qkv_grad, pre_grad, back_x, weight_qd, weight_expand, norm_bias_vectors, dtype
    )
    qkv_next = neighbours(tied(xa, branch_rows_own, dc_from), qkv_grad, qkv_got)
    qkv_from = sent_neighbours(qkv_next)
    expand_next = neighbours(tied(xm, qkv_next), pre_grad, expand_got)
    expand_from = sent_neighbours(expand_next)
    weighted_other, sums_other = backs(1, tied(x_all, expand_next), bf16)
    weighted_other = send(weighted_other, "fsdp", to_core)
    weighted_own, sums_own = backs(0, tied(x_all, sums_other, qkv_from), f32)
    branch_sum = lax.psum_scatter(branch_rows_own, "tensor", scatter_dimension=0, tiled=True)
    vector_part = jnp.concatenate(
        [sums_own + sums_other, dy_sum], axis=0
    )
    bias_part = jnp.concatenate([qkv_bias_part, expand_bias_part], axis=1)
    n_vector = vector_part.size
    small = jnp.concatenate([vector_part.reshape(-1), bias_part.reshape(-1)]).reshape(-1, 128)
    small = small + send(small, "fsdp", to_x)
    small = small + send(small, "fsdp", to_y)
    small_other = send(small, "fsdp", to_core)
    flat, flat_other = small.reshape(-1), small_other.reshape(-1)
    vector_sum = (flat[:n_vector] + flat_other[:n_vector]).reshape(-1, 128)
    for bit in (1, 2):
        vector_sum = vector_sum + send(
            vector_sum, "tensor", [(i, i ^ bit) for i in range(n_z)]
        )
    vector_sum = vector_sum.reshape(vector_part.shape)
    grad_norm_vectors = jnp.concatenate([vector_sum, vector_sum[4:]], axis=0)
    bias_first = jnp.where(first, flat[n_vector:], flat_other[n_vector:])
    bias_second = jnp.where(first, flat_other[n_vector:], flat[n_vector:])
    grad_qkv_bias = jnp.stack([bias_first[:qkv_cols], bias_second[:qkv_cols]])
    grad_expand_bias = jnp.concatenate([bias_first[qkv_cols:], bias_second[qkv_cols:]])
    weighted_rows = (weighted_own + weighted_other.astype(f32)).astype(bf16)
    weighted_rows = tied(weighted_rows, branch_sum)
    weighted = lax.psum_scatter(
        weighted_rows, "tensor", scatter_dimension=0, tiled=True
    ).astype(f32)
    output = (
        inputs.astype(f32) + branch_sum.astype(f32) + norm_bias_vectors[4] + norm_bias_vectors[5]
    )
    xhat_own, inverse_own = normalized_row_block(inputs.astype(f32))
    block_input_gradient = cotangent.astype(f32) + inverse_own * (
        weighted
        - jnp.mean(weighted, axis=-1, keepdims=True)
        - xhat_own * jnp.mean(weighted * xhat_own, axis=-1, keepdims=True)
    )

    dc_halves = own_gradient(dy_all, dc_right, dc_from)
    qkv_halves = own_gradient(xa, qkv_grad, qkv_from)
    expand_halves = own_gradient(xm, pre_grad, expand_from)
    dc_halves, qkv_halves = lax.optimization_barrier((dc_halves, qkv_halves, weighted_rows))[:2]
    grad_contract_weight = jnp.concatenate([part[:, head_dim:] for part in dc_halves], axis=1)
    grad_dense_weight = jnp.concatenate([part[:, :head_dim] for part in dc_halves], axis=1)
    grad_expand_weight = jnp.concatenate(expand_halves, axis=1)
    grad_qkv_weight = jnp.stack(qkv_halves, axis=1)
    new_qkv_weight, new_moment_qkv_weight, new_second_qkv_weight = adam_step(
        qkv_weight,
        grad_qkv_weight,
        moment_qkv_weight,
        second_qkv_weight,
        rate_qkv_weight,
        decay_matrix,
    )
    new_qkv_bias, new_moment_qkv_bias, new_second_qkv_bias = adam_step(
        qkv_bias, grad_qkv_bias, moment_qkv_bias, second_qkv_bias, rate_qkv_bias, 0.0
    )
    new_dense_weight, new_moment_dense_weight, new_second_dense_weight = adam_step(
        dense_weight,
        grad_dense_weight,
        moment_dense_weight,
        second_dense_weight,
        rate_dense_weight,
        decay_matrix,
    )
    new_expand_weight, new_moment_expand_weight, new_second_expand_weight = adam_step(
        expand_weight,
        grad_expand_weight,
        moment_expand_weight,
        second_expand_weight,
        rate_expand_weight,
        decay_matrix,
    )
    new_expand_bias, new_moment_expand_bias, new_second_expand_bias = adam_step(
        expand_bias, grad_expand_bias, moment_expand_bias, second_expand_bias, rate_expand_bias, 0.0
    )
    new_contract_weight, new_moment_contract_weight, new_second_contract_weight = adam_step(
        contract_weight,
        grad_contract_weight,
        moment_contract_weight,
        second_contract_weight,
        rate_contract_weight,
        decay_matrix,
    )
    new_norm_vectors, new_moment_norm_vectors, new_second_norm_vectors = adam_step(
        norm_bias_vectors,
        grad_norm_vectors,
        moment_norm_vectors,
        second_norm_vectors,
        rate_norm_vectors,
        0.0,
    )
    return (
        output,
        block_input_gradient,
        grad_qkv_weight,
        new_qkv_weight,
        new_moment_qkv_weight,
        new_second_qkv_weight,
        grad_qkv_bias,
        new_qkv_bias,
        new_moment_qkv_bias,
        new_second_qkv_bias,
        grad_dense_weight,
        new_dense_weight,
        new_moment_dense_weight,
        new_second_dense_weight,
        grad_expand_weight,
        new_expand_weight,
        new_moment_expand_weight,
        new_second_expand_weight,
        grad_expand_bias,
        new_expand_bias,
        new_moment_expand_bias,
        new_second_expand_bias,
        grad_contract_weight,
        new_contract_weight,
        new_moment_contract_weight,
        new_second_contract_weight,
        grad_norm_vectors,
        new_norm_vectors,
        new_moment_norm_vectors,
        new_second_norm_vectors,
    )


def solution(mesh):
    paired = mesh.shape["fsdp"] == 8 and mesh.shape["tensor"] == 4
    per_device = per_device_paired if paired else per_device_generic
    return jax.shard_map(
        per_device,
        mesh=mesh,
        in_specs=(
            P(("fsdp", "tensor"), None),
            P(("fsdp", "tensor"), None),
            P(),
            P("fsdp"),
            P("fsdp", "tensor", None),
            P("tensor", None),
            P("fsdp", "tensor"),
            P("fsdp", "tensor"),
            P("tensor"),
            P("fsdp", "tensor"),
            P(),
            P("fsdp", "tensor", None),
            P("tensor", None),
            P("fsdp", "tensor"),
            P("fsdp", "tensor"),
            P("tensor"),
            P("fsdp", "tensor"),
            P(),
            P("fsdp", "tensor", None),
            P("tensor", None),
            P("fsdp", "tensor"),
            P("fsdp", "tensor"),
            P("tensor"),
            P("fsdp", "tensor"),
            P(),
        ),
        out_specs=(
            P(("fsdp", "tensor"), None),
            P(("fsdp", "tensor"), None),
            P("fsdp", "tensor", None),
            P("fsdp", "tensor", None),
            P("fsdp", "tensor", None),
            P("fsdp", "tensor", None),
            P("tensor", None),
            P("tensor", None),
            P("tensor", None),
            P("tensor", None),
            P("fsdp", "tensor"),
            P("fsdp", "tensor"),
            P("fsdp", "tensor"),
            P("fsdp", "tensor"),
            P("fsdp", "tensor"),
            P("fsdp", "tensor"),
            P("fsdp", "tensor"),
            P("fsdp", "tensor"),
            P("tensor"),
            P("tensor"),
            P("tensor"),
            P("tensor"),
            P("fsdp", "tensor"),
            P("fsdp", "tensor"),
            P("fsdp", "tensor"),
            P("fsdp", "tensor"),
            P(),
            P(),
            P(),
            P(),
        ),
        check_vma=False,
    )
```
